8 devices in a mesh: data: 4 (over z, y, x), stage: 2 (over core).
Axes of the slice: x: 2, y: 2, z: 1, core: 2. Of those that a mesh axis runs over, the one named last changes fastest.
Arguments:
- master_up: float32 [2, 576, 1536], P('stage', 'data')
- master_down: float32 [2, 1536, 576], P('stage', 'data')
- moment1_up: float32 [2, 576, 1536], P('stage', 'data')
- moment2_up: float32 [2, 576, 1536], P('stage', 'data')
- moment1_down: float32 [2, 1536, 576], P('stage', 'data')
- moment2_down: float32 [2, 1536, 576], P('stage', 'data')
- compute_up: bfloat16 [2, 576, 1536], P('stage')
- compute_down: bfloat16 [2, 1536, 576], P('stage')
- accum_up: float32 [4, 2, 576, 1536], P('data', 'stage')
- accum_down: float32 [4, 2, 1536, 576], P('data', 'stage')
- stage_acts: bfloat16 [2, 8192, 576], P('stage', 'data')
- loss_grad: bfloat16 [8192, 576], P('data')
- next_micro: bfloat16 [16, 8192, 576], P(None, 'data')
- learn_rate: float32 [], replicated
- max_norm: float32 [], replicated
Outputs:
- output 1: float32 [2, 576, 1536], P('stage', 'data')
- output 2: float32 [2, 1536, 576], P('stage', 'data')
- output 3: float32 [2, 576, 1536], P('stage', 'data')
- output 4: float32 [2, 576, 1536], P('stage', 'data')
- output 5: float32 [2, 1536, 576], P('stage', 'data')
- output 6: float32 [2, 1536, 576], P('stage', 'data')
- output 7: bfloat16 [16, 8192, 576], P(None, 'data')
All inputs are finite; a program needn't handle non-finite values.
Results may differ from the reference program's by a relative error of at most 0.00552048.
Values are sent between devices in bfloat16 or wider.
A program may use at most 1 GiB of HBM per device.

```python
import jax
import jax.numpy as jnp
from jax import lax

D_MODEL = 576
FF_WIDTH = 1536
STAGES = 2
REPLICAS = 4
TOKENS_DEV = 2048
MICRO_NEXT = 16
STEP_NUM = 10

BETA_ONE = 0.9
BETA_TWO = 0.95
ADAM_EPS = 1e-8
WEIGHT_DECAY = 0.1
NORM_EPS = 1e-6
BIAS_ONE = 1.0 - BETA_ONE ** STEP_NUM
BIAS_TWO = 1.0 - BETA_TWO ** STEP_NUM


def gelu_tanh(pre_act):
    return jax.nn.gelu(pre_act, approximate=True)


def stage_forward(stage_in, w_up, w_down):
    pre_act = jnp.dot(stage_in, w_up, preferred_element_type=jnp.float32)
    hidden = gelu_tanh(pre_act).astype(jnp.bfloat16)
    branch = jnp.dot(hidden, w_down, preferred_element_type=jnp.float32)
    return (stage_in.astype(jnp.float32) + branch).astype(jnp.bfloat16)


def stage_backward(stage_in, grad_in, w_up, w_down):
    pre_act = jnp.dot(stage_in, w_up, preferred_element_type=jnp.float32)
    hidden, gelu_pull = jax.vjp(gelu_tanh, pre_act)
    hidden = hidden.astype(jnp.bfloat16)
    dw_down = jnp.dot(hidden.T, grad_in, preferred_element_type=jnp.float32)
    d_hidden = jnp.dot(grad_in, w_down.T, preferred_element_type=jnp.float32)
    d_pre = gelu_pull(d_hidden)[0].astype(jnp.bfloat16)
    dw_up = jnp.dot(stage_in.T, d_pre, preferred_element_type=jnp.float32)
    d_in = grad_in.astype(jnp.float32) + jnp.dot(d_pre, w_up.T, preferred_element_type=jnp.float32)
    return dw_up, dw_down, d_in.astype(jnp.bfloat16)


def replica_grads(compute_up, compute_down, acts_one, grad_one):
    def stage_step(grad_in, stage_items):
        dw_up, dw_down, d_in = stage_backward(stage_items[2], grad_in, stage_items[0], stage_items[1])
        return d_in, (dw_up, dw_down)
    first_grad, stage_grads = lax.scan(stage_step, grad_one, (compute_up, compute_down, acts_one), reverse=True)
    return stage_grads


def batch_grads(compute_up, compute_down, stage_acts, loss_grad):
    acts_rep = stage_acts.reshape(STAGES, REPLICAS, TOKENS_DEV, D_MODEL).transpose(1, 0, 2, 3)
    grad_rep = loss_grad.reshape(REPLICAS, TOKENS_DEV, D_MODEL)
    zero_up = jnp.zeros((STAGES, D_MODEL, FF_WIDTH), jnp.float32)
    zero_down = jnp.zeros((STAGES, FF_WIDTH, D_MODEL), jnp.float32)
    zero_sq = jnp.zeros((STAGES,), jnp.float32)

    def replica_step(carry, items):
        sum_up, sum_down, sq_up, sq_down = carry
        dw_up, dw_down = replica_grads(compute_up, compute_down, items[0], items[1])
        carry_new = (sum_up + dw_up, sum_down + dw_down,
                     sq_up + jnp.sum(dw_up * dw_up, axis=(1, 2)),
                     sq_down + jnp.sum(dw_down * dw_down, axis=(1, 2)))
        return carry_new, None
    totals, unused = lax.scan(replica_step, (zero_up, zero_down, zero_sq, zero_sq), (acts_rep, grad_rep))
    return totals


def adamw_update(master, moment_one, moment_two, grad_step, learn_rate):
    mom_one = BETA_ONE * moment_one + (1.0 - BETA_ONE) * grad_step
    mom_two = BETA_TWO * moment_two + (1.0 - BETA_TWO) * grad_step * grad_step
    step_dir = (mom_one / BIAS_ONE) / (jnp.sqrt(mom_two / BIAS_TWO) + ADAM_EPS)
    new_master = master - learn_rate * (step_dir + WEIGHT_DECAY * master)
    return new_master, mom_one, mom_two


def forward_all(weight_up, weight_down, next_micro):
    blocks = next_micro.reshape(MICRO_NEXT * REPLICAS, TOKENS_DEV, D_MODEL)

    def run_block(block):
        def stage_step(stage_in, weights):
            return stage_forward(stage_in, weights[0], weights[1]), None
        result, unused = lax.scan(stage_step, block, (weight_up, weight_down))
        return result
    return lax.map(run_block, blocks).reshape(MICRO_NEXT, REPLICAS * TOKENS_DEV, D_MODEL)


def setup_inputs(seed: int = 0) -> dict:
    keys = jax.random.split(jax.random.key(seed), 16)
    rows = REPLICAS * TOKENS_DEV
    shape_up = (STAGES, D_MODEL, FF_WIDTH)
    shape_down = (STAGES, FF_WIDTH, D_MODEL)
    up_scale = D_MODEL ** -0.5
    down_scale = (FF_WIDTH * STAGES) ** -0.5
    master_up = jax.random.normal(keys[0], shape_up, jnp.float32) * up_scale
    master_down = jax.random.normal(keys[1], shape_down, jnp.float32) * down_scale
    compute_up = master_up.astype(jnp.bfloat16)
    compute_down = master_down.astype(jnp.bfloat16)
    stage_acts = jax.random.normal(keys[2], (STAGES, rows, D_MODEL), jnp.float32).astype(jnp.bfloat16)
    loss_grad = jax.random.normal(keys[3], (rows, D_MODEL), jnp.float32).astype(jnp.bfloat16)
    next_micro = jax.random.normal(keys[4], (MICRO_NEXT, rows, D_MODEL), jnp.float32).astype(jnp.bfloat16)
    sum_up, sum_down, sq_up, sq_down = batch_grads(compute_up, compute_down, stage_acts, loss_grad)
    rms_up = jnp.sqrt(sq_up / (REPLICAS * D_MODEL * FF_WIDTH))
    rms_down = jnp.sqrt(sq_down / (REPLICAS * D_MODEL * FF_WIDTH))
    accum_up = jax.random.normal(keys[5], (REPLICAS,) + shape_up, jnp.float32) * rms_up[None, :, None, None]
    accum_down = jax.random.normal(keys[6], (REPLICAS,) + shape_down, jnp.float32) * rms_down[None, :, None, None]
    avg_up = (jnp.sum(accum_up, axis=0) + sum_up) / REPLICAS
    avg_down = (jnp.sum(accum_down, axis=0) + sum_down) / REPLICAS
    grad_norm = jnp.sqrt(jnp.sum(avg_up * avg_up) + jnp.sum(avg_down * avg_down))
    max_norm = jax.random.uniform(keys[7], (), jnp.float32, 0.35, 0.65) * grad_norm
    clip = jnp.minimum(1.0, max_norm / (grad_norm + NORM_EPS))
    step_up = clip * jnp.sqrt(jnp.mean(avg_up * avg_up, axis=(1, 2)))[:, None, None]
    step_down = clip * jnp.sqrt(jnp.mean(avg_down * avg_down, axis=(1, 2)))[:, None, None]
    moment1_up = jax.random.normal(keys[8], shape_up, jnp.float32) * (0.05 * step_up)
    moment2_up = jax.random.uniform(keys[9], shape_up, jnp.float32, 0.5, 1.5) * (0.025 * step_up * step_up)
    moment1_down = jax.random.normal(keys[10], shape_down, jnp.float32) * (0.05 * step_down)
    moment2_down = jax.random.uniform(keys[11], shape_down, jnp.float32, 0.5, 1.5) * (0.025 * step_down * step_down)
    learn_rate = jax.random.uniform(keys[12], (), jnp.float32, 0.5, 1.0) * (0.1 * up_scale)
    return {'master_up': master_up, 'master_down': master_down,
            'moment1_up': moment1_up, 'moment2_up': moment2_up,
            'moment1_down': moment1_down, 'moment2_down': moment2_down,
            'compute_up': compute_up, 'compute_down': compute_down,
            'accum_up': accum_up, 'accum_down': accum_down,
            'stage_acts': stage_acts, 'loss_grad': loss_grad, 'next_micro': next_micro,
            'learn_rate': learn_rate, 'max_norm': max_norm}


def reference(master_up, master_down, moment1_up, moment2_up, moment1_down, moment2_down,
              compute_up, compute_down, accum_up, accum_down, stage_acts, loss_grad, next_micro,
              learn_rate, max_norm):
    sum_up, sum_down, sq_up, sq_down = batch_grads(compute_up, compute_down, stage_acts, loss_grad)
    avg_up = (jnp.sum(accum_up, axis=0) + sum_up) / REPLICAS
    avg_down = (jnp.sum(accum_down, axis=0) + sum_down) / REPLICAS
    total_sq = jnp.sum(avg_up * avg_up) + jnp.sum(avg_down * avg_down)
    clip = jnp.minimum(1.0, max_norm / (jnp.sqrt(total_sq) + NORM_EPS))
    new_up, mom1_up, mom2_up = adamw_update(master_up, moment1_up, moment2_up, clip * avg_up, learn_rate)
    new_down, mom1_down, mom2_down = adamw_update(master_down, moment1_down, moment2_down, clip * avg_down, learn_rate)
    last_acts = forward_all(new_up.astype(jnp.bfloat16), new_down.astype(jnp.bfloat16), next_micro)
    return (new_up, new_down, mom1_up, mom2_up, mom1_down, mom2_down, last_acts)
```

```python
import jax
import jax.numpy as jnp
from jax import lax
from jax.experimental import pallas as pl
from jax.experimental.pallas import tpu as pltpu
from jax.sharding import PartitionSpec as P

BETA_ONE = 0.9
BETA_TWO = 0.95
ADAM_EPS = 1e-8
WEIGHT_DECAY = 0.1
NORM_EPS = 1e-6
STEP_NUM = 10
BIAS_ONE = 1.0 - BETA_ONE ** STEP_NUM
BIAS_TWO = 1.0 - BETA_TWO ** STEP_NUM
DOT_ROWS = (((0,), (0,)), ((), ()))
DOT_COLS = (((1,), (1,)), ((), ()))


def gelu_tanh(pre_act):
    return jax.nn.gelu(pre_act, approximate=True)


def stage_backward(stage_in, grad_in, w_up, w_down):
    pre_act = jnp.dot(stage_in, w_up, preferred_element_type=jnp.float32)
    hidden, gelu_pull = jax.vjp(gelu_tanh, pre_act)
    hidden = hidden.astype(jnp.bfloat16)
    dw_down = lax.dot_general(hidden, grad_in, DOT_ROWS, preferred_element_type=jnp.float32)
    d_hidden = lax.dot_general(grad_in, w_down, DOT_COLS, preferred_element_type=jnp.float32)
    d_pre = gelu_pull(d_hidden)[0].astype(jnp.bfloat16)
    dw_up = lax.dot_general(stage_in, d_pre, DOT_ROWS, preferred_element_type=jnp.float32)
    d_in = grad_in.astype(jnp.float32) + lax.dot_general(d_pre, w_up, DOT_COLS, preferred_element_type=jnp.float32)
    return dw_up, dw_down, d_in.astype(jnp.bfloat16)


def adamw_update(master, moment_one, moment_two, grad_step, learn_rate):
    mom_one = BETA_ONE * moment_one + (1.0 - BETA_ONE) * grad_step
    mom_two = BETA_TWO * moment_two + (1.0 - BETA_TWO) * grad_step * grad_step
    step_dir = (mom_one / BIAS_ONE) / (jnp.sqrt(mom_two / BIAS_TWO) + ADAM_EPS)
    new_master = master - learn_rate * (step_dir + WEIGHT_DECAY * master)
    return new_master, mom_one, mom_two


GELU_LIN = 0.7978845608028654
GELU_CUB = GELU_LIN * 0.044715
ROW_TILE = 512
FF_TILE = 512
CHUNKS = (4, 2, 1, 1)


def gelu_half(pre_act):
    inner = pre_act * (GELU_LIN + GELU_CUB * (pre_act * pre_act))
    half = 0.5 * pre_act
    return half + half * jnp.tanh(inner)


def block_forward(cols_in, w_up_t, w_down_t, block, hidden_ref):
    ff_width = w_up_t.shape[1]
    for start in range(0, ff_width, FF_TILE):
        pre_act = jnp.dot(w_up_t[block, start:start + FF_TILE, :], cols_in, preferred_element_type=jnp.float32)
        hidden_ref[start:start + FF_TILE, :] = gelu_half(pre_act).astype(jnp.bfloat16)
    branch = jnp.dot(w_down_t[block], hidden_ref[...], preferred_element_type=jnp.float32)
    return (cols_in.astype(jnp.float32) + branch).astype(jnp.bfloat16)


def forward_kernel(has_prev, n_recv, base, recv_base, n_own, n_tiles, *refs):
    refs = list(refs)
    x_ref, w_up_t, w_down_t = refs[:3]
    refs = refs[3:]
    recv_ref = None
    if n_recv:
        recv_ref = refs.pop(0)
    if has_prev:
        refs.pop(0)
    out_ref, y_ref, hidden_ref, y_buf, y_sem, recv_sem = refs
    mine = lax.axis_index('stage')
    micro, tile = pl.program_id(0), pl.program_id(1)
    step = micro * n_tiles + tile
    slot = lax.rem(step, 2)
    tile_cols = pl.ds(pl.multiple_of(tile * ROW_TILE, ROW_TILE), ROW_TILE)

    def y_copy(which):
        return pltpu.make_async_copy(y_buf.at[which], out_ref.at[mine * n_own + base + micro, :, tile_cols], y_sem.at[which])

    def recv_copy():
        first = (1 - mine) * n_own + recv_base
        return pltpu.make_async_copy(recv_ref, out_ref.at[pl.ds(first, n_recv), :, tile_cols], recv_sem)

    if n_recv:
        recv_copy().start()

    cols = x_ref[0]
    for block in range(2):
        cols = block_forward(cols, w_up_t, w_down_t, block, hidden_ref)

    @pl.when(step >= 2)
    def _():
        y_copy(slot).wait()

    y_buf[slot] = cols
    y_ref[0] = cols
    y_copy(slot).start()
    if n_recv:
        recv_copy().wait()

    @pl.when(step == pl.num_programs(0) * n_tiles - 1)
    def _():
        y_copy(slot).wait()
        y_copy(1 - slot).wait()


def forward_chunk(base, n_chunk, micro_t, w_up_t, w_down_t, prev_out, recv, recv_base):
    n_micro, width, n_rows = micro_t.shape
    n_own = n_micro // 2
    n_tiles = n_rows // ROW_TILE
    ff_width = w_up_t.shape[1]
    n_recv = 0 if recv is None else recv.shape[0]
    mine = lax.axis_index('stage')
    any_spec = pl.BlockSpec(memory_space=pl.ANY)
    scalar = jnp.full((1,), mine * n_own + base, jnp.int32)
    in_specs = [pl.BlockSpec((1, width, ROW_TILE), lambda i, j, first: (first[0] + i, 0, j)),
                pl.BlockSpec((2, ff_width, width), lambda i, j, first: (0, 0, 0)),
                pl.BlockSpec((2, width, ff_width), lambda i, j, first: (0, 0, 0))]
    operands = [micro_t, w_up_t, w_down_t]
    if n_recv:
        in_specs.append(pl.BlockSpec((n_recv, width, ROW_TILE), lambda i, j, first: (0, 0, j)))
        operands.append(recv)
    aliases = {}
    if prev_out is not None:
        in_specs.append(any_spec)
        operands.append(prev_out)
        aliases = {len(operands): 0}

    def body(first, *refs):
        forward_kernel(prev_out is not None, n_recv, base, recv_base, n_own, n_tiles, *refs)

    flops = 8 * n_chunk * n_rows * width * ff_width
    return pl.pallas_call(
        body,
        grid_spec=pltpu.PrefetchScalarGridSpec(
            num_scalar_prefetch=1, grid=(n_chunk, n_tiles), in_specs=in_specs,
            out_specs=[any_spec, pl.BlockSpec((1, width, ROW_TILE), lambda i, j, first: (i, 0, j))],
            scratch_shapes=[pltpu.VMEM((ff_width, ROW_TILE), jnp.bfloat16), pltpu.VMEM((2, width, ROW_TILE), jnp.bfloat16),
                            pltpu.SemaphoreType.DMA((2,)), pltpu.SemaphoreType.DMA]),
        out_shape=[jax.ShapeDtypeStruct(micro_t.shape, jnp.bfloat16),
                   jax.ShapeDtypeStruct((n_chunk, width, n_rows), jnp.bfloat16)],
        input_output_aliases=aliases,
        compiler_params=pltpu.CompilerParams(dimension_semantics=("arbitrary", "arbitrary"),
                                             vmem_limit_bytes=48 * 1024 * 1024),
        cost_estimate=pl.CostEstimate(flops=flops, bytes_accessed=4 * n_chunk * n_rows * width, transcendentals=0),
        name=f"fwd_{base}",
    )(scalar, *operands)


def forward_all(micro_in, w_up_t, w_down_t):
    micro_t = jnp.swapaxes(micro_in, 1, 2)
    n_own = micro_in.shape[0] // 2
    swap = [(0, 1), (1, 0)]
    mine = lax.axis_index('stage')
    out, base = None, 0
    received = []
    for n_chunk in CHUNKS:
        recv, recv_base = None, 0
        if len(received) >= 2 and received[-2] is not None:
            recv, recv_base = received[-2]
            received[-2] = None
        out, part = forward_chunk(base, n_chunk, micro_t, w_up_t, w_down_t, out, recv, recv_base)
        received.append((lax.ppermute(part, 'stage', swap), base))
        base += n_chunk
    for item in received:
        if item is not None:
            out = lax.dynamic_update_slice(out, item[0], ((1 - mine) * n_own + item[1], 0, 0))
    return jnp.swapaxes(out, 1, 2)


def solution(mesh):
    n_stage = mesh.shape['stage']
    n_data = mesh.shape['data']
    last_stage = n_stage - 1
    back_perm = [(source, source - 1) for source in range(1, n_stage)]

    def backward_stages(my_stage, stage_in, grad_last, w_up, w_down, acc_up, acc_down):
        def run_stage(operands):
            grad_in, sum_up, sum_down = operands
            dw_up, dw_down, d_in = stage_backward(stage_in, grad_in, w_up, w_down)
            return sum_up + dw_up, sum_down + dw_down, d_in

        def pass_through(operands):
            return operands[1], operands[2], operands[0]

        grad_buf = grad_last
        for step in range(n_stage):
            acc_up, acc_down, d_in = lax.cond(my_stage == last_stage - step, run_stage, pass_through,
                                              (grad_buf, acc_up, acc_down))
            if step < last_stage:
                grad_buf = lax.ppermute(d_in, 'stage', back_perm)
        return acc_up, acc_down

    def step_body(master_up, master_down, moment1_up, moment2_up, moment1_down, moment2_down,
                  compute_up, compute_down, accum_up, accum_down, stage_acts, loss_grad, next_micro,
                  learn_rate, max_norm):
        my_stage = lax.axis_index('stage')
        sum_up, sum_down = backward_stages(my_stage, stage_acts[0], loss_grad, compute_up[0], compute_down[0],
                                           accum_up[0, 0], accum_down[0, 0])
        shard_up = lax.psum_scatter(sum_up, 'data', scatter_dimension=0, tiled=True) / n_data
        shard_down = lax.psum_scatter(sum_down, 'data', scatter_dimension=0, tiled=True) / n_data
        local_sq = jnp.sum(shard_up * shard_up) + jnp.sum(shard_down * shard_down)
        total_sq = lax.psum(local_sq, ('stage', 'data'))
        clip = jnp.minimum(1.0, max_norm / (jnp.sqrt(total_sq) + NORM_EPS))
        new_up, mom1_up, mom2_up = adamw_update(master_up[0], moment1_up[0], moment2_up[0], clip * shard_up, learn_rate)
        new_down, mom1_down, mom2_down = adamw_update(master_down[0], moment1_down[0], moment2_down[0], clip * shard_down, learn_rate)
        full_up = lax.all_gather(new_up.astype(jnp.bfloat16), 'data', axis=0, tiled=True)
        full_down = lax.all_gather(new_down.astype(jnp.bfloat16), 'data', axis=0, tiled=True)
        both_up = lax.all_gather(full_up.T, 'stage')
        both_down = lax.all_gather(full_down.T, 'stage')
        last_acts = forward_all(next_micro, both_up, both_down)
        return (new_up[None], new_down[None], mom1_up[None], mom2_up[None],
                mom1_down[None], mom2_down[None], last_acts)

    shard_spec = P('stage', 'data', None)
    whole_spec = P('stage', None, None)
    accum_spec = P('data', 'stage', None, None)
    micro_spec = P(None, 'data', None)
    in_specs = (shard_spec,) * 6 + (whole_spec, whole_spec, accum_spec, accum_spec,
                                    P('stage', 'data', None), P('data', None), micro_spec, P(), P())
    out_specs = (shard_spec,) * 6 + (micro_spec,)
    return jax.shard_map(step_body, mesh=mesh, in_specs=in_specs, out_specs=out_specs, check_vma=False)
```

```python
import jax
import jax.numpy as jnp
from jax import lax
from jax.experimental import pallas as pl
from jax.experimental.pallas import tpu as pltpu
from jax.sharding import PartitionSpec as P

BETA_ONE = 0.9
BETA_TWO = 0.95
ADAM_EPS = 1e-8
WEIGHT_DECAY = 0.1
NORM_EPS = 1e-6
STEP_NUM = 10
BIAS_ONE = 1.0 - BETA_ONE ** STEP_NUM
BIAS_TWO = 1.0 - BETA_TWO ** STEP_NUM


def adamw_update(master, moment_one, moment_two, grad_step, learn_rate):
    mom_one = BETA_ONE * moment_one + (1.0 - BETA_ONE) * grad_step
    mom_two = BETA_TWO * moment_two + (1.0 - BETA_TWO) * grad_step * grad_step
    step_dir = (mom_one / BIAS_ONE) / (jnp.sqrt(mom_two / BIAS_TWO) + ADAM_EPS)
    new_master = master - learn_rate * (step_dir + WEIGHT_DECAY * master)
    return new_master, mom_one, mom_two


MESH_ID = pl.DeviceIdType.MESH
GRAD_TILE = 512
GELU_LIN = 0.7978845608028654
GELU_CUB = GELU_LIN * 0.044715
ROW_TILE = 512
FF_TILE = 512
CHUNKS = (4, 2, 1, 1)


def gelu_half(pre_act):
    inner = pre_act * (GELU_LIN + GELU_CUB * (pre_act * pre_act))
    half = 0.5 * pre_act
    return half + half * jnp.tanh(inner)


def block_forward(cols_in, w_up_t, w_down_t, block, hidden_ref):
    ff_width = w_up_t.shape[1]
    for start in range(0, ff_width, FF_TILE):
        pre_act = jnp.dot(w_up_t[block, start:start + FF_TILE, :], cols_in, preferred_element_type=jnp.float32)
        hidden_ref[start:start + FF_TILE, :] = gelu_half(pre_act).astype(jnp.bfloat16)
    branch = jnp.dot(w_down_t[block], hidden_ref[...], preferred_element_type=jnp.float32)
    return (cols_in.astype(jnp.float32) + branch).astype(jnp.bfloat16)


def forward_kernel(has_prev, n_recv, base, recv_base, n_own, n_tiles, *refs):
    refs = list(refs)
    x_ref, w_up_t, w_down_t = refs[:3]
    refs = refs[3:]
    recv_ref = None
    if n_recv:
        recv_ref = refs.pop(0)
    if has_prev:
        refs.pop(0)
    out_ref, y_ref, hidden_ref, y_buf, y_sem, recv_sem = refs
    mine = lax.axis_index('stage')
    micro, tile = pl.program_id(0), pl.program_id(1)
    step = micro * n_tiles + tile
    slot = lax.rem(step, 2)
    tile_cols = pl.ds(pl.multiple_of(tile * ROW_TILE, ROW_TILE), ROW_TILE)

    def y_copy(which):
        return pltpu.make_async_copy(y_buf.at[which], out_ref.at[mine * n_own + base + micro, :, tile_cols], y_sem.at[which])

    def recv_copy():
        first = (1 - mine) * n_own + recv_base
        return pltpu.make_async_copy(recv_ref, out_ref.at[pl.ds(first, n_recv), :, tile_cols], recv_sem)

    if n_recv:
        recv_copy().start()

    cols = x_ref[0]
    for block in range(2):
        cols = block_forward(cols, w_up_t, w_down_t, block, hidden_ref)

    @pl.when(step >= 2)
    def _():
        y_copy(slot).wait()

    y_buf[slot] = cols
    y_ref[0] = cols
    y_copy(slot).start()
    if n_recv:
        recv_copy().wait()

    @pl.when(step == pl.num_programs(0) * n_tiles - 1)
    def _():
        y_copy(slot).wait()
        y_copy(1 - slot).wait()


def forward_chunk(base, n_chunk, micro_t, w_up_t, w_down_t, prev_out, recv, recv_base):
    n_micro, width, n_rows = micro_t.shape
    n_own = n_micro // 2
    n_tiles = n_rows // ROW_TILE
    ff_width = w_up_t.shape[1]
    n_recv = 0 if recv is None else recv.shape[0]
    mine = lax.axis_index('stage')
    any_spec = pl.BlockSpec(memory_space=pl.ANY)
    scalar = jnp.full((1,), mine * n_own + base, jnp.int32)
    in_specs = [pl.BlockSpec((1, width, ROW_TILE), lambda i, j, first: (first[0] + i, 0, j)),
                pl.BlockSpec((2, ff_width, width), lambda i, j, first: (0, 0, 0)),
                pl.BlockSpec((2, width, ff_width), lambda i, j, first: (0, 0, 0))]
    operands = [micro_t, w_up_t, w_down_t]
    if n_recv:
        in_specs.append(pl.BlockSpec((n_recv, width, ROW_TILE), lambda i, j, first: (0, 0, j)))
        operands.append(recv)
    aliases = {}
    if prev_out is not None:
        in_specs.append(any_spec)
        operands.append(prev_out)
        aliases = {len(operands): 0}

    def body(first, *refs):
        forward_kernel(prev_out is not None, n_recv, base, recv_base, n_own, n_tiles, *refs)

    flops = 8 * n_chunk * n_rows * width * ff_width
    return pl.pallas_call(
        body,
        grid_spec=pltpu.PrefetchScalarGridSpec(
            num_scalar_prefetch=1, grid=(n_chunk, n_tiles), in_specs=in_specs,
            out_specs=[any_spec, pl.BlockSpec((1, width, ROW_TILE), lambda i, j, first: (i, 0, j))],
            scratch_shapes=[pltpu.VMEM((ff_width, ROW_TILE), jnp.bfloat16), pltpu.VMEM((2, width, ROW_TILE), jnp.bfloat16),
                            pltpu.SemaphoreType.DMA((2,)), pltpu.SemaphoreType.DMA]),
        out_shape=[jax.ShapeDtypeStruct(micro_t.shape, jnp.bfloat16),
                   jax.ShapeDtypeStruct((n_chunk, width, n_rows), jnp.bfloat16)],
        input_output_aliases=aliases,
        compiler_params=pltpu.CompilerParams(dimension_semantics=("arbitrary", "arbitrary"),
                                             vmem_limit_bytes=48 * 1024 * 1024),
        cost_estimate=pl.CostEstimate(flops=flops, bytes_accessed=4 * n_chunk * n_rows * width, transcendentals=0),
        name=f"fwd_{base}",
    )(scalar, *operands)


def forward_all(micro_in, w_up_t, w_down_t):
    micro_t = jnp.swapaxes(micro_in, 1, 2)
    n_own = micro_in.shape[0] // 2
    swap = [(0, 1), (1, 0)]
    mine = lax.axis_index('stage')
    out, base = None, 0
    received = []
    for n_chunk in CHUNKS:
        recv, recv_base = None, 0
        if len(received) >= 2 and received[-2] is not None:
            recv, recv_base = received[-2]
            received[-2] = None
        out, part = forward_chunk(base, n_chunk, micro_t, w_up_t, w_down_t, out, recv, recv_base)
        received.append((lax.ppermute(part, 'stage', swap), base))
        base += n_chunk
    for item in received:
        if item is not None:
            out = lax.dynamic_update_slice(out, item[0], ((1 - mine) * n_own + item[1], 0, 0))
    return jnp.swapaxes(out, 1, 2)


def gelu_pair(pre_act):
    square = pre_act * pre_act
    tanh_in = jnp.tanh(pre_act * (GELU_LIN + GELU_CUB * square))
    half = 0.5 * pre_act
    value = half + half * tanh_in
    slope = 0.5 + 0.5 * tanh_in + half * (1.0 - tanh_in * tanh_in) * (GELU_LIN + 3.0 * GELU_CUB * square)
    return value, slope


def update_kernel(n_data, mst_up, mst_dn, mo1_up, mo2_up, mo1_dn, mo2_dn, cmp_up, cmp_dn, acc_up, acc_dn, acts_in, grad_in,
                  rate_ref, norm_ref,
                  new_up, new_dn, out1_up, out2_up, out1_dn, out2_dn, w_up_out, w_dn_out,
                  wts, acts, acts_row, grad, grad_row, d_pre, sums, part, fwd_up, fwd_dn, last_up, last_dn,
                  st_up, st_dn, norm_tiles, turned, send_sem, recv_sem, load_sem, store_sem):
    chip = lax.axis_index('data')
    core = lax.axis_index('stage')
    peer = 1 - core
    pos_x, pos_y = lax.rem(chip, 2), chip // 2
    chip_x = pos_y * 2 + (1 - pos_x)
    chip_y = (1 - pos_y) * 2 + pos_x
    chip_d = 3 - chip
    me = chip * 2 + core
    n_dev = 2 * n_data
    half_rows = grad.shape[1]
    ff_width = wts.shape[3]
    up_rows = st_up.shape[1]
    dn_cols = st_dn.shape[2]
    n_tile = ff_width // GRAD_TILE

    def cols_of(index, size):
        return pl.ds(pl.multiple_of(index * size, size), size)

    def rows_of(index):
        return pl.ds(pl.multiple_of(index * up_rows, 8), up_rows)

    def remote(src, dst, index, device):
        return pltpu.make_async_remote_copy(src_ref=src, dst_ref=dst, send_sem=send_sem.at[index], recv_sem=recv_sem.at[index],
                                            device_id=device, device_id_type=MESH_ID)

    to_peer, to_x, to_y = (chip, peer), (chip_x, core), (chip_y, core)

    barrier = pltpu.get_barrier_semaphore()
    for offset in range(1, n_dev):
        other = lax.rem(me + offset, n_dev)
        pl.semaphore_signal(barrier, inc=1, device_id=(other // 2, lax.rem(other, 2)), device_id_type=MESH_ID)
    pl.semaphore_wait(barrier, n_dev - 1)

    swap_in = [remote(acts_in.at[:, cols_of(peer, half_rows)], acts.at[core], 0, to_peer),
               remote(cmp_up, wts.at[core, 0], 1, to_peer),
               remote(cmp_dn, wts.at[core, 1], 2, to_peer)]
    for copy in swap_in:
        copy.start()
    loads = [pltpu.make_async_copy(src, dst, load_sem.at[index]) for index, (src, dst) in enumerate([
        (grad_in.at[:, cols_of(core, half_rows)], grad), (acts_in.at[:, cols_of(core, half_rows)], acts.at[core]),
        (cmp_up, wts.at[core, 0]), (cmp_dn, wts.at[core, 1]),
        (acc_up, sums.at[core, 0]), (acc_dn, sums.at[core, 1]),
        (mst_up, st_up.at[0]), (mo1_up, st_up.at[1]), (mo2_up, st_up.at[2]),
        (mst_dn, st_dn.at[0]), (mo1_dn, st_dn.at[1]), (mo2_dn, st_dn.at[2])])]
    for copy in loads:
        copy.start()

    def part_copy(kind, tile):
        cols = cols_of(tile, GRAD_TILE)
        return remote(sums.at[peer, kind, :, cols], part.at[kind, :, cols], 3 + kind * n_tile + tile, to_peer)

    up_first = [remote(sums.at[core, 0, rows_of(row * 2 + 1 - pos_x)], fwd_up.at[slot], 9 + slot, to_x)
                for slot, row in enumerate((1 - pos_y, pos_y))]
    dn_first = [remote(sums.at[core, 1, :, cols_of((1 - pos_y) * 2 + col, dn_cols)], fwd_dn.at[slot], 12 + slot, to_y)
                for slot, col in enumerate((1 - pos_x, pos_x))]
    up_next = remote(sums.at[core, 0, rows_of(chip_y)], last_up, 11, to_y)
    dn_next = remote(sums.at[core, 1, :, cols_of(chip_x, dn_cols)], last_dn, 14, to_x)

    def add_up(index):
        sums[core, 0, rows_of(index)] += part[0, rows_of(index)]

    def add_dn(index):
        cols = cols_of(index, dn_cols)
        sums[core, 1, :, cols] += part[1, :, cols]

    def begin_scatter():
        for kind in range(2):
            for tile in range(n_tile):
                part_copy(kind, tile).wait_recv()
        for slot in range(2):
            add_up((1 - pos_y if slot == 0 else pos_y) * 2 + 1 - pos_x)
            up_first[slot].start()
            add_dn((1 - pos_y) * 2 + (1 - pos_x if slot == 0 else pos_x))
            dn_first[slot].start()
        add_up(chip_y)
        add_dn(chip_x)
        add_up(chip)
        add_dn(chip)

    loads[0].wait()
    for block in (1, 0):
        own = core == block

        @pl.when(own)
        def _():
            for copy in loads[1:6]:
                copy.wait()

        @pl.when(jnp.logical_not(own))
        def _():
            for copy in swap_in:
                copy.wait_recv()

        acts_row[...] = acts[block].T
        grad_row[...] = grad[...].T

        def tile_step(tile, carry, block=block, own=own):
            cols = cols_of(tile, GRAD_TILE)
            pre_act = jnp.dot(acts_row[...], wts[block, 0, :, cols], preferred_element_type=jnp.float32)
            hidden, slope = gelu_pair(pre_act)
            dw_down = jnp.dot(grad[...], hidden.astype(jnp.bfloat16), preferred_element_type=jnp.float32)
            d_hidden = jnp.dot(grad_row[...], wts[block, 1, :, cols], preferred_element_type=jnp.float32)
            d_pre[:, cols] = (d_hidden * slope).astype(jnp.bfloat16)
            dw_up = jnp.dot(acts[block], d_pre[:, cols], preferred_element_type=jnp.float32)

            @pl.when(own)
            def _():
                sums[block, 0, :, cols] += dw_up
                sums[block, 1, :, cols] += dw_down

            @pl.when(jnp.logical_not(own))
            def _():
                sums[block, 0, :, cols] = dw_up
                sums[block, 1, :, cols] = dw_down
                part_copy(0, tile).start()
                part_copy(1, tile).start()
            return carry

        if block == 1:
            lax.fori_loop(0, n_tile, tile_step, 0)
            d_in = lax.dot_general(wts[1, 0], d_pre[...], (((1,), (1,)), ((), ())), preferred_element_type=jnp.float32)
            grad[...] = (grad[...].astype(jnp.float32) + d_in).astype(jnp.bfloat16)
        else:
            lax.fori_loop(0, 1, tile_step, 0)
            pl.when(core == 1)(begin_scatter)
            lax.fori_loop(1, n_tile, tile_step, 0)
    pl.when(core == 0)(begin_scatter)

    up_first[0].wait_recv()
    sums[core, 0, rows_of(chip_y)] += fwd_up[0]
    up_next.start()
    dn_first[0].wait_recv()
    sums[core, 1, :, cols_of(chip_x, dn_cols)] += fwd_dn[0]
    dn_next.start()
    up_first[1].wait_recv()
    dn_first[1].wait_recv()
    up_next.wait_recv()
    scale = 1.0 / n_data
    mean_up = (sums[core, 0, rows_of(chip)] + fwd_up[1] + last_up[...]) * scale
    last_up[...] = mean_up
    square = jnp.sum((mean_up * mean_up).reshape(up_rows // 8, 8, ff_width), axis=0)
    dn_next.wait_recv()
    mean_dn = (sums[core, 1, :, cols_of(chip, dn_cols)] + fwd_dn[1] + last_dn[...]) * scale
    last_dn[...] = mean_dn
    square_dn = jnp.sum((mean_dn * mean_dn).reshape(st_dn.shape[1] // 8, 8, dn_cols), axis=0)
    tile_sum = sum(square[:, first:first + 128] for first in range(0, ff_width, 128))
    tile_sum = tile_sum + sum(square_dn[:, first:first + 128] for first in range(0, dn_cols, 128))
    norm_tiles[me] = tile_sum
    norm_copies = []
    for offset in range(1, n_dev):
        other = lax.rem(me + offset, n_dev)
        norm_copies.append(remote(norm_tiles.at[me], norm_tiles.at[me], 14 + offset, (other // 2, lax.rem(other, 2))))
    for copy in norm_copies:
        copy.start()
    for copy in loads[6:]:
        copy.wait()
    for copy in norm_copies:
        copy.wait_recv()
    total_sq = jnp.sum(jnp.sum(norm_tiles[...], axis=0), keepdims=True)
    clip = jnp.minimum(1.0, norm_ref[0] / (jnp.sqrt(total_sq) + NORM_EPS))
    rate = rate_ref[0]

    own_up, own_dn = rows_of(chip), cols_of(chip, dn_cols)
    state = adamw_update(st_up[0], st_up[1], st_up[2], clip * last_up[...], rate)
    wts[core, 0, own_up] = state[0].astype(jnp.bfloat16)
    for index in range(3):
        st_up[index] = state[index]
    up_at = [wts.at[core, 0, rows_of(index)] for index in (chip, chip_x, chip_y, chip_d)]
    dn_at = [wts.at[core, 1, :, cols_of(index, dn_cols)] for index in (chip, chip_x, chip_y, chip_d)]
    up_x, up_y, up_relay = remote(up_at[0], up_at[0], 22, to_x), remote(up_at[0], up_at[0], 24, to_y), remote(up_at[1], up_at[1], 26, to_y)
    dn_x, dn_y, dn_relay = remote(dn_at[0], dn_at[0], 23, to_x), remote(dn_at[0], dn_at[0], 25, to_y), remote(dn_at[2], dn_at[2], 27, to_x)
    up_peer = [remote(up_at[index], up_at[index], 28 + index, to_peer) for index in range(4)]
    dn_peer = [remote(dn_at[index], dn_at[index], 32 + index, to_peer) for index in range(4)]
    up_x.start()
    up_y.start()
    up_peer[0].start()
    state = adamw_update(st_dn[0], st_dn[1], st_dn[2], clip * last_dn[...], rate)
    wts[core, 1, :, own_dn] = state[0].astype(jnp.bfloat16)
    for index in range(3):
        st_dn[index] = state[index]
    dn_y.start()
    dn_x.start()
    dn_peer[0].start()
    stores = [pltpu.make_async_copy(src, dst, store_sem.at[index]) for index, (src, dst) in enumerate([
        (st_up.at[0], new_up), (st_up.at[1], out1_up), (st_up.at[2], out2_up),
        (st_dn.at[0], new_dn), (st_dn.at[1], out1_dn), (st_dn.at[2], out2_dn)])]
    for copy in stores:
        copy.start()
    up_x.wait_recv()
    up_relay.start()
    up_peer[1].start()
    dn_y.wait_recv()
    dn_relay.start()
    dn_peer[2].start()
    up_y.wait_recv()
    up_peer[2].start()
    dn_x.wait_recv()
    dn_peer[1].start()
    up_relay.wait_recv()
    up_peer[3].start()
    dn_relay.wait_recv()
    dn_peer[3].start()
    for copy in up_peer + dn_peer:
        copy.wait_recv()
    finals = []
    for block in range(2):
        finals.append(pltpu.make_async_copy(wts.at[block, 1], w_dn_out.at[block], store_sem.at[6 + block]))
        finals[-1].start()
    for block in range(2):
        if block:
            finals[-1].wait()
        turned[...] = wts[block, 0].T
        finals.append(pltpu.make_async_copy(turned, w_up_out.at[block], store_sem.at[8 + block]))
        finals[-1].start()
    for copy in swap_in + up_first + dn_first + [up_next, dn_next] + norm_copies:
        copy.wait_send()
    for kind in range(2):
        for tile in range(n_tile):
            part_copy(kind, tile).wait_send()
    for copy in [up_x, up_y, up_relay, dn_x, dn_y, dn_relay] + up_peer + dn_peer:
        copy.wait_send()
    for copy in stores + finals[:2] + finals[3:]:
        copy.wait()


def update_weights(n_data, arrays, learn_rate, max_norm):
    width, ff_width = arrays[6].shape
    half_rows = arrays[11].shape[1] // 2
    up_rows, dn_cols = arrays[0].shape[0], arrays[1].shape[1]
    f32, bf16 = jnp.float32, jnp.bfloat16
    up_state, dn_state = jax.ShapeDtypeStruct((up_rows, ff_width), f32), jax.ShapeDtypeStruct((width, dn_cols), f32)
    any_spec = pl.BlockSpec(memory_space=pl.ANY)
    smem_spec = pl.BlockSpec(memory_space=pltpu.SMEM)

    def body(*refs):
        update_kernel(n_data, *refs)

    return pl.pallas_call(
        body,
        in_specs=[any_spec] * 12 + [smem_spec] * 2,
        out_specs=[any_spec] * 8,
        out_shape=[up_state, dn_state, up_state, up_state, dn_state, dn_state,
                   jax.ShapeDtypeStruct((2, ff_width, width), bf16), jax.ShapeDtypeStruct((2, width, ff_width), bf16)],
        scratch_shapes=[
            pltpu.VMEM((2, 2, width, ff_width), bf16), pltpu.VMEM((2, width, half_rows), bf16),
            pltpu.VMEM((half_rows, width), bf16), pltpu.VMEM((width, half_rows), bf16), pltpu.VMEM((half_rows, width), bf16),
            pltpu.VMEM((half_rows, ff_width), bf16), pltpu.VMEM((2, 2, width, ff_width), f32), pltpu.VMEM((2, width, ff_width), f32),
            pltpu.VMEM((2, up_rows, ff_width), f32), pltpu.VMEM((2, width, dn_cols), f32),
            pltpu.VMEM((up_rows, ff_width), f32), pltpu.VMEM((width, dn_cols), f32),
            pltpu.VMEM((3, up_rows, ff_width), f32), pltpu.VMEM((3, width, dn_cols), f32), pltpu.VMEM((2 * n_data, 8, 128), f32),
            pltpu.VMEM((ff_width, width), bf16),
            pltpu.SemaphoreType.DMA((36,)), pltpu.SemaphoreType.DMA((36,)), pltpu.SemaphoreType.DMA((12,)),
            pltpu.SemaphoreType.DMA((10,))],
        compiler_params=pltpu.CompilerParams(collective_id=0, has_side_effects=True, vmem_limit_bytes=67000000),
        cost_estimate=pl.CostEstimate(flops=20 * half_rows * width * ff_width, bytes_accessed=40000000, transcendentals=0),
        name="update",
    )(*arrays, learn_rate.reshape(1), max_norm.reshape(1))


def solution(mesh):
    n_data = mesh.shape['data']

    def step_body(master_up, master_down, moment1_up, moment2_up, moment1_down, moment2_down,
                  compute_up, compute_down, accum_up, accum_down, stage_acts, loss_grad, next_micro,
                  learn_rate, max_norm):
        arrays = (master_up[0], master_down[0].T, moment1_up[0], moment2_up[0], moment1_down[0].T, moment2_down[0].T,
                  compute_up[0], compute_down[0].T, accum_up[0, 0], accum_down[0, 0].T, stage_acts[0].T, loss_grad.T)
        new_up, new_dn, out1_up, out2_up, out1_dn, out2_dn, w_up_t, w_dn_t = update_weights(n_data, arrays, learn_rate, max_norm)
        last_acts = forward_all(next_micro, w_up_t, w_dn_t)
        return (new_up[None], new_dn.T[None], out1_up[None], out2_up[None], out1_dn.T[None], out2_dn.T[None], last_acts)

    shard_spec = P('stage', 'data', None)
    whole_spec = P('stage', None, None)
    accum_spec = P('data', 'stage', None, None)
    micro_spec = P(None, 'data', None)
    in_specs = (shard_spec,) * 6 + (whole_spec, whole_spec, accum_spec, accum_spec,
                                    P('stage', 'data', None), P('data', None), micro_spec, P(), P())
    out_specs = (shard_spec,) * 6 + (micro_spec,)
    return jax.shard_map(step_body, mesh=mesh, in_specs=in_specs, out_specs=out_specs, check_vma=False)
```

```python
import jax
import jax.numpy as jnp
from jax import lax
from jax.experimental import pallas as pl
from jax.experimental.pallas import tpu as pltpu
from jax.sharding import PartitionSpec as P

BETA_ONE = 0.9
BETA_TWO = 0.95
ADAM_EPS = 1e-8
WEIGHT_DECAY = 0.1
NORM_EPS = 1e-6
STEP_NUM = 10
BIAS_ONE = 1.0 - BETA_ONE ** STEP_NUM
BIAS_TWO = 1.0 - BETA_TWO ** STEP_NUM


def adamw_update(master, moment_one, moment_two, grad_step, learn_rate):
    mom_one = BETA_ONE * moment_one + (1.0 - BETA_ONE) * grad_step
    mom_two = BETA_TWO * moment_two + (1.0 - BETA_TWO) * grad_step * grad_step
    step_dir = (mom_one / BIAS_ONE) / (jnp.sqrt(mom_two / BIAS_TWO) + ADAM_EPS)
    new_master = master - learn_rate * (step_dir + WEIGHT_DECAY * master)
    return new_master, mom_one, mom_two


MESH_ID = pl.DeviceIdType.MESH
GRAD_HALF = 768
GRAD_TILE = 256
GELU_LIN = 0.7978845608028654
GELU_CUB = GELU_LIN * 0.044715
ROW_TILE = 512
FF_TILE = 512
CHUNKS = (4, 1, 1)
N_FIRST = 2


def gelu_half(pre_act):
    inner = pre_act * (GELU_LIN + GELU_CUB * (pre_act * pre_act))
    half = 0.5 * pre_act
    return half + half * jnp.tanh(inner)


def block_forward(cols_in, w_up_t, w_down_t, block, hidden_ref):
    ff_width = w_up_t.shape[1]
    for start in range(0, ff_width, FF_TILE):
        pre_act = jnp.dot(w_up_t[block, start:start + FF_TILE, :], cols_in, preferred_element_type=jnp.float32)
        hidden_ref[start:start + FF_TILE, :] = gelu_half(pre_act).astype(jnp.bfloat16)
    branch = jnp.dot(w_down_t[block], hidden_ref[...], preferred_element_type=jnp.float32)
    return (cols_in.astype(jnp.float32) + branch).astype(jnp.bfloat16)


def forward_kernel(has_prev, copies, n_state, base, n_own, n_tiles, *refs):
    refs = list(refs)
    x_ref, w_up_t, w_down_t = refs[:3]
    refs = refs[3:]
    n_copy = len(copies)
    copy_refs, refs = refs[:n_copy], refs[n_copy:]
    state_in, refs = refs[:n_state], refs[n_state:]
    if has_prev:
        refs.pop(0)
    out_ref, y_ref = refs[:2]
    state_out, refs = refs[2:2 + n_state], refs[2 + n_state:]
    hidden_ref, y_buf, y_sem, copy_sem, state_sem = refs[:5]
    state_buf = refs[5:]
    mine = lax.axis_index('stage')
    micro, tile = pl.program_id(0), pl.program_id(1)
    step = micro * n_tiles + tile
    n_steps = pl.num_programs(0) * n_tiles
    slot = lax.rem(step, 2)
    tile_cols = pl.ds(pl.multiple_of(tile * ROW_TILE, ROW_TILE), ROW_TILE)

    def y_copy(which):
        return pltpu.make_async_copy(y_buf.at[which], out_ref.at[mine * n_own + base + micro, :, tile_cols], y_sem.at[which])

    def tile_copy(index):
        from_peer, first, count = copies[index]
        owner = 1 - mine if from_peer else mine
        return pltpu.make_async_copy(copy_refs[index], out_ref.at[pl.ds(owner * n_own + first, count), :, tile_cols], copy_sem.at[index])

    def state_copy(index, leaving):
        src, dst = (state_buf[index], state_out[index]) if leaving else (state_in[index], state_buf[index])
        return pltpu.make_async_copy(src, dst, state_sem.at[index])

    if n_copy:
        @pl.when(micro == 0)
        def _():
            for index in range(n_copy):
                tile_copy(index).start()

    if n_state:
        @pl.when(step == 0)
        def _():
            for index in range(n_state):
                state_copy(index, False).start()

        @pl.when(step == 1)
        def _():
            for index in range(n_state):
                state_copy(index, False).wait()
                state_copy(index, True).start()

    cols = x_ref[0]
    for block in range(2):
        cols = block_forward(cols, w_up_t, w_down_t, block, hidden_ref)

    @pl.when(step >= 2)
    def _():
        y_copy(slot).wait()

    y_buf[slot] = cols
    y_ref[0] = cols
    y_copy(slot).start()
    if n_copy:
        @pl.when(micro == 0)
        def _():
            for index in range(n_copy):
                tile_copy(index).wait()

    @pl.when(step == n_steps - 1)
    def _():
        y_copy(slot).wait()
        y_copy(1 - slot).wait()
        for index in range(n_state):
            state_copy(index, True).wait()


def forward_chunk(base, n_chunk, micro_t, w_up_t, w_down_t, prev_out, copied, states):
    n_micro, width, n_rows = micro_t.shape
    n_own = n_micro // 2
    n_tiles = n_rows // ROW_TILE
    ff_width = w_up_t.shape[1]
    mine = lax.axis_index('stage')
    any_spec = pl.BlockSpec(memory_space=pl.ANY)
    scalar = jnp.full((1,), mine * n_own + base, jnp.int32)
    in_specs = [pl.BlockSpec((1, width, ROW_TILE), lambda i, j, first: (first[0] + i, 0, j)),
                pl.BlockSpec((2, ff_width, width), lambda i, j, first: (0, 0, 0)),
                pl.BlockSpec((2, width, ff_width), lambda i, j, first: (0, 0, 0))]
    operands = [micro_t, w_up_t, w_down_t]
    for array, _, _ in copied:
        in_specs.append(pl.BlockSpec((array.shape[0], width, ROW_TILE), lambda i, j, first: (0, 0, jnp.where(i == 0, j, n_tiles - 1))))
        operands.append(array)
    for array in states:
        in_specs.append(any_spec)
        operands.append(array)
    aliases = {}
    if prev_out is not None:
        in_specs.append(any_spec)
        operands.append(prev_out)
        aliases = {len(operands): 0}
    copies = [(from_peer, first, array.shape[0]) for array, from_peer, first in copied]

    def body(first, *refs):
        forward_kernel(prev_out is not None, copies, len(states), base, n_own, n_tiles, *refs)

    flops = 8 * n_chunk * n_rows * width * ff_width
    return pl.pallas_call(
        body,
        grid_spec=pltpu.PrefetchScalarGridSpec(
            num_scalar_prefetch=1, grid=(n_chunk, n_tiles), in_specs=in_specs,
            out_specs=[any_spec, pl.BlockSpec((1, width, ROW_TILE), lambda i, j, first: (i, 0, j))] + [any_spec] * len(states),
            scratch_shapes=[pltpu.VMEM((ff_width, ROW_TILE), jnp.bfloat16), pltpu.VMEM((2, width, ROW_TILE), jnp.bfloat16),
                            pltpu.SemaphoreType.DMA((2,)), pltpu.SemaphoreType.DMA((2,)), pltpu.SemaphoreType.DMA((6,))]
            + [pltpu.VMEM(array.shape, array.dtype) for array in states]),
        out_shape=[jax.ShapeDtypeStruct(micro_t.shape, jnp.bfloat16),
                   jax.ShapeDtypeStruct((n_chunk, width, n_rows), jnp.bfloat16)]
        + [jax.ShapeDtypeStruct(array.shape, array.dtype) for array in states],
        input_output_aliases=aliases,
        compiler_params=pltpu.CompilerParams(dimension_semantics=("arbitrary", "arbitrary"),
                                             vmem_limit_bytes=52 * 1024 * 1024),
        cost_estimate=pl.CostEstimate(flops=flops, bytes_accessed=4 * n_chunk * n_rows * width, transcendentals=0),
        name=f"fwd_{base}",
    )(scalar, *operands)


def forward_rest(micro_t, w_up_t, w_down_t, own_first, peer_first, states):
    n_own = micro_t.shape[0] // 2
    swap = [(0, 1), (1, 0)]
    mine = lax.axis_index('stage')
    out, base = None, own_first.shape[0]
    received, results = [], []
    for number, n_chunk in enumerate(CHUNKS):
        copied, passed = [], []
        if number == 0:
            copied, passed = [(own_first, False, 0), (peer_first, True, 0)], states
        elif number >= 2:
            copied = [received[number - 2]]
            received[number - 2] = None
        out, part, *handed = forward_chunk(base, n_chunk, micro_t, w_up_t, w_down_t, out, copied, passed)
        results += handed
        received.append((lax.ppermute(part, 'stage', swap), True, base))
        base += n_chunk
    for item in received:
        if item is not None:
            out = lax.dynamic_update_slice(out, item[0], ((1 - mine) * n_own + item[2], 0, 0))
    return jnp.swapaxes(out, 1, 2), results


def gelu_pair(pre_act):
    square = pre_act * pre_act
    tanh_in = jnp.tanh(pre_act * (GELU_LIN + GELU_CUB * square))
    half = 0.5 * pre_act
    value = half + half * tanh_in
    slope = 0.5 + 0.5 * tanh_in + half * (1.0 - tanh_in * tanh_in) * (GELU_LIN + 3.0 * GELU_CUB * square)
    return value, slope


def update_kernel(n_data, mst_up, mst_dn, mo1_up, mo2_up, mo1_dn, mo2_dn, cmp_up, cmp_dn, acc_up, acc_dn, acts_in, grad_in,
                  micro_in, rate_ref, norm_ref,
                  new_up, new_dn, out1_up, out2_up, out1_dn, out2_dn, w_up_out, w_dn_out, own_first, peer_first,
                  wts, acts, acts_row, grad, grad_row, d_pre, sums, part, fwd_up, fwd_dn, last_up, last_dn,
                  norm_tiles, turned, hidden_ref, send_sem, recv_sem, load_sem, store_sem, tile_sem):
    chip = lax.axis_index('data')
    core = lax.axis_index('stage')
    peer = 1 - core
    pos_x, pos_y = lax.rem(chip, 2), chip // 2
    chip_x = pos_y * 2 + (1 - pos_x)
    chip_y = (1 - pos_y) * 2 + pos_x
    chip_d = 3 - chip
    me = chip * 2 + core
    n_dev = 2 * n_data
    half_rows = grad.shape[1]
    width, ff_width = wts.shape[2:]
    up_rows, dn_cols = last_up.shape[0], last_dn.shape[1]
    n_own = micro_in.shape[0] // 2
    n_tiles = micro_in.shape[2] // ROW_TILE
    n_sub = GRAD_HALF // GRAD_TILE
    halves = (1 - pos_y, pos_y)

    def cols_of(index, size):
        return pl.ds(pl.multiple_of(index * size, size), size)

    def rows_of(index):
        return pl.ds(pl.multiple_of(index * up_rows, 8), up_rows)

    def remote(src, dst, index, device):
        return pltpu.make_async_remote_copy(src_ref=src, dst_ref=dst, send_sem=send_sem.at[index], recv_sem=recv_sem.at[index],
                                            device_id=device, device_id_type=MESH_ID)

    to_peer, to_x, to_y = (chip, peer), (chip_x, core), (chip_y, core)

    loads = [pltpu.make_async_copy(src, dst, load_sem.at[index]) for index, (src, dst) in enumerate([
        (grad_in.at[:, cols_of(core, half_rows)], grad), (acts_in.at[:, cols_of(core, half_rows)], acts.at[core]),
        (cmp_up, wts.at[core, 0]), (cmp_dn, wts.at[core, 1]),
        (acc_up, sums.at[core, 0]), (acc_dn, sums.at[core, 1]),
        (mst_up, part.at[0, 0:up_rows]), (mo1_up, part.at[0, up_rows:2 * up_rows]), (mo2_up, part.at[0, 2 * up_rows:3 * up_rows]),
        (mst_dn, part.at[1, :, 0:dn_cols]), (mo1_dn, part.at[1, :, dn_cols:2 * dn_cols]),
        (mo2_dn, part.at[1, :, 2 * dn_cols:3 * dn_cols])])]
    for copy in loads[:6]:
        copy.start()

    barrier = pltpu.get_barrier_semaphore()
    for offset in range(1, n_dev):
        other = lax.rem(me + offset, n_dev)
        pl.semaphore_signal(barrier, inc=1, device_id=(other // 2, lax.rem(other, 2)), device_id_type=MESH_ID)
    pl.semaphore_wait(barrier, n_dev - 1)

    swap_acts = remote(acts_in.at[:, cols_of(peer, half_rows)], acts.at[core], 0, to_peer)
    swap_wts = [[remote((cmp_up, cmp_dn)[kind].at[:, cols_of(half, GRAD_HALF)], wts.at[core, kind, :, cols_of(half, GRAD_HALF)],
                        1 + order * 2 + kind, to_peer) for kind in range(2)] for order, half in enumerate(halves)]
    swap_acts.start()
    for order in range(2):
        for kind in range(2):
            swap_wts[order][kind].start()

    def part_copy(kind, order, tile):
        cols = cols_of(halves[order] * n_sub + tile, GRAD_TILE)
        return remote(sums.at[peer, kind, :, cols], part.at[kind, :, cols], 5 + (kind * 2 + order) * n_sub + tile, to_peer)

    up_first = [[remote(sums.at[core, 0, rows_of(row * 2 + 1 - pos_x), cols_of(half, GRAD_HALF)],
                        fwd_up.at[slot, :, cols_of(half, GRAD_HALF)], 17 + order * 2 + slot, to_x)
                 for slot, row in enumerate(halves)] for order, half in enumerate(halves)]
    dn_first = [remote(sums.at[core, 1, :, cols_of((1 - pos_y) * 2 + col, dn_cols)], fwd_dn.at[slot], 21 + slot, to_y)
                for slot, col in enumerate((1 - pos_x, pos_x))]
    up_next = [remote(sums.at[core, 0, rows_of(chip_y), cols_of(half, GRAD_HALF)], last_up.at[:, cols_of(half, GRAD_HALF)],
                      23 + order, to_y) for order, half in enumerate(halves)]
    dn_next = remote(sums.at[core, 1, :, cols_of(chip_x, dn_cols)], last_dn, 25, to_x)

    def add_up(index, order):
        cols = cols_of(halves[order], GRAD_HALF)
        sums[core, 0, rows_of(index), cols] += part[0, rows_of(index), cols]

    def add_dn(index):
        cols = cols_of(index, dn_cols)
        sums[core, 1, :, cols] += part[1, :, cols]

    def scatter_half(order):
        for kind in range(2):
            for tile in range(n_sub):
                part_copy(kind, order, tile).wait_recv()
        for slot in range(2):
            add_up((halves[slot]) * 2 + 1 - pos_x, order)
            up_first[order][slot].start()
            if order == 0:
                add_dn((1 - pos_y) * 2 + (1 - pos_x if slot == 0 else pos_x))
                dn_first[slot].start()
        add_up(chip_y, order)
        if order == 1:
            add_dn(chip_x)
            add_dn(chip)
        add_up(chip, order)

    loads[0].wait()
    for block in (1, 0):
        own = core == block

        @pl.when(own)
        def _():
            for copy in loads[1:6]:
                copy.wait()

        @pl.when(jnp.logical_not(own))
        def _():
            swap_acts.wait_recv()

        acts_row[...] = acts[block].T
        grad_row[...] = grad[...].T
        for order in range(2):
            @pl.when(jnp.logical_not(own))
            def _(order=order):
                for copy in swap_wts[order]:
                    copy.wait_recv()

            def tile_step(tile, carry, block=block, own=own, order=order):
                cols = cols_of(halves[order] * n_sub + tile, GRAD_TILE)
                pre_act = jnp.dot(acts_row[...], wts[block, 0, :, cols], preferred_element_type=jnp.float32)
                d_hidden = jnp.dot(grad_row[...], wts[block, 1, :, cols], preferred_element_type=jnp.float32)
                hidden, slope = gelu_pair(pre_act)
                dw_down = jnp.dot(grad[...], hidden.astype(jnp.bfloat16), preferred_element_type=jnp.float32)
                d_tile = (d_hidden * slope).astype(jnp.bfloat16)
                if block == 1:
                    d_pre[:, cols] = d_tile
                dw_up = jnp.dot(acts[block], d_tile, preferred_element_type=jnp.float32)

                @pl.when(own)
                def _():
                    sums[block, 0, :, cols] += dw_up
                    sums[block, 1, :, cols] += dw_down

                @pl.when(jnp.logical_not(own))
                def _():
                    sums[block, 0, :, cols] = dw_up
                    sums[block, 1, :, cols] = dw_down
                    part_copy(0, order, tile).start()
                    part_copy(1, order, tile).start()
                return carry

            lax.fori_loop(0, n_sub, tile_step, 0)
            if block == 0 and order == 0:
                pl.when(core == 1)(lambda: scatter_half(1))
        if block == 1:
            d_in = lax.dot_general(wts[1, 0], d_pre[...], (((1,), (1,)), ((), ())), preferred_element_type=jnp.float32)
            grad[...] = (grad[...].astype(jnp.float32) + d_in).astype(jnp.bfloat16)
            pl.when(core == 1)(lambda: scatter_half(0))

    @pl.when(core == 0)
    def _():
        scatter_half(0)
        scatter_half(1)

    for copy in loads[6:]:
        copy.start()

    def x_slot(tile):
        slot = lax.rem(tile, 4)
        return acts.at[slot // 2, :, cols_of(lax.rem(slot, 2), ROW_TILE)]

    def x_load(tile):
        return pltpu.make_async_copy(micro_in.at[core * n_own + tile // n_tiles, :, cols_of(lax.rem(tile, n_tiles), ROW_TILE)],
                                     x_slot(tile), tile_sem.at[0, lax.rem(tile, 4)])

    for tile in range(4):
        x_load(tile).start()

    up_first[0][0].wait_recv()
    cols = cols_of(halves[0], GRAD_HALF)
    sums[core, 0, rows_of(chip_y), cols] += fwd_up[0, :, cols]
    up_next[0].start()
    dn_first[0].wait_recv()
    sums[core, 1, :, cols_of(chip_x, dn_cols)] += fwd_dn[0]
    dn_next.start()
    up_first[1][0].wait_recv()
    cols = cols_of(halves[1], GRAD_HALF)
    sums[core, 0, rows_of(chip_y), cols] += fwd_up[0, :, cols]
    up_next[1].start()
    for order in range(2):
        up_first[order][1].wait_recv()
        up_next[order].wait_recv()
    dn_first[1].wait_recv()
    scale = 1.0 / n_data
    mean_up = (sums[core, 0, rows_of(chip)] + fwd_up[1] + last_up[...]) * scale
    last_up[...] = mean_up
    square = jnp.sum((mean_up * mean_up).reshape(up_rows // 8, 8, ff_width), axis=0)
    dn_next.wait_recv()
    mean_dn = (sums[core, 1, :, cols_of(chip, dn_cols)] + fwd_dn[1] + last_dn[...]) * scale
    last_dn[...] = mean_dn
    square_dn = jnp.sum((mean_dn * mean_dn).reshape(width // 8, 8, dn_cols), axis=0)
    tile_sum = sum(square[:, first:first + 128] for first in range(0, ff_width, 128))
    tile_sum = tile_sum + sum(square_dn[:, first:first + 128] for first in range(0, dn_cols, 128))
    norm_tiles[me] = tile_sum
    norm_copies = []
    for offset in range(1, n_dev):
        other = lax.rem(me + offset, n_dev)
        norm_copies.append(remote(norm_tiles.at[me], norm_tiles.at[me], 25 + offset, (other // 2, lax.rem(other, 2))))
    for copy in norm_copies:
        copy.start()
    for copy in loads[6:]:
        copy.wait()
    for copy in norm_copies:
        copy.wait_recv()
    total_sq = jnp.sum(jnp.sum(norm_tiles[...], axis=0), keepdims=True)
    clip = jnp.minimum(1.0, norm_ref[0] / (jnp.sqrt(total_sq) + NORM_EPS))
    rate = rate_ref[0]

    chips = (chip, chip_x, chip_y, chip_d)
    up_at = [wts.at[core, 0, rows_of(index)] for index in chips]
    dn_at = [wts.at[core, 1, :, cols_of(index, dn_cols)] for index in chips]
    up_x, up_y, up_relay = remote(up_at[0], up_at[0], 33, to_x), remote(up_at[0], up_at[0], 34, to_y), remote(up_at[1], up_at[1], 35, to_y)
    dn_x, dn_y, dn_relay = remote(dn_at[0], dn_at[0], 36, to_x), remote(dn_at[0], dn_at[0], 37, to_y), remote(dn_at[2], dn_at[2], 38, to_x)
    up_peer = [remote(up_at[index], up_at[index], 39 + index, to_peer) for index in range(4)]
    dn_peer = [remote(dn_at[index], dn_at[index], 43 + index, to_peer) for index in range(4)]

    def gather_up():
        up_x.start()
        up_y.start()
        up_peer[0].start()

    def gather_dn():
        dn_y.start()
        dn_x.start()
        dn_peer[0].start()

    def gather_relay():
        up_x.wait_recv()
        up_relay.start()
        up_peer[1].start()
        dn_y.wait_recv()
        dn_relay.start()
        dn_peer[2].start()

    def gather_near():
        up_y.wait_recv()
        up_peer[2].start()
        dn_x.wait_recv()
        dn_peer[1].start()

    def gather_far():
        up_relay.wait_recv()
        up_peer[3].start()
        dn_relay.wait_recv()
        dn_peer[3].start()

    def gather_peer():
        for copy in up_peer + dn_peer:
            copy.wait_recv()

    state = adamw_update(part[0, 0:up_rows], part[0, up_rows:2 * up_rows], part[0, 2 * up_rows:3 * up_rows], clip * last_up[...], rate)
    wts[core, 0, rows_of(chip)] = state[0].astype(jnp.bfloat16)
    for index in range(3):
        part[0, index * up_rows:(index + 1) * up_rows] = state[index]
    pl.when(core == 0)(gather_up)
    state = adamw_update(part[1, :, 0:dn_cols], part[1, :, dn_cols:2 * dn_cols], part[1, :, 2 * dn_cols:3 * dn_cols], clip * last_dn[...], rate)
    wts[core, 1, :, cols_of(chip, dn_cols)] = state[0].astype(jnp.bfloat16)
    for index in range(3):
        part[1, :, index * dn_cols:(index + 1) * dn_cols] = state[index]
    pl.when(core == 0)(gather_dn)
    stores = [pltpu.make_async_copy(src, dst, store_sem.at[index]) for index, (src, dst) in enumerate([
        (part.at[0, 0:up_rows], new_up), (part.at[0, up_rows:2 * up_rows], out1_up), (part.at[0, 2 * up_rows:3 * up_rows], out2_up),
        (part.at[1, :, 0:dn_cols], new_dn), (part.at[1, :, dn_cols:2 * dn_cols], out1_dn),
        (part.at[1, :, 2 * dn_cols:3 * dn_cols], out2_dn)])]
    for copy in stores:
        copy.start()

    @pl.when(core == 0)
    def _():
        gather_relay()
        gather_near()
        gather_far()

    @pl.when(core == 1)
    def _():
        gather_peer()
        gather_up()
        gather_dn()

    swap_acts.wait_send()
    for order in range(2):
        for copy in swap_wts[order] + up_first[order] + [up_next[order]]:
            copy.wait_send()
        for kind in range(2):
            for tile in range(n_sub):
                part_copy(kind, order, tile).wait_send()
    for copy in dn_first + [dn_next] + norm_copies:
        copy.wait_send()

    def weights_out(block):
        return [pltpu.make_async_copy(turned, w_up_out.at[block], store_sem.at[6 + block]),
                pltpu.make_async_copy(wts.at[block, 1], w_dn_out.at[block], store_sem.at[8 + block])]

    def forward_tile(cols_in, block):
        for start in range(0, ff_width, FF_TILE):
            pre_act = jnp.dot(turned[start:start + FF_TILE, :], cols_in, preferred_element_type=jnp.float32)
            hidden_ref[start:start + FF_TILE, :] = gelu_half(pre_act).astype(jnp.bfloat16)
        branch = jnp.dot(wts[block, 1], hidden_ref[...], preferred_element_type=jnp.float32)
        return (cols_in.astype(jnp.float32) + branch).astype(jnp.bfloat16)

    n_first = own_first.shape[0] * n_tiles
    per_row = ff_width // ROW_TILE

    def mid_slot(tile):
        row = tile // per_row
        return row // 2, lax.rem(row, 2), slice(None), cols_of(lax.rem(tile, per_row), ROW_TILE)

    turned[...] = wts[0, 0].T
    for copy in weights_out(0):
        copy.start()

    def first_block(tile, carry):
        @pl.when(jnp.logical_and(core == 1, tile == 3))
        def _():
            gather_relay()

        @pl.when(jnp.logical_and(core == 1, tile == 5))
        def _():
            gather_near()

        @pl.when(jnp.logical_and(core == 1, tile == 7))
        def _():
            gather_far()

        x_load(tile).wait()
        slot = lax.rem(tile, 4)
        mid = forward_tile(acts[slot // 2, :, cols_of(lax.rem(slot, 2), ROW_TILE)], 0)
        sums[mid_slot(tile)] = mid.astype(jnp.float32)

        @pl.when(tile + 4 < n_first)
        def _():
            x_load(tile + 4).start()
        return carry

    lax.fori_loop(0, n_first, first_block, 0)
    pl.when(core == 0)(gather_peer)
    weights_out(0)[0].wait()
    turned[...] = wts[1, 0].T
    for copy in weights_out(1):
        copy.start()

    def y_slot(tile):
        return grad.at[:, cols_of(lax.rem(tile, 2), ROW_TILE)]

    def y_out(tile):
        place = (tile // n_tiles, slice(None), cols_of(lax.rem(tile, n_tiles), ROW_TILE))
        keep = pltpu.make_async_copy(y_slot(tile), own_first.at[place], tile_sem.at[1, lax.rem(tile, 2)])
        give = pltpu.make_async_remote_copy(src_ref=y_slot(tile), dst_ref=peer_first.at[place], send_sem=tile_sem.at[2, lax.rem(tile, 2)],
                                            recv_sem=recv_sem.at[47 + tile], device_id=to_peer, device_id_type=MESH_ID)
        return keep, give

    def second_block(tile, carry):
        result = forward_tile(sums[mid_slot(tile)].astype(jnp.bfloat16), 1)

        @pl.when(tile >= 2)
        def _():
            keep, give = y_out(tile - 2)
            keep.wait()
            give.wait_send()

        grad[:, cols_of(lax.rem(tile, 2), ROW_TILE)] = result
        for copy in y_out(tile):
            copy.start()
        return carry

    lax.fori_loop(0, n_first, second_block, 0)
    for tile in range(n_first - 2, n_first):
        keep, give = y_out(tile)
        keep.wait()
        give.wait_send()
    for tile in range(n_first):
        y_out(tile)[1].wait_recv()

    for copy in [up_x, up_y, up_relay, dn_x, dn_y, dn_relay] + up_peer + dn_peer:
        copy.wait_send()
    for copy in stores + weights_out(0)[1:] + weights_out(1):
        copy.wait()


def update_weights(n_data, arrays, learn_rate, max_norm):
    width, ff_width = arrays[6].shape
    n_rows = arrays[11].shape[1]
    half_rows = n_rows // 2
    up_rows, dn_cols = arrays[0].shape[0], arrays[1].shape[1]
    f32, bf16 = jnp.float32, jnp.bfloat16
    up_state, dn_state = jax.ShapeDtypeStruct((up_rows, ff_width), f32), jax.ShapeDtypeStruct((width, dn_cols), f32)
    first = jax.ShapeDtypeStruct((N_FIRST, width, n_rows), bf16)
    any_spec = pl.BlockSpec(memory_space=pl.ANY)
    smem_spec = pl.BlockSpec(memory_space=pltpu.SMEM)
    n_sem = 47 + N_FIRST * n_rows // ROW_TILE

    def body(*refs):
        update_kernel(n_data, *refs)

    flops = 20 * half_rows * width * ff_width + 8 * N_FIRST * n_rows * width * ff_width
    return pl.pallas_call(
        body,
        in_specs=[any_spec] * 13 + [smem_spec] * 2,
        out_specs=[any_spec] * 10,
        out_shape=[up_state, dn_state, up_state, up_state, dn_state, dn_state,
                   jax.ShapeDtypeStruct((2, ff_width, width), bf16), jax.ShapeDtypeStruct((2, width, ff_width), bf16), first, first],
        scratch_shapes=[
            pltpu.VMEM((2, 2, width, ff_width), bf16), pltpu.VMEM((2, width, half_rows), bf16),
            pltpu.VMEM((half_rows, width), bf16), pltpu.VMEM((width, half_rows), bf16), pltpu.VMEM((half_rows, width), bf16),
            pltpu.VMEM((half_rows, ff_width), bf16), pltpu.VMEM((2, 2, width, ff_width), f32), pltpu.VMEM((2, width, ff_width), f32),
            pltpu.VMEM((2, up_rows, ff_width), f32), pltpu.VMEM((2, width, dn_cols), f32),
            pltpu.VMEM((up_rows, ff_width), f32), pltpu.VMEM((width, dn_cols), f32), pltpu.VMEM((2 * n_data, 8, 128), f32),
            pltpu.VMEM((ff_width, width), bf16), pltpu.VMEM((ff_width, ROW_TILE), bf16),
            pltpu.SemaphoreType.DMA((n_sem,)), pltpu.SemaphoreType.DMA((n_sem,)), pltpu.SemaphoreType.DMA((12,)),
            pltpu.SemaphoreType.DMA((10,)), pltpu.SemaphoreType.DMA((3, 4))],
        compiler_params=pltpu.CompilerParams(collective_id=0, has_side_effects=True, vmem_limit_bytes=67000000),
        cost_estimate=pl.CostEstimate(flops=flops, bytes_accessed=60000000, transcendentals=0),
        name="update",
    )(*arrays, learn_rate.reshape(1), max_norm.reshape(1))


def solution(mesh):
    n_data = mesh.shape['data']

    def step_body(master_up, master_down, moment1_up, moment2_up, moment1_down, moment2_down,
                  compute_up, compute_down, accum_up, accum_down, stage_acts, loss_grad, next_micro,
                  learn_rate, max_norm):
        arrays = (master_up[0], master_down[0].T, moment1_up[0], moment2_up[0], moment1_down[0].T, moment2_down[0].T,
                  compute_up[0], compute_down[0].T, accum_up[0, 0], accum_down[0, 0].T, stage_acts[0].T, loss_grad.T,
                  jnp.swapaxes(next_micro, 1, 2))
        *states, w_up_t, w_dn_t, own_first, peer_first = update_weights(n_data, arrays, learn_rate, max_norm)
        last_acts, states = forward_rest(arrays[12], w_up_t, w_dn_t, own_first, peer_first, states)
        new_up, new_dn, out1_up, out2_up, out1_dn, out2_dn = states
        return (new_up[None], new_dn.T[None], out1_up[None], out2_up[None], out1_dn.T[None], out2_dn.T[None], last_acts)

    shard_spec = P('stage', 'data', None)
    whole_spec = P('stage', None, None)
    accum_spec = P('data', 'stage', None, None)
    micro_spec = P(None, 'data', None)
    in_specs = (shard_spec,) * 6 + (whole_spec, whole_spec, accum_spec, accum_spec,
                                    P('stage', 'data', None), P('data', None), micro_spec, P(), P())
    out_specs = (shard_spec,) * 6 + (micro_spec,)
    return jax.shard_map(step_body, mesh=mesh, in_specs=in_specs, out_specs=out_specs, check_vma=False)
```

```python
import functools

import jax
import jax.numpy as jnp
from jax import lax
from jax.experimental import pallas as pl
from jax.experimental.pallas import tpu as pltpu
from jax.sharding import PartitionSpec as P

BETA_ONE = 0.9
BETA_TWO = 0.95
ADAM_EPS = 1e-8
WEIGHT_DECAY = 0.1
NORM_EPS = 1e-6
STEP_NUM = 10
BIAS_ONE = 1.0 - BETA_ONE ** STEP_NUM
BIAS_TWO = 1.0 - BETA_TWO ** STEP_NUM


def adamw_update(master, moment_one, moment_two, grad_step, learn_rate):
    mom_one = BETA_ONE * moment_one + (1.0 - BETA_ONE) * grad_step
    mom_two = BETA_TWO * moment_two + (1.0 - BETA_TWO) * grad_step * grad_step
    step_dir = (mom_one / BIAS_ONE) / (jnp.sqrt(mom_two / BIAS_TWO) + ADAM_EPS)
    new_master = master - learn_rate * (step_dir + WEIGHT_DECAY * master)
    return new_master, mom_one, mom_two


MESH_ID = pl.DeviceIdType.MESH
GRAD_HALF = 768
GRAD_TILE = 256
GELU_LIN = 0.7978845608028654
GELU_CUB = GELU_LIN * 0.044715
ROW_TILE = 512
UNIT = 2 * ROW_TILE
FF_TILE = 512
CHUNKS = (7, 2, 1)
N_FIRST = 6


def gelu_half(pre_act):
    inner = pre_act * (GELU_LIN + GELU_CUB * (pre_act * pre_act))
    half = 0.5 * pre_act
    return half + half * jnp.tanh(inner)


def pair_forward(pair, up_rows_of, w_down, hidden_ref):
    ff_width = hidden_ref.shape[1]
    for half, cols_in in enumerate(pair):
        for start in range(0, ff_width, FF_TILE):
            pre_act = jnp.dot(up_rows_of(start), cols_in, preferred_element_type=jnp.float32)
            hidden_ref[half, start:start + FF_TILE, :] = gelu_half(pre_act).astype(jnp.bfloat16)
    results = []
    for half, cols_in in enumerate(pair):
        branch = jnp.dot(w_down, hidden_ref[half], preferred_element_type=jnp.float32)
        results.append((cols_in.astype(jnp.float32) + branch).astype(jnp.bfloat16))
    return results


def forward_kernel(is_short, has_prev, copies, n_state, base, n_own, *refs):
    refs = list(refs)
    x_ref, w_up_t, w_down_t = refs[:3]
    refs = refs[3:]
    n_copy = len(copies)
    copy_refs, refs = refs[:n_copy], refs[n_copy:]
    state_in, refs = refs[:n_state], refs[n_state:]
    if has_prev:
        refs.pop(0)
    out_ref, y_ref = refs[:2]
    state_out, refs = refs[2:2 + n_state], refs[2 + n_state:]
    hidden_ref, mid_ref, y_buf, y_sem, in_sem, out_sem, state_sem = refs[:7]
    copy_bufs, state_buf = refs[7:7 + n_copy], refs[7 + n_copy:]
    mine = lax.axis_index('stage')
    step, n_steps = pl.program_id(0), pl.num_programs(0)
    slot = lax.rem(step, 2)

    def out_at(owner, unit):
        return out_ref.at[owner * n_own + unit // 2, :, pl.ds(pl.multiple_of(lax.rem(unit, 2) * UNIT, UNIT), UNIT)]

    def y_copy(which):
        return pltpu.make_async_copy(y_buf.at[which], out_at(mine, base + step), y_sem.at[which])

    def enter(index):
        share = copies[index][3]
        return pltpu.make_async_copy(copy_refs[index].at[pl.ds(step * share, share)], copy_bufs[index], in_sem.at[index])

    def leave(index):
        from_peer, first, _, share = copies[index]
        owner = 1 - mine if from_peer else mine
        return [pltpu.make_async_copy(copy_bufs[index].at[unit], out_at(owner, first + step * share + unit), out_sem.at[index, unit])
                for unit in range(share)]

    def state_copy(index, leaving):
        src, dst = (state_buf[index], state_out[index]) if leaving else (state_in[index], state_buf[index])
        return pltpu.make_async_copy(src, dst, state_sem.at[index])

    def for_copies(action):
        for index in range(n_copy):
            pl.when(step * copies[index][3] < copies[index][2])(functools.partial(action, index))

    def leave_start(index):
        enter(index).wait()
        for copy in leave(index):
            copy.start()

    def leave_wait(index):
        for copy in leave(index):
            copy.wait()

    for_copies(lambda index: enter(index).start())
    if n_state:
        @pl.when(step == 0)
        def _():
            for index in range(n_state):
                state_copy(index, False).start()

        @pl.when(step == 1)
        def _():
            for index in range(n_state):
                state_copy(index, False).wait()
                state_copy(index, True).start()

    half_cols = UNIT // 2
    sides = (slice(0, half_cols), slice(half_cols, UNIT))
    pair = [x_ref[0, :, cols] for cols in sides]

    def block_step(block, carry):
        inputs = [mid_ref[:, cols] for cols in sides]
        results = pair_forward(inputs, lambda start: w_up_t[block, start:start + FF_TILE, :], w_down_t[block], hidden_ref)
        for half in range(2):
            mid_ref[:, sides[half]] = results[half]
        pl.when(block == 0)(lambda: for_copies(leave_start))
        return carry

    if is_short:
        mid_ref[...] = x_ref[0]
        lax.fori_loop(0, 2, block_step, 0)
        pair = [mid_ref[:, cols] for cols in sides]
    for block in range(0 if is_short else 2):
        pair = pair_forward(pair, lambda start, block=block: w_up_t[block, start:start + FF_TILE, :], w_down_t[block], hidden_ref)
        if block == 0:
            for_copies(leave_start)

    @pl.when(step >= 2)
    def _():
        y_copy(slot).wait()

    for half in range(2):
        cols = slice(half * half_cols, (half + 1) * half_cols)
        y_buf[slot, :, cols] = pair[half]
        y_ref[0, :, cols] = pair[half]
    y_copy(slot).start()
    for_copies(leave_wait)

    @pl.when(step == n_steps - 1)
    def _():
        y_copy(slot).wait()
        for index in range(n_state):
            state_copy(index, True).wait()

    @pl.when(jnp.logical_and(step == n_steps - 1, step >= 1))
    def _():
        y_copy(1 - slot).wait()


def forward_chunk(base, n_chunk, micro_t, w_up_t, w_down_t, prev_out, copied, states):
    n_micro, width, n_rows = micro_t.shape
    n_own = n_micro // 2
    ff_width = w_up_t.shape[1]
    mine = lax.axis_index('stage')
    any_spec = pl.BlockSpec(memory_space=pl.ANY)
    scalar = jnp.full((1,), mine * n_own, jnp.int32)
    in_specs = [pl.BlockSpec((1, width, UNIT), lambda i, first: (first[0] + (base + i) // 2, 0, lax.rem(base + i, 2))),
                pl.BlockSpec((2, ff_width, width), lambda i, first: (0, 0, 0)),
                pl.BlockSpec((2, width, ff_width), lambda i, first: (0, 0, 0))]
    operands = [micro_t, w_up_t, w_down_t] + [array for array, _, _ in copied] + list(states)
    in_specs += [any_spec] * (len(copied) + len(states))
    aliases = {}
    if prev_out is not None:
        in_specs.append(any_spec)
        operands.append(prev_out)
        aliases = {len(operands): 0}
    copies = [(from_peer, first, array.shape[0], pl.cdiv(array.shape[0], n_chunk)) for array, from_peer, first in copied]
    max_share = max([1] + [share for *_, share in copies])

    def body(first, *refs):
        forward_kernel(n_chunk <= 2, prev_out is not None, copies, len(states), base, n_own, *refs)

    flops = 8 * n_chunk * UNIT * width * ff_width
    return pl.pallas_call(
        body,
        grid_spec=pltpu.PrefetchScalarGridSpec(
            num_scalar_prefetch=1, grid=(n_chunk,), in_specs=in_specs,
            out_specs=[any_spec, pl.BlockSpec((1, width, UNIT), lambda i, first: (i, 0, 0))] + [any_spec] * len(states),
            scratch_shapes=[pltpu.VMEM((2, ff_width, UNIT // 2), jnp.bfloat16), pltpu.VMEM((width, UNIT), jnp.bfloat16),
                            pltpu.VMEM((2, width, UNIT), jnp.bfloat16),
                            pltpu.SemaphoreType.DMA((2,)), pltpu.SemaphoreType.DMA((2,)), pltpu.SemaphoreType.DMA((2, max_share)),
                            pltpu.SemaphoreType.DMA((6,))]
            + [pltpu.VMEM((share, width, UNIT), jnp.bfloat16) for *_, share in copies]
            + [pltpu.VMEM(array.shape, array.dtype) for array in states]),
        out_shape=[jax.ShapeDtypeStruct(micro_t.shape, jnp.bfloat16),
                   jax.ShapeDtypeStruct((n_chunk, width, UNIT), jnp.bfloat16)]
        + [jax.ShapeDtypeStruct(array.shape, array.dtype) for array in states],
        input_output_aliases=aliases,
        compiler_params=pltpu.CompilerParams(dimension_semantics=("arbitrary",), vmem_limit_bytes=50 * 1024 * 1024),
        cost_estimate=pl.CostEstimate(flops=flops, bytes_accessed=4 * n_chunk * UNIT * width, transcendentals=0),
        name=f"fwd_{base}",
    )(scalar, *operands)


def forward_rest(micro_t, w_up_t, w_down_t, own_first, peer_first, states):
    n_own = micro_t.shape[0] // 2
    swap = [(0, 1), (1, 0)]
    mine = lax.axis_index('stage')
    out, base = None, own_first.shape[0]
    received, results = [], []
    for number, n_chunk in enumerate(CHUNKS):
        copied, passed = [], []
        if number == 0:
            copied, passed = [(own_first, False, 0), (peer_first, True, 0)], states
        elif number >= 2:
            copied = [received[number - 2]]
            received[number - 2] = None
        out, part, *handed = forward_chunk(base, n_chunk, micro_t, w_up_t, w_down_t, out, copied, passed)
        results += handed
        received.append((lax.ppermute(part, 'stage', swap), True, base))
        base += n_chunk
    for item in received:
        if item is not None:
            for index in range(item[0].shape[0]):
                unit = item[2] + index
                out = lax.dynamic_update_slice(out, item[0][index:index + 1], ((1 - mine) * n_own + unit // 2, 0, unit % 2 * UNIT))
    return jnp.swapaxes(out, 1, 2), results


def gelu_pair(pre_act):
    square = pre_act * pre_act
    tanh_in = jnp.tanh(pre_act * (GELU_LIN + GELU_CUB * square))
    half = 0.5 * pre_act
    value = half + half * tanh_in
    slope = 0.5 + 0.5 * tanh_in + half * (1.0 - tanh_in * tanh_in) * (GELU_LIN + 3.0 * GELU_CUB * square)
    return value, slope


def update_kernel(n_data, mst_up, mst_dn, mo1_up, mo2_up, mo1_dn, mo2_dn, cmp_up, cmp_dn, acc_up, acc_dn, acts_in, grad_in,
                  micro_in, rate_ref, norm_ref,
                  new_up, new_dn, out1_up, out2_up, out1_dn, out2_dn, w_up_out, w_dn_out, own_first, peer_first,
                  wts, acts, acts_row, grad, grad_row, d_pre, sums, part, fwd_up, fwd_dn, last_up, last_dn,
                  norm_tiles, turned, hidden_ref, send_sem, recv_sem, load_sem, store_sem, tile_sem):
    chip = lax.axis_index('data')
    core = lax.axis_index('stage')
    peer = 1 - core
    pos_x, pos_y = lax.rem(chip, 2), chip // 2
    chip_x = pos_y * 2 + (1 - pos_x)
    chip_y = (1 - pos_y) * 2 + pos_x
    chip_d = 3 - chip
    me = chip * 2 + core
    n_dev = 2 * n_data
    half_rows = grad.shape[1]
    width, ff_width = wts.shape[2:]
    up_rows, dn_cols = last_up.shape[0], last_dn.shape[1]
    n_own = micro_in.shape[0] // 2
    n_sub = GRAD_HALF // GRAD_TILE
    halves = (1 - pos_y, pos_y)

    def cols_of(index, size):
        return pl.ds(pl.multiple_of(index * size, size), size)

    def rows_of(index):
        return pl.ds(pl.multiple_of(index * up_rows, 8), up_rows)

    def remote(src, dst, index, device):
        return pltpu.make_async_remote_copy(src_ref=src, dst_ref=dst, send_sem=send_sem.at[index], recv_sem=recv_sem.at[index],
                                            device_id=device, device_id_type=MESH_ID)

    to_peer, to_x, to_y = (chip, peer), (chip_x, core), (chip_y, core)

    loads = [pltpu.make_async_copy(src, dst, load_sem.at[index]) for index, (src, dst) in enumerate([
        (grad_in.at[:, cols_of(core, half_rows)], grad), (acts_in.at[:, cols_of(core, half_rows)], acts.at[core]),
        (cmp_up, wts.at[core, 0]), (cmp_dn, wts.at[core, 1]),
        (acc_up, sums.at[core, 0]), (acc_dn, sums.at[core, 1]),
        (mst_up, part.at[0, 0:up_rows]), (mo1_up, part.at[0, up_rows:2 * up_rows]), (mo2_up, part.at[0, 2 * up_rows:3 * up_rows]),
        (mst_dn, part.at[1, :, 0:dn_cols]), (mo1_dn, part.at[1, :, dn_cols:2 * dn_cols]),
        (mo2_dn, part.at[1, :, 2 * dn_cols:3 * dn_cols])])]
    for copy in loads[:6]:
        copy.start()

    barrier = pltpu.get_barrier_semaphore()
    for offset in range(1, n_dev):
        other = lax.rem(me + offset, n_dev)
        pl.semaphore_signal(barrier, inc=1, device_id=(other // 2, lax.rem(other, 2)), device_id_type=MESH_ID)
    pl.semaphore_wait(barrier, n_dev - 1)

    swap_acts = remote(acts_in.at[:, cols_of(peer, half_rows)], acts.at[core], 0, to_peer)
    def swap_piece(kind, tile):
        cols = cols_of(halves[0] * n_sub + tile, GRAD_TILE)
        return remote((cmp_up, cmp_dn)[kind].at[:, cols], wts.at[core, kind, :, cols], 1 + kind * n_sub + tile, to_peer)

    swap_late = [remote((cmp_up, cmp_dn)[kind].at[:, cols_of(halves[1], GRAD_HALF)], wts.at[core, kind, :, cols_of(halves[1], GRAD_HALF)],
                        1 + 2 * n_sub + kind, to_peer) for kind in range(2)]
    swap_acts.start()
    for tile in range(n_sub):
        for kind in range(2):
            swap_piece(kind, tile).start()
    for copy in swap_late:
        copy.start()

    def part_copy(kind, step):
        late = step // n_sub
        cols = cols_of((1 - pos_y + late * (2 * pos_y - 1)) * n_sub + lax.rem(step, n_sub), GRAD_TILE)
        return remote(sums.at[peer, kind, :, cols], part.at[kind, :, cols], 9 + kind * 2 * n_sub + step, to_peer)

    up_first = [[remote(sums.at[core, 0, rows_of(row * 2 + 1 - pos_x), cols_of(half, GRAD_HALF)],
                        fwd_up.at[slot, :, cols_of(half, GRAD_HALF)], 21 + order * 2 + slot, to_x)
                 for slot, row in enumerate(halves)] for order, half in enumerate(halves)]
    dn_first = [remote(sums.at[core, 1, :, cols_of((1 - pos_y) * 2 + col, dn_cols)], fwd_dn.at[slot], 25 + slot, to_y)
                for slot, col in enumerate((1 - pos_x, pos_x))]
    up_next = [remote(sums.at[core, 0, rows_of(chip_y), cols_of(half, GRAD_HALF)], last_up.at[:, cols_of(half, GRAD_HALF)],
                      27 + order, to_y) for order, half in enumerate(halves)]
    dn_next = remote(sums.at[core, 1, :, cols_of(chip_x, dn_cols)], last_dn, 29, to_x)

    def add_up(index, order):
        cols = cols_of(halves[order], GRAD_HALF)
        sums[core, 0, rows_of(index), cols] += part[0, rows_of(index), cols]

    def add_dn(index):
        cols = cols_of(index, dn_cols)
        sums[core, 1, :, cols] += part[1, :, cols]

    def scatter_half(order):
        for kind in range(2):
            for tile in range(n_sub):
                part_copy(kind, order * n_sub + tile).wait_recv()
        for slot in range(2):
            add_up((halves[slot]) * 2 + 1 - pos_x, order)
            up_first[order][slot].start()
            if order == 0:
                add_dn((1 - pos_y) * 2 + (1 - pos_x if slot == 0 else pos_x))
                dn_first[slot].start()
        add_up(chip_y, order)
        if order == 1:
            add_dn(chip_x)
            add_dn(chip)
        add_up(chip, order)

    loads[0].wait()
    for block in (1, 0):
        own = core == block

        @pl.when(own)
        def _():
            for copy in loads[1:4]:
                copy.wait()

        @pl.when(jnp.logical_not(own))
        def _():
            swap_acts.wait_recv()

        acts_row[...] = acts[block].T
        grad_row[...] = grad[...].T
        def tile_step(step, carry, block=block, own=own):
            late = step // n_sub
            cols = cols_of((1 - pos_y + late * (2 * pos_y - 1)) * n_sub + lax.rem(step, n_sub), GRAD_TILE)

            @pl.when(jnp.logical_and(jnp.logical_not(own), step < n_sub))
            def _():
                swap_piece(0, step).wait_recv()
                swap_piece(1, step).wait_recv()

            @pl.when(jnp.logical_and(jnp.logical_not(own), step == n_sub))
            def _():
                for copy in swap_late:
                    copy.wait_recv()

            half, at_step = (0, 2 * n_sub - 1) if block == 1 else (1, n_sub)
            pl.when(jnp.logical_and(core == 1, step == at_step))(functools.partial(scatter_half, half))

            pre_act = jnp.dot(acts_row[...], wts[block, 0, :, cols], preferred_element_type=jnp.float32)
            d_hidden = jnp.dot(grad_row[...], wts[block, 1, :, cols], preferred_element_type=jnp.float32)
            hidden, slope = gelu_pair(pre_act)
            dw_down = jnp.dot(grad[...], hidden.astype(jnp.bfloat16), preferred_element_type=jnp.float32)
            d_tile = (d_hidden * slope).astype(jnp.bfloat16)
            if block == 1:
                d_pre[:, cols] = d_tile
            dw_up = jnp.dot(acts[block], d_tile, preferred_element_type=jnp.float32)

            @pl.when(jnp.logical_and(own, step == 0))
            def _():
                for copy in loads[4:6]:
                    copy.wait()

            @pl.when(own)
            def _():
                sums[block, 0, :, cols] += dw_up
                sums[block, 1, :, cols] += dw_down

            @pl.when(jnp.logical_not(own))
            def _():
                sums[block, 0, :, cols] = dw_up
                sums[block, 1, :, cols] = dw_down
                part_copy(0, step).start()
                part_copy(1, step).start()
            return carry

        lax.fori_loop(0, 2 * n_sub, tile_step, 0)
        if block == 1:
            d_in = lax.dot_general(wts[1, 0], d_pre[...], (((1,), (1,)), ((), ())), preferred_element_type=jnp.float32)
            grad[...] = (grad[...].astype(jnp.float32) + d_in).astype(jnp.bfloat16)

    @pl.when(core == 0)
    def _():
        scatter_half(0)
        scatter_half(1)

    for copy in loads[6:]:
        copy.start()

    def x_load(pair):
        return pltpu.make_async_copy(micro_in.at[core * n_own + pair // 2, :, cols_of(lax.rem(pair, 2), UNIT)],
                                     acts.at[lax.rem(pair, 2)], tile_sem.at[0, lax.rem(pair, 2)])

    for pair in range(2):
        x_load(pair).start()

    up_first[0][0].wait_recv()
    cols = cols_of(halves[0], GRAD_HALF)
    sums[core, 0, rows_of(chip_y), cols] += fwd_up[0, :, cols]
    up_next[0].start()
    dn_first[0].wait_recv()
    sums[core, 1, :, cols_of(chip_x, dn_cols)] += fwd_dn[0]
    dn_next.start()
    up_first[1][0].wait_recv()
    cols = cols_of(halves[1], GRAD_HALF)
    sums[core, 0, rows_of(chip_y), cols] += fwd_up[0, :, cols]
    up_next[1].start()
    for order in range(2):
        up_first[order][1].wait_recv()
        up_next[order].wait_recv()
    dn_first[1].wait_recv()
    scale = 1.0 / n_data
    mean_up = (sums[core, 0, rows_of(chip)] + fwd_up[1] + last_up[...]) * scale
    last_up[...] = mean_up
    square = jnp.sum((mean_up * mean_up).reshape(up_rows // 8, 8, ff_width), axis=0)
    dn_next.wait_recv()
    mean_dn = (sums[core, 1, :, cols_of(chip, dn_cols)] + fwd_dn[1] + last_dn[...]) * scale
    last_dn[...] = mean_dn
    square_dn = jnp.sum((mean_dn * mean_dn).reshape(width // 8, 8, dn_cols), axis=0)
    tile_sum = sum(square[:, first:first + 128] for first in range(0, ff_width, 128))
    tile_sum = tile_sum + sum(square_dn[:, first:first + 128] for first in range(0, dn_cols, 128))
    norm_tiles[me] = tile_sum
    norm_copies = []
    for offset in range(1, n_dev):
        other = lax.rem(me + offset, n_dev)
        norm_copies.append(remote(norm_tiles.at[me], norm_tiles.at[me], 29 + offset, (other // 2, lax.rem(other, 2))))
    for copy in norm_copies:
        copy.start()
    for copy in loads[6:]:
        copy.wait()
    for copy in norm_copies:
        copy.wait_recv()
    total_sq = jnp.sum(jnp.sum(norm_tiles[...], axis=0), keepdims=True)
    clip = jnp.minimum(1.0, norm_ref[0] / (jnp.sqrt(total_sq) + NORM_EPS))
    rate = rate_ref[0]

    chips = (chip, chip_x, chip_y, chip_d)
    up_at = [wts.at[core, 0, rows_of(index)] for index in chips]
    dn_at = [wts.at[core, 1, :, cols_of(index, dn_cols)] for index in chips]
    up_x, up_y, up_relay = remote(up_at[0], up_at[0], 37, to_x), remote(up_at[0], up_at[0], 38, to_y), remote(up_at[1], up_at[1], 39, to_y)
    dn_x, dn_y, dn_relay = remote(dn_at[0], dn_at[0], 40, to_x), remote(dn_at[0], dn_at[0], 41, to_y), remote(dn_at[2], dn_at[2], 42, to_x)
    up_peer = [remote(up_at[index], up_at[index], 43 + index, to_peer) for index in range(4)]
    dn_peer = [remote(dn_at[index], dn_at[index], 47 + index, to_peer) for index in range(4)]

    def gather_up():
        up_x.start()
        up_y.start()
        up_peer[0].start()

    def gather_dn():
        dn_y.start()
        dn_x.start()
        dn_peer[0].start()

    def gather_relay():
        up_x.wait_recv()
        up_relay.start()
        up_peer[1].start()
        dn_y.wait_recv()
        dn_relay.start()
        dn_peer[2].start()

    def gather_near():
        up_y.wait_recv()
        up_peer[2].start()
        dn_x.wait_recv()
        dn_peer[1].start()

    def gather_far():
        up_relay.wait_recv()
        up_peer[3].start()
        dn_relay.wait_recv()
        dn_peer[3].start()

    def gather_peer():
        for copy in up_peer + dn_peer:
            copy.wait_recv()

    state = adamw_update(part[0, 0:up_rows], part[0, up_rows:2 * up_rows], part[0, 2 * up_rows:3 * up_rows], clip * last_up[...], rate)
    wts[core, 0, rows_of(chip)] = state[0].astype(jnp.bfloat16)
    for index in range(3):
        part[0, index * up_rows:(index + 1) * up_rows] = state[index]
    pl.when(core == 0)(gather_up)
    state = adamw_update(part[1, :, 0:dn_cols], part[1, :, dn_cols:2 * dn_cols], part[1, :, 2 * dn_cols:3 * dn_cols], clip * last_dn[...], rate)
    wts[core, 1, :, cols_of(chip, dn_cols)] = state[0].astype(jnp.bfloat16)
    for index in range(3):
        part[1, :, index * dn_cols:(index + 1) * dn_cols] = state[index]
    pl.when(core == 0)(gather_dn)
    stores = [pltpu.make_async_copy(src, dst, store_sem.at[index]) for index, (src, dst) in enumerate([
        (part.at[0, 0:up_rows], new_up), (part.at[0, up_rows:2 * up_rows], out1_up), (part.at[0, 2 * up_rows:3 * up_rows], out2_up),
        (part.at[1, :, 0:dn_cols], new_dn), (part.at[1, :, dn_cols:2 * dn_cols], out1_dn),
        (part.at[1, :, 2 * dn_cols:3 * dn_cols], out2_dn)])]
    for copy in stores:
        copy.start()

    @pl.when(core == 0)
    def _():
        gather_relay()
        gather_near()
        gather_far()

    @pl.when(core == 1)
    def _():
        gather_peer()
        gather_up()
        gather_dn()

    swap_acts.wait_send()
    for order in range(2):
        for copy in up_first[order] + [up_next[order]]:
            copy.wait_send()
        for kind in range(2):
            for tile in range(n_sub):
                part_copy(kind, order * n_sub + tile).wait_send()
    for copy in dn_first + [dn_next] + norm_copies + swap_late + [swap_piece(kind, tile) for kind in range(2) for tile in range(n_sub)]:
        copy.wait_send()

    def weights_out(block):
        return [pltpu.make_async_copy(turned, w_up_out.at[block], store_sem.at[6 + block]),
                pltpu.make_async_copy(wts.at[block, 1], w_dn_out.at[block], store_sem.at[8 + block])]

    def unit_forward(pair, block):
        return pair_forward(pair, lambda start: turned[start:start + FF_TILE, :], wts[block, 1], hidden_ref)

    n_first = own_first.shape[0]
    per_row = ff_width // ROW_TILE
    sides = (slice(0, ROW_TILE), slice(ROW_TILE, UNIT))

    def mid_slot(tile):
        row = tile // per_row
        return row // 2, lax.rem(row, 2), slice(None), cols_of(lax.rem(tile, per_row), ROW_TILE)

    turned[...] = wts[0, 0].T
    for copy in weights_out(0):
        copy.start()

    def first_block(pair, carry):
        for number, action in ((2, gather_relay), (3, gather_near), (4, gather_far)):
            pl.when(jnp.logical_and(core == 1, pair == number))(action)
        x_load(pair).wait()
        slot = lax.rem(pair, 2)
        mids = unit_forward([acts[slot, :, cols] for cols in sides], 0)
        for half in range(2):
            sums[mid_slot(2 * pair + half)] = mids[half].astype(jnp.float32)

        @pl.when(pair + 2 < n_first)
        def _():
            x_load(pair + 2).start()
        return carry

    lax.fori_loop(0, n_first, first_block, 0)
    pl.when(core == 0)(gather_peer)
    weights_out(0)[0].wait()
    turned[...] = wts[1, 0].T
    for copy in weights_out(1):
        copy.start()

    def y_out(pair):
        keep = pltpu.make_async_copy(grad, own_first.at[pair], tile_sem.at[1, 0])
        give = pltpu.make_async_remote_copy(src_ref=grad, dst_ref=peer_first.at[pair], send_sem=tile_sem.at[1, 1],
                                            recv_sem=recv_sem.at[51 + pair], device_id=to_peer, device_id_type=MESH_ID)
        return keep, give

    def y_wait(pair):
        keep, give = y_out(pair)
        keep.wait()
        give.wait_send()

    def second_block(pair, carry):
        results = unit_forward([sums[mid_slot(2 * pair + half)].astype(jnp.bfloat16) for half in range(2)], 1)
        pl.when(pair >= 1)(lambda: y_wait(pair - 1))
        for half in range(2):
            grad[:, sides[half]] = results[half]
        for copy in y_out(pair):
            copy.start()
        return carry

    lax.fori_loop(0, n_first, second_block, 0)
    y_wait(n_first - 1)
    for pair in range(n_first):
        y_out(pair)[1].wait_recv()

    for copy in [up_x, up_y, up_relay, dn_x, dn_y, dn_relay] + up_peer + dn_peer:
        copy.wait_send()
    for copy in stores + weights_out(0)[1:] + weights_out(1):
        copy.wait()


def update_weights(n_data, arrays, learn_rate, max_norm):
    width, ff_width = arrays[6].shape
    n_rows = arrays[11].shape[1]
    half_rows = n_rows // 2
    up_rows, dn_cols = arrays[0].shape[0], arrays[1].shape[1]
    f32, bf16 = jnp.float32, jnp.bfloat16
    up_state, dn_state = jax.ShapeDtypeStruct((up_rows, ff_width), f32), jax.ShapeDtypeStruct((width, dn_cols), f32)
    first = jax.ShapeDtypeStruct((N_FIRST, width, UNIT), bf16)
    any_spec = pl.BlockSpec(memory_space=pl.ANY)
    smem_spec = pl.BlockSpec(memory_space=pltpu.SMEM)
    n_sem = 51 + N_FIRST

    def body(*refs):
        update_kernel(n_data, *refs)

    flops = 20 * half_rows * width * ff_width + 8 * N_FIRST * UNIT * width * ff_width
    return pl.pallas_call(
        body,
        in_specs=[any_spec] * 13 + [smem_spec] * 2,
        out_specs=[any_spec] * 10,
        out_shape=[up_state, dn_state, up_state, up_state, dn_state, dn_state,
                   jax.ShapeDtypeStruct((2, ff_width, width), bf16), jax.ShapeDtypeStruct((2, width, ff_width), bf16), first, first],
        scratch_shapes=[
            pltpu.VMEM((2, 2, width, ff_width), bf16), pltpu.VMEM((2, width, half_rows), bf16),
            pltpu.VMEM((half_rows, width), bf16), pltpu.VMEM((width, half_rows), bf16), pltpu.VMEM((half_rows, width), bf16),
            pltpu.VMEM((half_rows, ff_width), bf16), pltpu.VMEM((2, 2, width, ff_width), f32), pltpu.VMEM((2, width, ff_width), f32),
            pltpu.VMEM((2, up_rows, ff_width), f32), pltpu.VMEM((2, width, dn_cols), f32),
            pltpu.VMEM((up_rows, ff_width), f32), pltpu.VMEM((width, dn_cols), f32), pltpu.VMEM((2 * n_data, 8, 128), f32),
            pltpu.VMEM((ff_width, width), bf16), pltpu.VMEM((2, ff_width, ROW_TILE), bf16),
            pltpu.SemaphoreType.DMA((n_sem,)), pltpu.SemaphoreType.DMA((n_sem,)), pltpu.SemaphoreType.DMA((12,)),
            pltpu.SemaphoreType.DMA((10,)), pltpu.SemaphoreType.DMA((2, 2))],
        compiler_params=pltpu.CompilerParams(collective_id=0, has_side_effects=True, vmem_limit_bytes=67000000),
        cost_estimate=pl.CostEstimate(flops=flops, bytes_accessed=60000000, transcendentals=0),
        name="update",
    )(*arrays, learn_rate.reshape(1), max_norm.reshape(1))


def solution(mesh):
    n_data = mesh.shape['data']

    def step_body(master_up, master_down, moment1_up, moment2_up, moment1_down, moment2_down,
                  compute_up, compute_down, accum_up, accum_down, stage_acts, loss_grad, next_micro,
                  learn_rate, max_norm):
        arrays = (master_up[0], master_down[0].T, moment1_up[0], moment2_up[0], moment1_down[0].T, moment2_down[0].T,
                  compute_up[0], compute_down[0].T, accum_up[0, 0], accum_down[0, 0].T, stage_acts[0].T, loss_grad.T,
                  jnp.swapaxes(next_micro, 1, 2))
        *states, w_up_t, w_dn_t, own_first, peer_first = update_weights(n_data, arrays, learn_rate, max_norm)
        last_acts, states = forward_rest(arrays[12], w_up_t, w_dn_t, own_first, peer_first, states)
        new_up, new_dn, out1_up, out2_up, out1_dn, out2_dn = states
        return (new_up[None], new_dn.T[None], out1_up[None], out2_up[None], out1_dn.T[None], out2_dn.T[None], last_acts)

    shard_spec = P('stage', 'data', None)
    whole_spec = P('stage', None, None)
    accum_spec = P('data', 'stage', None, None)
    micro_spec = P(None, 'data', None)
    in_specs = (shard_spec,) * 6 + (whole_spec, whole_spec, accum_spec, accum_spec,
                                    P('stage', 'data', None), P('data', None), micro_spec, P(), P())
    out_specs = (shard_spec,) * 6 + (micro_spec,)
    return jax.shard_map(step_body, mesh=mesh, in_specs=in_specs, out_specs=out_specs, check_vma=False)
```

```python
import functools

import jax
import jax.numpy as jnp
from jax import lax
from jax.experimental import pallas as pl
from jax.experimental.pallas import tpu as pltpu
from jax.sharding import PartitionSpec as P

BETA_ONE = 0.9
BETA_TWO = 0.95
ADAM_EPS = 1e-8
WEIGHT_DECAY = 0.1
NORM_EPS = 1e-6
STEP_NUM = 10
BIAS_ONE = 1.0 - BETA_ONE ** STEP_NUM
BIAS_TWO = 1.0 - BETA_TWO ** STEP_NUM


def adamw_update(master, moment_one, moment_two, grad_step, learn_rate):
    mom_one = BETA_ONE * moment_one + (1.0 - BETA_ONE) * grad_step
    mom_two = BETA_TWO * moment_two + (1.0 - BETA_TWO) * grad_step * grad_step
    step_dir = (mom_one / BIAS_ONE) / (jnp.sqrt(mom_two / BIAS_TWO) + ADAM_EPS)
    new_master = master - learn_rate * (step_dir + WEIGHT_DECAY * master)
    return new_master, mom_one, mom_two


MESH_ID = pl.DeviceIdType.MESH
GRAD_HALF = 768
GRAD_TILE = 256
GELU_LIN = 0.7978845608028654
GELU_CUB = GELU_LIN * 0.044715
ROW_TILE = 512
FF_TILE = 512
CHUNKS = ((15, 768), (4, 1536), (1, 512))
N_FIRST = 12
VMEM_LIMIT = 67000000


def gelu_half(pre_act):
    inner = pre_act * (GELU_LIN + GELU_CUB * (pre_act * pre_act))
    half = 0.5 * pre_act
    return half + half * jnp.tanh(inner)


def tile_forward(cols_in, w_up_t, w_down_t, hidden_ref, ff_tile):
    for start in range(0, hidden_ref.shape[0], ff_tile):
        rows = pl.ds(start, ff_tile)
        pre_act = jnp.dot(w_up_t[rows, :], cols_in, preferred_element_type=jnp.float32)
        hidden_ref[rows, :] = gelu_half(pre_act).astype(jnp.bfloat16)
    branch = jnp.dot(w_down_t[...], hidden_ref[...], preferred_element_type=jnp.float32)
    return (cols_in.astype(jnp.float32) + branch).astype(jnp.bfloat16)


def tile_place(n_own, per_micro, owner, tile):
    return owner * n_own + tile // per_micro, slice(None), pl.ds(pl.multiple_of(lax.rem(tile, per_micro) * ROW_TILE, ROW_TILE), ROW_TILE)


def start_all(copies):
    for copy in copies:
        copy.start()


def wait_all(copies):
    for copy in copies:
        copy.wait()


def forward_kernel(has_prev, ff_tile, copies, n_state, base, n_own, per_micro, *refs):
    refs = list(refs)
    x_ref, w_up_in, w_dn_in = refs[:3]
    refs = refs[3:]
    n_copy = len(copies)
    copy_refs, refs = refs[:n_copy], refs[n_copy:]
    state_in, refs = refs[:n_state], refs[n_state:]
    if has_prev:
        refs.pop(0)
    out_ref, y_ref, refs = refs[0], refs[1], refs[2:]
    state_out, refs = refs[:n_state], refs[n_state:]
    w_up_t, w_dn_t, hidden_ref, y_buf, y_sem, wt_sem, in_sem, out_sem, state_sem, *refs = refs
    copy_bufs, state_buf = refs[:n_copy], refs[n_copy:]
    mine = lax.axis_index('stage')
    step, n_steps = pl.program_id(0), pl.num_programs(0)
    slot = lax.rem(step, 2)

    def y_copy(which):
        return pltpu.make_async_copy(y_buf.at[which], out_ref.at[tile_place(n_own, per_micro, mine, base + step)], y_sem.at[which])

    def enter(index):
        share = copies[index][3]
        return pltpu.make_async_copy(copy_refs[index].at[pl.ds(step * share, share)], copy_bufs[index], in_sem.at[index])

    def leave(index):
        from_peer, first, _, share = copies[index]
        owner = 1 - mine if from_peer else mine
        return [pltpu.make_async_copy(copy_bufs[index].at[tile], out_ref.at[tile_place(n_own, per_micro, owner, first + step * share + tile)],
                                      out_sem.at[index, tile]) for tile in range(share)]

    def weight_copies(block):
        return [pltpu.make_async_copy(src.at[block], dst.at[block], wt_sem.at[block, kind])
                for kind, (src, dst) in enumerate(((w_up_in, w_up_t), (w_dn_in, w_dn_t)))]

    def state_copies(leaving):
        pairs = zip(state_buf, state_out) if leaving else zip(state_in, state_buf)
        return [pltpu.make_async_copy(src, dst, state_sem.at[index]) for index, (src, dst) in enumerate(pairs)]

    def for_copies(action):
        for index in range(n_copy):
            pl.when(step * copies[index][3] < copies[index][2])(functools.partial(action, index))

    def leave_start(index):
        enter(index).wait()
        start_all(leave(index))

    @pl.when(step == 0)
    def _():
        start_all(weight_copies(0) + weight_copies(1) + state_copies(False))

    for_copies(lambda index: enter(index).start())
    cols = x_ref[0]
    for block in range(2):
        pl.when(step == 0)(lambda: wait_all(weight_copies(block)))
        cols = tile_forward(cols, w_up_t.at[block], w_dn_t.at[block], hidden_ref, ff_tile)
        if block == 0:
            for_copies(leave_start)

    pl.when(step >= 2)(lambda: y_copy(slot).wait())
    y_buf[slot] = cols
    y_ref[0] = cols
    y_copy(slot).start()
    for_copies(lambda index: wait_all(leave(index)))
    if n_state:
        @pl.when(step == 1)
        def _():
            wait_all(state_copies(False))
            start_all(state_copies(True))

    @pl.when(step == n_steps - 1)
    def _():
        y_copy(slot).wait()
        wait_all(state_copies(True))

    pl.when(jnp.logical_and(step == n_steps - 1, step >= 1))(lambda: y_copy(1 - slot).wait())


def forward_chunk(base, n_chunk, ff_tile, micro_t, w_up_t, w_down_t, prev_out, copied, states):
    n_micro, width, n_rows = micro_t.shape
    n_own, per_micro = n_micro // 2, n_rows // ROW_TILE
    ff_width = w_up_t.shape[1]
    any_spec = pl.BlockSpec(memory_space=pl.ANY)
    scalar = jnp.full((1,), lax.axis_index('stage') * n_own, jnp.int32)
    in_specs = [pl.BlockSpec((1, width, ROW_TILE), lambda i, first: (first[0] + (base + i) // per_micro, 0, lax.rem(base + i, per_micro)))]
    operands = [micro_t, w_up_t, w_down_t] + [array for array, _, _ in copied] + list(states)
    in_specs += [any_spec] * (len(operands) - 1)
    aliases = {}
    if prev_out is not None:
        in_specs.append(any_spec)
        operands.append(prev_out)
        aliases = {len(operands): 0}
    copies = [(from_peer, first, array.shape[0], pl.cdiv(array.shape[0], n_chunk)) for array, from_peer, first in copied]
    max_share = max([1] + [share for *_, share in copies])
    dma = pltpu.SemaphoreType.DMA

    def body(first, *refs):
        forward_kernel(prev_out is not None, ff_tile, copies, len(states), base, n_own, per_micro, *refs)

    return pl.pallas_call(
        body,
        grid_spec=pltpu.PrefetchScalarGridSpec(
            num_scalar_prefetch=1, grid=(n_chunk,), in_specs=in_specs,
            out_specs=[any_spec, pl.BlockSpec((1, width, ROW_TILE), lambda i, first: (i, 0, 0))] + [any_spec] * len(states),
            scratch_shapes=[pltpu.VMEM(w_up_t.shape, jnp.bfloat16), pltpu.VMEM(w_down_t.shape, jnp.bfloat16),
                            pltpu.VMEM((ff_width, ROW_TILE), jnp.bfloat16), pltpu.VMEM((2, width, ROW_TILE), jnp.bfloat16),
                            dma((2,)), dma((2, 2)), dma((2,)), dma((2, max_share)), dma((6,))]
            + [pltpu.VMEM((share, width, ROW_TILE), jnp.bfloat16) for *_, share in copies]
            + [pltpu.VMEM(array.shape, array.dtype) for array in states]),
        out_shape=[jax.ShapeDtypeStruct(micro_t.shape, jnp.bfloat16),
                   jax.ShapeDtypeStruct((n_chunk, width, ROW_TILE), jnp.bfloat16)]
        + [jax.ShapeDtypeStruct(array.shape, array.dtype) for array in states],
        input_output_aliases=aliases,
        compiler_params=pltpu.CompilerParams(dimension_semantics=("arbitrary",), vmem_limit_bytes=VMEM_LIMIT),
        cost_estimate=pl.CostEstimate(flops=8 * n_chunk * ROW_TILE * width * ff_width, bytes_accessed=n_chunk * ROW_TILE * width,
                                      transcendentals=0),
        name=f"fwd_{base}",
    )(scalar, *operands)


def place_tiles(out, tiles, first, n_own):
    count, per_micro = tiles.shape[0], out.shape[2] // ROW_TILE
    any_spec = pl.BlockSpec(memory_space=pl.ANY)

    def body(tiles_ref, old_ref, out_ref, buf, in_sem, out_sem):
        owner = 1 - lax.axis_index('stage')
        enter = [pltpu.make_async_copy(tiles_ref.at[tile], buf.at[tile], in_sem.at[tile]) for tile in range(count)]
        leave = [pltpu.make_async_copy(buf.at[tile], out_ref.at[tile_place(n_own, per_micro, owner, first + tile)], out_sem.at[tile])
                 for tile in range(count)]
        start_all(enter)
        for tile in range(count):
            enter[tile].wait()
            leave[tile].start()
        wait_all(leave)

    return pl.pallas_call(
        body, in_specs=[any_spec] * 2, out_specs=any_spec, out_shape=jax.ShapeDtypeStruct(out.shape, out.dtype),
        scratch_shapes=[pltpu.VMEM(tiles.shape, tiles.dtype), pltpu.SemaphoreType.DMA((count,)), pltpu.SemaphoreType.DMA((count,))],
        input_output_aliases={1: 0}, compiler_params=pltpu.CompilerParams(vmem_limit_bytes=VMEM_LIMIT), name=f"place_{first}")(tiles, out)


def forward_rest(micro_t, w_up_t, w_down_t, own_first, peer_first, states):
    n_own = micro_t.shape[0] // 2
    out, base = None, own_first.shape[0]
    received, results = [], []
    for number, (n_chunk, ff_tile) in enumerate(CHUNKS):
        copied, passed = [], []
        if number == 0:
            copied, passed = [(own_first, False, 0), (peer_first, True, 0)], states
        elif number >= 2:
            copied = [received.pop(0)]
        out, part, *handed = forward_chunk(base, n_chunk, ff_tile, micro_t, w_up_t, w_down_t, out, copied, passed)
        results += handed
        received.append((lax.ppermute(part, 'stage', [(0, 1), (1, 0)]), True, base))
        base += n_chunk
    for tiles, _, first in received:
        out = place_tiles(out, tiles, first, n_own)
    return jnp.swapaxes(out, 1, 2), results


def gelu_pair(pre_act):
    square = pre_act * pre_act
    tanh_in = jnp.tanh(pre_act * (GELU_LIN + GELU_CUB * square))
    half = 0.5 * pre_act
    value = half + half * tanh_in
    slope = 0.5 + 0.5 * tanh_in + half * (1.0 - tanh_in * tanh_in) * (GELU_LIN + 3.0 * GELU_CUB * square)
    return value, slope


def update_kernel(n_data, mst_up, mst_dn, mo1_up, mo2_up, mo1_dn, mo2_dn, cmp_up, cmp_dn, acc_up, acc_dn, acts_in, grad_in,
                  micro_in, rate_ref, norm_ref,
                  new_up, new_dn, out1_up, out2_up, out1_dn, out2_dn, w_up_out, w_dn_out, own_first, peer_first,
                  wts, acts, acts_row, grad, grad_row, d_pre, sums, part, fwd_up, fwd_dn, last_up, last_dn,
                  norm_tiles, turned, hidden_ref, send_sem, recv_sem, load_sem, store_sem, tile_sem):
    chip = lax.axis_index('data')
    core = lax.axis_index('stage')
    peer = 1 - core
    pos_x, pos_y = lax.rem(chip, 2), chip // 2
    chip_x = pos_y * 2 + (1 - pos_x)
    chip_y = (1 - pos_y) * 2 + pos_x
    chip_d = 3 - chip
    me = chip * 2 + core
    n_dev = 2 * n_data
    half_rows = grad.shape[1]
    width, ff_width = wts.shape[2:]
    up_rows, dn_cols = last_up.shape[0], last_dn.shape[1]
    n_own = micro_in.shape[0] // 2
    n_sub = GRAD_HALF // GRAD_TILE
    halves = (1 - pos_y, pos_y)

    def cols_of(index, size):
        return pl.ds(pl.multiple_of(index * size, size), size)

    def rows_of(index):
        return pl.ds(pl.multiple_of(index * up_rows, 8), up_rows)

    def remote(src, dst, index, device):
        return pltpu.make_async_remote_copy(src_ref=src, dst_ref=dst, send_sem=send_sem.at[index], recv_sem=recv_sem.at[index],
                                            device_id=device, device_id_type=MESH_ID)

    to_peer, to_x, to_y = (chip, peer), (chip_x, core), (chip_y, core)

    loads = [pltpu.make_async_copy(src, dst, load_sem.at[index]) for index, (src, dst) in enumerate([
        (grad_in.at[:, cols_of(core, half_rows)], grad), (acts_in.at[:, cols_of(core, half_rows)], acts.at[core]),
        (cmp_up, wts.at[core, 0]), (cmp_dn, wts.at[core, 1]),
        (acc_up, sums.at[core, 0]), (acc_dn, sums.at[core, 1]),
        (mst_up, part.at[0, 0:up_rows]), (mo1_up, part.at[0, up_rows:2 * up_rows]), (mo2_up, part.at[0, 2 * up_rows:3 * up_rows]),
        (mst_dn, part.at[1, :, 0:dn_cols]), (mo1_dn, part.at[1, :, dn_cols:2 * dn_cols]),
        (mo2_dn, part.at[1, :, 2 * dn_cols:3 * dn_cols])])]
    for copy in loads[:6]:
        copy.start()

    barrier = pltpu.get_barrier_semaphore()
    for offset in range(1, n_dev):
        other = lax.rem(me + offset, n_dev)
        pl.semaphore_signal(barrier, inc=1, device_id=(other // 2, lax.rem(other, 2)), device_id_type=MESH_ID)
    pl.semaphore_wait(barrier, n_dev - 1)

    swap_acts = remote(acts_in.at[:, cols_of(peer, half_rows)], acts.at[core], 0, to_peer)
    def swap_piece(kind, tile):
        cols = cols_of(halves[0] * n_sub + tile, GRAD_TILE)
        return remote((cmp_up, cmp_dn)[kind].at[:, cols], wts.at[core, kind, :, cols], 1 + kind * n_sub + tile, to_peer)

    swap_late = [remote((cmp_up, cmp_dn)[kind].at[:, cols_of(halves[1], GRAD_HALF)], wts.at[core, kind, :, cols_of(halves[1], GRAD_HALF)],
                        1 + 2 * n_sub + kind, to_peer) for kind in range(2)]
    swap_acts.start()
    for tile in range(n_sub):
        for kind in range(2):
            swap_piece(kind, tile).start()
    for copy in swap_late:
        copy.start()

    def part_copy(kind, step):
        late = step // n_sub
        cols = cols_of((1 - pos_y + late * (2 * pos_y - 1)) * n_sub + lax.rem(step, n_sub), GRAD_TILE)
        return remote(sums.at[peer, kind, :, cols], part.at[kind, :, cols], 9 + kind * 2 * n_sub + step, to_peer)

    up_first = [[remote(sums.at[core, 0, rows_of(row * 2 + 1 - pos_x), cols_of(half, GRAD_HALF)],
                        fwd_up.at[slot, :, cols_of(half, GRAD_HALF)], 21 + order * 2 + slot, to_x)
                 for slot, row in enumerate(halves)] for order, half in enumerate(halves)]
    dn_first = [remote(sums.at[core, 1, :, cols_of((1 - pos_y) * 2 + col, dn_cols)], fwd_dn.at[slot], 25 + slot, to_y)
                for slot, col in enumerate((1 - pos_x, pos_x))]
    up_next = [remote(sums.at[core, 0, rows_of(chip_y), cols_of(half, GRAD_HALF)], last_up.at[:, cols_of(half, GRAD_HALF)],
                      27 + order, to_y) for order, half in enumerate(halves)]
    dn_next = remote(sums.at[core, 1, :, cols_of(chip_x, dn_cols)], last_dn, 29, to_x)

    def add_up(index, order):
        cols = cols_of(halves[order], GRAD_HALF)
        sums[core, 0, rows_of(index), cols] += part[0, rows_of(index), cols]

    def add_dn(index):
        cols = cols_of(index, dn_cols)
        sums[core, 1, :, cols] += part[1, :, cols]

    def scatter_half(order):
        for kind in range(2):
            for tile in range(n_sub):
                part_copy(kind, order * n_sub + tile).wait_recv()
        for slot in range(2):
            add_up((halves[slot]) * 2 + 1 - pos_x, order)
            up_first[order][slot].start()
            if order == 0:
                add_dn((1 - pos_y) * 2 + (1 - pos_x if slot == 0 else pos_x))
                dn_first[slot].start()
        add_up(chip_y, order)
        if order == 1:
            add_dn(chip_x)
            add_dn(chip)
        add_up(chip, order)

    loads[0].wait()
    for block in (1, 0):
        own = core == block

        @pl.when(own)
        def _():
            for copy in loads[1:4]:
                copy.wait()

        @pl.when(jnp.logical_not(own))
        def _():
            swap_acts.wait_recv()

        acts_row[...] = acts[block].T
        grad_row[...] = grad[...].T
        def tile_step(step, carry, block=block, own=own):
            late = step // n_sub
            cols = cols_of((1 - pos_y + late * (2 * pos_y - 1)) * n_sub + lax.rem(step, n_sub), GRAD_TILE)

            @pl.when(jnp.logical_and(jnp.logical_not(own), step < n_sub))
            def _():
                swap_piece(0, step).wait_recv()
                swap_piece(1, step).wait_recv()

            @pl.when(jnp.logical_and(jnp.logical_not(own), step == n_sub))
            def _():
                for copy in swap_late:
                    copy.wait_recv()

            half, at_step = (0, 2 * n_sub - 1) if block == 1 else (1, n_sub)
            pl.when(jnp.logical_and(core == 1, step == at_step))(functools.partial(scatter_half, half))

            pre_act = jnp.dot(acts_row[...], wts[block, 0, :, cols], preferred_element_type=jnp.float32)
            d_hidden = jnp.dot(grad_row[...], wts[block, 1, :, cols], preferred_element_type=jnp.float32)
            hidden, slope = gelu_pair(pre_act)
            dw_down = jnp.dot(grad[...], hidden.astype(jnp.bfloat16), preferred_element_type=jnp.float32)
            d_tile = (d_hidden * slope).astype(jnp.bfloat16)
            if block == 1:
                d_pre[:, cols] = d_tile
            dw_up = jnp.dot(acts[block], d_tile, preferred_element_type=jnp.float32)

            @pl.when(jnp.logical_and(own, step == 0))
            def _():
                for copy in loads[4:6]:
                    copy.wait()

            @pl.when(own)
            def _():
                sums[block, 0, :, cols] += dw_up
                sums[block, 1, :, cols] += dw_down

            @pl.when(jnp.logical_not(own))
            def _():
                sums[block, 0, :, cols] = dw_up
                sums[block, 1, :, cols] = dw_down
                part_copy(0, step).start()
                part_copy(1, step).start()
            return carry

        lax.fori_loop(0, 2 * n_sub, tile_step, 0)
        if block == 1:
            d_in = lax.dot_general(wts[1, 0], d_pre[...], (((1,), (1,)), ((), ())), preferred_element_type=jnp.float32)
            grad[...] = (grad[...].astype(jnp.float32) + d_in).astype(jnp.bfloat16)

    @pl.when(core == 0)
    def _():
        scatter_half(0)
        scatter_half(1)

    for copy in loads[6:]:
        copy.start()

    n_slot = 2 * half_rows // ROW_TILE
    per_micro = micro_in.shape[2] // ROW_TILE

    def x_slot(tile):
        slot = lax.rem(tile, n_slot)
        return acts.at[slot // 2, :, cols_of(lax.rem(slot, 2), ROW_TILE)]

    def x_load(tile):
        return pltpu.make_async_copy(micro_in.at[tile_place(n_own, per_micro, core, tile)], x_slot(tile), tile_sem.at[0, lax.rem(tile, n_slot)])

    start_all([x_load(tile) for tile in range(n_slot)])

    up_first[0][0].wait_recv()
    cols = cols_of(halves[0], GRAD_HALF)
    sums[core, 0, rows_of(chip_y), cols] += fwd_up[0, :, cols]
    up_next[0].start()
    dn_first[0].wait_recv()
    sums[core, 1, :, cols_of(chip_x, dn_cols)] += fwd_dn[0]
    dn_next.start()
    up_first[1][0].wait_recv()
    cols = cols_of(halves[1], GRAD_HALF)
    sums[core, 0, rows_of(chip_y), cols] += fwd_up[0, :, cols]
    up_next[1].start()
    for order in range(2):
        up_first[order][1].wait_recv()
        up_next[order].wait_recv()
    dn_first[1].wait_recv()
    scale = 1.0 / n_data
    mean_up = (sums[core, 0, rows_of(chip)] + fwd_up[1] + last_up[...]) * scale
    last_up[...] = mean_up
    square = jnp.sum((mean_up * mean_up).reshape(up_rows // 8, 8, ff_width), axis=0)
    dn_next.wait_recv()
    mean_dn = (sums[core, 1, :, cols_of(chip, dn_cols)] + fwd_dn[1] + last_dn[...]) * scale
    last_dn[...] = mean_dn
    square_dn = jnp.sum((mean_dn * mean_dn).reshape(width // 8, 8, dn_cols), axis=0)
    tile_sum = sum(square[:, first:first + 128] for first in range(0, ff_width, 128))
    tile_sum = tile_sum + sum(square_dn[:, first:first + 128] for first in range(0, dn_cols, 128))
    norm_tiles[me] = tile_sum
    norm_copies = []
    for offset in range(1, n_dev):
        other = lax.rem(me + offset, n_dev)
        norm_copies.append(remote(norm_tiles.at[me], norm_tiles.at[me], 29 + offset, (other // 2, lax.rem(other, 2))))
    for copy in norm_copies:
        copy.start()
    for copy in loads[6:]:
        copy.wait()
    for copy in norm_copies:
        copy.wait_recv()
    total_sq = jnp.sum(jnp.sum(norm_tiles[...], axis=0), keepdims=True)
    clip = jnp.minimum(1.0, norm_ref[0] / (jnp.sqrt(total_sq) + NORM_EPS))
    rate = rate_ref[0]

    chips = (chip, chip_x, chip_y, chip_d)
    up_at = [wts.at[core, 0, rows_of(index)] for index in chips]
    dn_at = [wts.at[core, 1, :, cols_of(index, dn_cols)] for index in chips]
    up_x, up_y, up_relay = remote(up_at[0], up_at[0], 37, to_x), remote(up_at[0], up_at[0], 38, to_y), remote(up_at[1], up_at[1], 39, to_y)
    dn_x, dn_y, dn_relay = remote(dn_at[0], dn_at[0], 40, to_x), remote(dn_at[0], dn_at[0], 41, to_y), remote(dn_at[2], dn_at[2], 42, to_x)
    up_peer = [remote(up_at[index], up_at[index], 43 + index, to_peer) for index in range(4)]
    dn_peer = [remote(dn_at[index], dn_at[index], 47 + index, to_peer) for index in range(4)]

    def gather_up():
        up_x.start()
        up_y.start()
        up_peer[0].start()

    def gather_dn():
        dn_y.start()
        dn_x.start()
        dn_peer[0].start()

    def gather_relay():
        up_x.wait_recv()
        up_relay.start()
        up_peer[1].start()
        dn_y.wait_recv()
        dn_relay.start()
        dn_peer[2].start()

    def gather_near():
        up_y.wait_recv()
        up_peer[2].start()
        dn_x.wait_recv()
        dn_peer[1].start()

    def gather_far():
        up_relay.wait_recv()
        up_peer[3].start()
        dn_relay.wait_recv()
        dn_peer[3].start()

    def gather_peer():
        for copy in up_peer + dn_peer:
            copy.wait_recv()

    state = adamw_update(part[0, 0:up_rows], part[0, up_rows:2 * up_rows], part[0, 2 * up_rows:3 * up_rows], clip * last_up[...], rate)
    wts[core, 0, rows_of(chip)] = state[0].astype(jnp.bfloat16)
    for index in range(3):
        part[0, index * up_rows:(index + 1) * up_rows] = state[index]
    pl.when(core == 0)(gather_up)
    state = adamw_update(part[1, :, 0:dn_cols], part[1, :, dn_cols:2 * dn_cols], part[1, :, 2 * dn_cols:3 * dn_cols], clip * last_dn[...], rate)
    wts[core, 1, :, cols_of(chip, dn_cols)] = state[0].astype(jnp.bfloat16)
    for index in range(3):
        part[1, :, index * dn_cols:(index + 1) * dn_cols] = state[index]
    pl.when(core == 0)(gather_dn)
    stores = [pltpu.make_async_copy(src, dst, store_sem.at[index]) for index, (src, dst) in enumerate([
        (part.at[0, 0:up_rows], new_up), (part.at[0, up_rows:2 * up_rows], out1_up), (part.at[0, 2 * up_rows:3 * up_rows], out2_up),
        (part.at[1, :, 0:dn_cols], new_dn), (part.at[1, :, dn_cols:2 * dn_cols], out1_dn),
        (part.at[1, :, 2 * dn_cols:3 * dn_cols], out2_dn)])]
    for copy in stores:
        copy.start()

    @pl.when(core == 0)
    def _():
        gather_relay()
        gather_near()
        gather_far()

    @pl.when(core == 1)
    def _():
        gather_peer()
        gather_up()
        gather_dn()

    swap_acts.wait_send()
    for order in range(2):
        for copy in up_first[order] + [up_next[order]]:
            copy.wait_send()
        for kind in range(2):
            for tile in range(n_sub):
                part_copy(kind, order * n_sub + tile).wait_send()
    for copy in dn_first + [dn_next] + norm_copies + swap_late + [swap_piece(kind, tile) for kind in range(2) for tile in range(n_sub)]:
        copy.wait_send()

    def weights_out(block):
        return [pltpu.make_async_copy(turned, w_up_out.at[block], store_sem.at[6 + block]),
                pltpu.make_async_copy(wts.at[block, 1], w_dn_out.at[block], store_sem.at[8 + block])]

    n_first = own_first.shape[0]
    per_row = ff_width // ROW_TILE

    def mid_slot(tile):
        row = tile // per_row
        return row // 2, lax.rem(row, 2), slice(None), cols_of(lax.rem(tile, per_row), ROW_TILE)

    turned[...] = wts[0, 0].T
    start_all(weights_out(0))

    def first_block(tile, carry):
        for number, action in ((4, gather_relay), (5, gather_near), (7, gather_far)):
            pl.when(jnp.logical_and(core == 1, tile == number))(action)
        x_load(tile).wait()
        mid = tile_forward(x_slot(tile)[...], turned, wts.at[0, 1], hidden_ref, FF_TILE)
        sums[mid_slot(tile)] = mid.astype(jnp.float32)
        pl.when(tile + n_slot < n_first)(lambda: x_load(tile + n_slot).start())
        return carry

    lax.fori_loop(0, n_first, first_block, 0)
    pl.when(core == 0)(gather_peer)
    weights_out(0)[0].wait()
    turned[...] = wts[1, 0].T
    start_all(weights_out(1))

    def y_out(tile):
        slot = lax.rem(tile, 2)
        y_slot = grad.at[:, cols_of(slot, ROW_TILE)]
        keep = pltpu.make_async_copy(y_slot, own_first.at[tile], tile_sem.at[1, slot])
        give = pltpu.make_async_remote_copy(src_ref=y_slot, dst_ref=peer_first.at[tile], send_sem=tile_sem.at[2, slot],
                                            recv_sem=recv_sem.at[51 + tile], device_id=to_peer, device_id_type=MESH_ID)
        return keep, give

    def y_wait(tile):
        keep, give = y_out(tile)
        keep.wait()
        give.wait_send()

    def second_block(tile, carry):
        result = tile_forward(sums[mid_slot(tile)].astype(jnp.bfloat16), turned, wts.at[1, 1], hidden_ref, FF_TILE)
        pl.when(tile >= 2)(lambda: y_wait(tile - 2))
        grad[:, cols_of(lax.rem(tile, 2), ROW_TILE)] = result
        start_all(y_out(tile))
        return carry

    lax.fori_loop(0, n_first, second_block, 0)
    y_wait(n_first - 2)
    y_wait(n_first - 1)
    for tile in range(n_first):
        y_out(tile)[1].wait_recv()

    for copy in [up_x, up_y, up_relay, dn_x, dn_y, dn_relay] + up_peer + dn_peer:
        copy.wait_send()
    for copy in stores + weights_out(0)[1:] + weights_out(1):
        copy.wait()


def update_weights(n_data, arrays, learn_rate, max_norm):
    width, ff_width = arrays[6].shape
    n_rows = arrays[11].shape[1]
    half_rows = n_rows // 2
    up_rows, dn_cols = arrays[0].shape[0], arrays[1].shape[1]
    f32, bf16 = jnp.float32, jnp.bfloat16
    up_state, dn_state = jax.ShapeDtypeStruct((up_rows, ff_width), f32), jax.ShapeDtypeStruct((width, dn_cols), f32)
    first = jax.ShapeDtypeStruct((N_FIRST, width, ROW_TILE), bf16)
    any_spec = pl.BlockSpec(memory_space=pl.ANY)
    smem_spec = pl.BlockSpec(memory_space=pltpu.SMEM)
    n_sem = 51 + N_FIRST

    def body(*refs):
        update_kernel(n_data, *refs)

    flops = 20 * half_rows * width * ff_width + 8 * N_FIRST * ROW_TILE * width * ff_width
    return pl.pallas_call(
        body,
        in_specs=[any_spec] * 13 + [smem_spec] * 2,
        out_specs=[any_spec] * 10,
        out_shape=[up_state, dn_state, up_state, up_state, dn_state, dn_state,
                   jax.ShapeDtypeStruct((2, ff_width, width), bf16), jax.ShapeDtypeStruct((2, width, ff_width), bf16), first, first],
        scratch_shapes=[
            pltpu.VMEM((2, 2, width, ff_width), bf16), pltpu.VMEM((2, width, half_rows), bf16),
            pltpu.VMEM((half_rows, width), bf16), pltpu.VMEM((width, half_rows), bf16), pltpu.VMEM((half_rows, width), bf16),
            pltpu.VMEM((half_rows, ff_width), bf16), pltpu.VMEM((2, 2, width, ff_width), f32), pltpu.VMEM((2, width, ff_width), f32),
            pltpu.VMEM((2, up_rows, ff_width), f32), pltpu.VMEM((2, width, dn_cols), f32),
            pltpu.VMEM((up_rows, ff_width), f32), pltpu.VMEM((width, dn_cols), f32), pltpu.VMEM((2 * n_data, 8, 128), f32),
            pltpu.VMEM((ff_width, width), bf16), pltpu.VMEM((ff_width, ROW_TILE), bf16),
            pltpu.SemaphoreType.DMA((n_sem,)), pltpu.SemaphoreType.DMA((n_sem,)), pltpu.SemaphoreType.DMA((12,)),
            pltpu.SemaphoreType.DMA((10,)), pltpu.SemaphoreType.DMA((3, 4))],
        compiler_params=pltpu.CompilerParams(collective_id=0, has_side_effects=True, vmem_limit_bytes=VMEM_LIMIT),
        cost_estimate=pl.CostEstimate(flops=flops, bytes_accessed=60000000, transcendentals=0),
        name="update",
    )(*arrays, learn_rate.reshape(1), max_norm.reshape(1))


def solution(mesh):
    n_data = mesh.shape['data']

    def step_body(master_up, master_down, moment1_up, moment2_up, moment1_down, moment2_down,
                  compute_up, compute_down, accum_up, accum_down, stage_acts, loss_grad, next_micro,
                  learn_rate, max_norm):
        arrays = (master_up[0], master_down[0].T, moment1_up[0], moment2_up[0], moment1_down[0].T, moment2_down[0].T,
                  compute_up[0], compute_down[0].T, accum_up[0, 0], accum_down[0, 0].T, stage_acts[0].T, loss_grad.T,
                  jnp.swapaxes(next_micro, 1, 2))
        *states, w_up_t, w_dn_t, own_first, peer_first = update_weights(n_data, arrays, learn_rate, max_norm)
        last_acts, states = forward_rest(arrays[12], w_up_t, w_dn_t, own_first, peer_first, states)
        new_up, new_dn, out1_up, out2_up, out1_dn, out2_dn = states
        return (new_up[None], new_dn.T[None], out1_up[None], out2_up[None], out1_dn.T[None], out2_dn.T[None], last_acts)

    shard_spec = P('stage', 'data', None)
    whole_spec = P('stage', None, None)
    accum_spec = P('data', 'stage', None, None)
    micro_spec = P(None, 'data', None)
    in_specs = (shard_spec,) * 6 + (whole_spec, whole_spec, accum_spec, accum_spec,
                                    P('stage', 'data', None), P('data', None), micro_spec, P(), P())
    out_specs = (shard_spec,) * 6 + (micro_spec,)
    return jax.shard_map(step_body, mesh=mesh, in_specs=in_specs, out_specs=out_specs, check_vma=False)
```

```python
import functools

import jax
import jax.numpy as jnp
from jax import lax
from jax.experimental import pallas as pl
from jax.experimental.pallas import tpu as pltpu
from jax.sharding import PartitionSpec as P

BETA_ONE = 0.9
BETA_TWO = 0.95
ADAM_EPS = 1e-8
WEIGHT_DECAY = 0.1
NORM_EPS = 1e-6
STEP_NUM = 10
BIAS_ONE = 1.0 - BETA_ONE ** STEP_NUM
BIAS_TWO = 1.0 - BETA_TWO ** STEP_NUM


def adamw_update(master, moment_one, moment_two, grad_step, learn_rate):
    mom_one = BETA_ONE * moment_one + (1.0 - BETA_ONE) * grad_step
    mom_two = BETA_TWO * moment_two + (1.0 - BETA_TWO) * grad_step * grad_step
    step_dir = (mom_one / BIAS_ONE) / (jnp.sqrt(mom_two / BIAS_TWO) + ADAM_EPS)
    new_master = master - learn_rate * (step_dir + WEIGHT_DECAY * master)
    return new_master, mom_one, mom_two


MESH_ID = pl.DeviceIdType.MESH
GRAD_HALF = 768
GRAD_TILE = 256
GELU_LIN = 0.7978845608028654
GELU_CUB = GELU_LIN * 0.044715
ROW_TILE = 512
FF_TILE = 256
CHUNKS = ((12, 256), (5, 128), (3, 384))
N_FIRST = 12
VMEM_LIMIT = 67000000


def gelu_half(pre_act):
    inner = pre_act * (GELU_LIN + GELU_CUB * (pre_act * pre_act))
    half = 0.5 * pre_act
    return half + half * jnp.tanh(inner)


def tile_forward(cols_in, w_up_t, w_down_t, hidden_ref, ff_tile):
    for start in range(0, hidden_ref.shape[0], ff_tile):
        rows = pl.ds(start, ff_tile)
        pre_act = jnp.dot(w_up_t[rows, :], cols_in, preferred_element_type=jnp.float32)
        hidden_ref[rows, :] = gelu_half(pre_act).astype(jnp.bfloat16)
    branch = jnp.dot(w_down_t[...], hidden_ref[...], preferred_element_type=jnp.float32)
    return (cols_in.astype(jnp.float32) + branch).astype(jnp.bfloat16)


def tile_place(n_own, per_micro, owner, tile):
    return owner * n_own + tile // per_micro, slice(None), pl.ds(pl.multiple_of(lax.rem(tile, per_micro) * ROW_TILE, ROW_TILE), ROW_TILE)


def start_all(copies):
    for copy in copies:
        copy.start()


def wait_all(copies):
    for copy in copies:
        copy.wait()


def forward_kernel(has_prev, ff_tile, copies, n_state, base, n_own, per_micro, *refs):
    refs = list(refs)
    x_ref, w_up_in, w_dn_in = refs[:3]
    refs = refs[3:]
    n_copy = len(copies)
    copy_refs, refs = refs[:n_copy], refs[n_copy:]
    state_in, refs = refs[:n_state], refs[n_state:]
    if has_prev:
        refs.pop(0)
    out_ref, y_ref, refs = refs[0], refs[1], refs[2:]
    state_out, refs = refs[:n_state], refs[n_state:]
    w_up_t, w_dn_t, hidden_ref, y_buf, y_sem, wt_sem, in_sem, out_sem, state_sem, *refs = refs
    copy_bufs, state_buf = refs[:n_copy], refs[n_copy:]
    mine = lax.axis_index('stage')
    step, n_steps = pl.program_id(0), pl.num_programs(0)
    slot = lax.rem(step, 2)

    def y_copy(which):
        return pltpu.make_async_copy(y_buf.at[which], out_ref.at[tile_place(n_own, per_micro, mine, base + step)], y_sem.at[which])

    def enter(index):
        share = copies[index][3]
        return pltpu.make_async_copy(copy_refs[index].at[pl.ds(step * share, share)], copy_bufs[index], in_sem.at[index])

    def leave(index):
        from_peer, first, _, share = copies[index]
        owner = 1 - mine if from_peer else mine
        return [pltpu.make_async_copy(copy_bufs[index].at[tile], out_ref.at[tile_place(n_own, per_micro, owner, first + step * share + tile)],
                                      out_sem.at[index, tile]) for tile in range(share)]

    def weight_copies(block):
        return [pltpu.make_async_copy(src.at[block], dst.at[block], wt_sem.at[block, kind])
                for kind, (src, dst) in enumerate(((w_up_in, w_up_t), (w_dn_in, w_dn_t)))]

    def state_copies(leaving):
        pairs = zip(state_buf, state_out) if leaving else zip(state_in, state_buf)
        return [pltpu.make_async_copy(src, dst, state_sem.at[index]) for index, (src, dst) in enumerate(pairs)]

    def for_copies(action):
        for index in range(n_copy):
            pl.when(step * copies[index][3] < copies[index][2])(functools.partial(action, index))

    def leave_start(index):
        enter(index).wait()
        start_all(leave(index))

    @pl.when(step == 0)
    def _():
        start_all(weight_copies(0) + weight_copies(1) + state_copies(False))

    for_copies(lambda index: enter(index).start())
    cols = x_ref[0]
    for block in range(2):
        pl.when(step == 0)(lambda: wait_all(weight_copies(block)))
        cols = tile_forward(cols, w_up_t.at[block], w_dn_t.at[block], hidden_ref, ff_tile)
        if block == 0:
            for_copies(leave_start)

    pl.when(step >= 2)(lambda: y_copy(slot).wait())
    y_buf[slot] = cols
    y_ref[0] = cols
    y_copy(slot).start()
    for_copies(lambda index: wait_all(leave(index)))
    if n_state:
        @pl.when(step == 1)
        def _():
            wait_all(state_copies(False))
            start_all(state_copies(True))

    @pl.when(step == n_steps - 1)
    def _():
        y_copy(slot).wait()
        wait_all(state_copies(True))

    pl.when(jnp.logical_and(step == n_steps - 1, step >= 1))(lambda: y_copy(1 - slot).wait())


def forward_chunk(base, n_chunk, ff_tile, micro_t, w_up_t, w_down_t, prev_out, copied, states):
    n_micro, width, n_rows = micro_t.shape
    n_own, per_micro = n_micro // 2, n_rows // ROW_TILE
    ff_width = w_up_t.shape[1]
    any_spec = pl.BlockSpec(memory_space=pl.ANY)
    scalar = jnp.full((1,), lax.axis_index('stage') * n_own, jnp.int32)
    in_specs = [pl.BlockSpec((1, width, ROW_TILE), lambda i, first: (first[0] + (base + i) // per_micro, 0, lax.rem(base + i, per_micro)))]
    operands = [micro_t, w_up_t, w_down_t] + [array for array, _, _ in copied] + list(states)
    in_specs += [any_spec] * (len(operands) - 1)
    aliases = {}
    if prev_out is not None:
        in_specs.append(any_spec)
        operands.append(prev_out)
        aliases = {len(operands): 0}
    copies = [(from_peer, first, array.shape[0], pl.cdiv(array.shape[0], n_chunk)) for array, from_peer, first in copied]
    max_share = max([1] + [share for *_, share in copies])
    dma = pltpu.SemaphoreType.DMA

    def body(first, *refs):
        forward_kernel(prev_out is not None, ff_tile, copies, len(states), base, n_own, per_micro, *refs)

    return pl.pallas_call(
        body,
        grid_spec=pltpu.PrefetchScalarGridSpec(
            num_scalar_prefetch=1, grid=(n_chunk,), in_specs=in_specs,
            out_specs=[any_spec, pl.BlockSpec((1, width, ROW_TILE), lambda i, first: (i, 0, 0))] + [any_spec] * len(states),
            scratch_shapes=[pltpu.VMEM(w_up_t.shape, jnp.bfloat16), pltpu.VMEM(w_down_t.shape, jnp.bfloat16),
                            pltpu.VMEM((ff_width, ROW_TILE), jnp.bfloat16), pltpu.VMEM((2, width, ROW_TILE), jnp.bfloat16),
                            dma((2,)), dma((2, 2)), dma((2,)), dma((2, max_share)), dma((6,))]
            + [pltpu.VMEM((share, width, ROW_TILE), jnp.bfloat16) for *_, share in copies]
            + [pltpu.VMEM(array.shape, array.dtype) for array in states]),
        out_shape=[jax.ShapeDtypeStruct(micro_t.shape, jnp.bfloat16),
                   jax.ShapeDtypeStruct((n_chunk, width, ROW_TILE), jnp.bfloat16)]
        + [jax.ShapeDtypeStruct(array.shape, array.dtype) for array in states],
        input_output_aliases=aliases,
        compiler_params=pltpu.CompilerParams(dimension_semantics=("arbitrary",), vmem_limit_bytes=VMEM_LIMIT),
        cost_estimate=pl.CostEstimate(flops=8 * n_chunk * ROW_TILE * width * ff_width, bytes_accessed=n_chunk * ROW_TILE * width,
                                      transcendentals=0),
        name=f"fwd_{base}",
    )(scalar, *operands)


def place_tiles(out, tiles, first, n_own):
    count, per_micro = tiles.shape[0], out.shape[2] // ROW_TILE
    any_spec = pl.BlockSpec(memory_space=pl.ANY)

    def body(tiles_ref, old_ref, out_ref, buf, in_sem, out_sem):
        owner = 1 - lax.axis_index('stage')
        enter = [pltpu.make_async_copy(tiles_ref.at[tile], buf.at[tile], in_sem.at[tile]) for tile in range(count)]
        leave = [pltpu.make_async_copy(buf.at[tile], out_ref.at[tile_place(n_own, per_micro, owner, first + tile)], out_sem.at[tile])
                 for tile in range(count)]
        start_all(enter)
        for tile in range(count):
            enter[tile].wait()
            leave[tile].start()
        wait_all(leave)

    return pl.pallas_call(
        body, in_specs=[any_spec] * 2, out_specs=any_spec, out_shape=jax.ShapeDtypeStruct(out.shape, out.dtype),
        scratch_shapes=[pltpu.VMEM(tiles.shape, tiles.dtype), pltpu.SemaphoreType.DMA((count,)), pltpu.SemaphoreType.DMA((count,))],
        input_output_aliases={1: 0}, compiler_params=pltpu.CompilerParams(vmem_limit_bytes=VMEM_LIMIT), name=f"place_{first}")(tiles, out)


def forward_rest(micro_t, w_up_t, w_down_t, own_first, peer_first, states):
    n_own = micro_t.shape[0] // 2
    out, base = None, own_first.shape[0]
    received, results = [], []
    for number, (n_chunk, ff_tile) in enumerate(CHUNKS):
        copied, passed = [], []
        if number == 0:
            copied, passed = [(own_first, False, 0), (peer_first, True, 0)], states
        elif number >= 2:
            copied = [received.pop(0)]
        out, part, *handed = forward_chunk(base, n_chunk, ff_tile, micro_t, w_up_t, w_down_t, out, copied, passed)
        results += handed
        received.append((lax.ppermute(part, 'stage', [(0, 1), (1, 0)]), True, base))
        base += n_chunk
    for tiles, _, first in received:
        out = place_tiles(out, tiles, first, n_own)
    return jnp.swapaxes(out, 1, 2), results


def gelu_pair(pre_act):
    square = pre_act * pre_act
    tanh_in = jnp.tanh(pre_act * (GELU_LIN + GELU_CUB * square))
    half = 0.5 * pre_act
    value = half + half * tanh_in
    slope = 0.5 + 0.5 * tanh_in + half * (1.0 - tanh_in * tanh_in) * (GELU_LIN + 3.0 * GELU_CUB * square)
    return value, slope


def update_kernel(n_data, mst_up, mst_dn, mo1_up, mo2_up, mo1_dn, mo2_dn, cmp_up, cmp_dn, acc_up, acc_dn, acts_in, grad_in,
                  micro_in, rate_ref, norm_ref,
                  new_up, new_dn, out1_up, out2_up, out1_dn, out2_dn, w_up_out, w_dn_out, own_first, peer_first,
                  wts, acts, acts_row, grad, grad_row, d_pre, sums, part, fwd_up, fwd_dn, last_up, last_dn,
                  norm_tiles, turned, hidden_ref, send_sem, recv_sem, load_sem, store_sem, tile_sem):
    chip = lax.axis_index('data')
    core = lax.axis_index('stage')
    peer = 1 - core
    pos_x, pos_y = lax.rem(chip, 2), chip // 2
    chip_x = pos_y * 2 + (1 - pos_x)
    chip_y = (1 - pos_y) * 2 + pos_x
    chip_d = 3 - chip
    me = chip * 2 + core
    n_dev = 2 * n_data
    half_rows = grad.shape[1]
    width, ff_width = wts.shape[2:]
    up_rows, dn_cols = last_up.shape[0], last_dn.shape[1]
    n_own = micro_in.shape[0] // 2
    n_sub = GRAD_HALF // GRAD_TILE
    halves = (1 - pos_y, pos_y)

    def cols_of(index, size):
        return pl.ds(pl.multiple_of(index * size, size), size)

    def rows_of(index):
        return pl.ds(pl.multiple_of(index * up_rows, 8), up_rows)

    def remote(src, dst, index, device):
        return pltpu.make_async_remote_copy(src_ref=src, dst_ref=dst, send_sem=send_sem.at[index], recv_sem=recv_sem.at[index],
                                            device_id=device, device_id_type=MESH_ID)

    to_peer, to_x, to_y = (chip, peer), (chip_x, core), (chip_y, core)

    loads = [pltpu.make_async_copy(src, dst, load_sem.at[index]) for index, (src, dst) in enumerate([
        (grad_in.at[:, cols_of(core, half_rows)], grad), (acts_in.at[:, cols_of(core, half_rows)], acts.at[core]),
        (cmp_up, wts.at[core, 0]), (cmp_dn, wts.at[core, 1]),
        (acc_up, sums.at[core, 0]), (acc_dn, sums.at[core, 1]),
        (mst_up, part.at[0, 0:up_rows]), (mo1_up, part.at[0, up_rows:2 * up_rows]), (mo2_up, part.at[0, 2 * up_rows:3 * up_rows]),
        (mst_dn, part.at[1, :, 0:dn_cols]), (mo1_dn, part.at[1, :, dn_cols:2 * dn_cols]),
        (mo2_dn, part.at[1, :, 2 * dn_cols:3 * dn_cols])])]
    for copy in loads[:6]:
        copy.start()

    barrier = pltpu.get_barrier_semaphore()
    for offset in range(1, n_dev):
        other = lax.rem(me + offset, n_dev)
        pl.semaphore_signal(barrier, inc=1, device_id=(other // 2, lax.rem(other, 2)), device_id_type=MESH_ID)
    pl.semaphore_wait(barrier, n_dev - 1)

    swap_acts = remote(acts_in.at[:, cols_of(peer, half_rows)], acts.at[core], 0, to_peer)
    def swap_piece(kind, tile):
        cols = cols_of(halves[0] * n_sub + tile, GRAD_TILE)
        return remote((cmp_up, cmp_dn)[kind].at[:, cols], wts.at[core, kind, :, cols], 1 + kind * n_sub + tile, to_peer)

    swap_late = [remote((cmp_up, cmp_dn)[kind].at[:, cols_of(halves[1], GRAD_HALF)], wts.at[core, kind, :, cols_of(halves[1], GRAD_HALF)],
                        1 + 2 * n_sub + kind, to_peer) for kind in range(2)]
    swap_acts.start()
    for tile in range(n_sub):
        for kind in range(2):
            swap_piece(kind, tile).start()
    for copy in swap_late:
        copy.start()

    def part_copy(kind, step):
        late = step // n_sub
        cols = cols_of((1 - pos_y + late * (2 * pos_y - 1)) * n_sub + lax.rem(step, n_sub), GRAD_TILE)
        return remote(sums.at[peer, kind, :, cols], part.at[kind, :, cols], 9 + kind * 2 * n_sub + step, to_peer)

    up_first = [[remote(sums.at[core, 0, rows_of(row * 2 + 1 - pos_x), cols_of(half, GRAD_HALF)],
                        fwd_up.at[slot, :, cols_of(half, GRAD_HALF)], 21 + order * 2 + slot, to_x)
                 for slot, row in enumerate(halves)] for order, half in enumerate(halves)]
    dn_first = [remote(sums.at[core, 1, :, cols_of((1 - pos_y) * 2 + col, dn_cols)], fwd_dn.at[slot], 25 + slot, to_y)
                for slot, col in enumerate((1 - pos_x, pos_x))]
    up_next = [remote(sums.at[core, 0, rows_of(chip_y), cols_of(half, GRAD_HALF)], last_up.at[:, cols_of(half, GRAD_HALF)],
                      27 + order, to_y) for order, half in enumerate(halves)]
    dn_next = remote(sums.at[core, 1, :, cols_of(chip_x, dn_cols)], last_dn, 29, to_x)

    def add_up(index, order):
        cols = cols_of(halves[order], GRAD_HALF)
        sums[core, 0, rows_of(index), cols] += part[0, rows_of(index), cols]

    def add_dn(index):
        cols = cols_of(index, dn_cols)
        sums[core, 1, :, cols] += part[1, :, cols]

    def scatter_half(order):
        for kind in range(2):
            for tile in range(n_sub):
                part_copy(kind, order * n_sub + tile).wait_recv()
        for slot in range(2):
            add_up((halves[slot]) * 2 + 1 - pos_x, order)
            up_first[order][slot].start()
            if order == 0:
                add_dn((1 - pos_y) * 2 + (1 - pos_x if slot == 0 else pos_x))
                dn_first[slot].start()
        add_up(chip_y, order)
        if order == 1:
            add_dn(chip_x)
            add_dn(chip)
        add_up(chip, order)

    loads[0].wait()
    for block in (1, 0):
        own = core == block

        @pl.when(own)
        def _():
            for copy in loads[1:4]:
                copy.wait()

        @pl.when(jnp.logical_not(own))
        def _():
            swap_acts.wait_recv()

        acts_row[...] = acts[block].T
        grad_row[...] = grad[...].T
        def tile_step(step, carry, block=block, own=own):
            late = step // n_sub
            cols = cols_of((1 - pos_y + late * (2 * pos_y - 1)) * n_sub + lax.rem(step, n_sub), GRAD_TILE)

            @pl.when(jnp.logical_and(jnp.logical_not(own), step < n_sub))
            def _():
                swap_piece(0, step).wait_recv()
                swap_piece(1, step).wait_recv()

            @pl.when(jnp.logical_and(jnp.logical_not(own), step == n_sub))
            def _():
                for copy in swap_late:
                    copy.wait_recv()

            half, at_step = (0, 2 * n_sub - 1) if block == 1 else (1, n_sub)
            pl.when(jnp.logical_and(core == 1, step == at_step))(functools.partial(scatter_half, half))

            pre_act = jnp.dot(acts_row[...], wts[block, 0, :, cols], preferred_element_type=jnp.float32)
            d_hidden = jnp.dot(grad_row[...], wts[block, 1, :, cols], preferred_element_type=jnp.float32)
            hidden, slope = gelu_pair(pre_act)
            dw_down = jnp.dot(grad[...], hidden.astype(jnp.bfloat16), preferred_element_type=jnp.float32)
            d_tile = (d_hidden * slope).astype(jnp.bfloat16)
            if block == 1:
                d_pre[:, cols] = d_tile
            dw_up = jnp.dot(acts[block], d_tile, preferred_element_type=jnp.float32)

            @pl.when(jnp.logical_and(own, step == 0))
            def _():
                for copy in loads[4:6]:
                    copy.wait()

            @pl.when(own)
            def _():
                sums[block, 0, :, cols] += dw_up
                sums[block, 1, :, cols] += dw_down

            @pl.when(jnp.logical_not(own))
            def _():
                sums[block, 0, :, cols] = dw_up
                sums[block, 1, :, cols] = dw_down
                part_copy(0, step).start()
                part_copy(1, step).start()
            return carry

        lax.fori_loop(0, 2 * n_sub, tile_step, 0)
        if block == 1:
            d_in = lax.dot_general(wts[1, 0], d_pre[...], (((1,), (1,)), ((), ())), preferred_element_type=jnp.float32)
            grad[...] = (grad[...].astype(jnp.float32) + d_in).astype(jnp.bfloat16)

    @pl.when(core == 0)
    def _():
        scatter_half(0)
        scatter_half(1)

    for copy in loads[6:]:
        copy.start()

    n_slot = 2 * half_rows // ROW_TILE
    per_micro = micro_in.shape[2] // ROW_TILE

    def x_slot(tile):
        slot = lax.rem(tile, n_slot)
        return acts.at[slot // 2, :, cols_of(lax.rem(slot, 2), ROW_TILE)]

    def x_load(tile):
        return pltpu.make_async_copy(micro_in.at[tile_place(n_own, per_micro, core, tile)], x_slot(tile), tile_sem.at[0, lax.rem(tile, n_slot)])

    start_all([x_load(tile) for tile in range(n_slot)])

    up_first[0][0].wait_recv()
    cols = cols_of(halves[0], GRAD_HALF)
    sums[core, 0, rows_of(chip_y), cols] += fwd_up[0, :, cols]
    up_next[0].start()
    dn_first[0].wait_recv()
    sums[core, 1, :, cols_of(chip_x, dn_cols)] += fwd_dn[0]
    dn_next.start()
    up_first[1][0].wait_recv()
    cols = cols_of(halves[1], GRAD_HALF)
    sums[core, 0, rows_of(chip_y), cols] += fwd_up[0, :, cols]
    up_next[1].start()
    for order in range(2):
        up_first[order][1].wait_recv()
        up_next[order].wait_recv()
    dn_first[1].wait_recv()
    scale = 1.0 / n_data
    mean_up = (sums[core, 0, rows_of(chip)] + fwd_up[1] + last_up[...]) * scale
    last_up[...] = mean_up
    square = jnp.sum((mean_up * mean_up).reshape(up_rows // 8, 8, ff_width), axis=0)
    dn_next.wait_recv()
    mean_dn = (sums[core, 1, :, cols_of(chip, dn_cols)] + fwd_dn[1] + last_dn[...]) * scale
    last_dn[...] = mean_dn
    square_dn = jnp.sum((mean_dn * mean_dn).reshape(width // 8, 8, dn_cols), axis=0)
    tile_sum = sum(square[:, first:first + 128] for first in range(0, ff_width, 128))
    tile_sum = tile_sum + sum(square_dn[:, first:first + 128] for first in range(0, dn_cols, 128))
    norm_tiles[me] = tile_sum
    norm_copies = []
    for offset in range(1, n_dev):
        other = lax.rem(me + offset, n_dev)
        norm_copies.append(remote(norm_tiles.at[me], norm_tiles.at[me], 29 + offset, (other // 2, lax.rem(other, 2))))
    for copy in norm_copies:
        copy.start()
    for copy in loads[6:]:
        copy.wait()
    for copy in norm_copies:
        copy.wait_recv()
    total_sq = jnp.sum(jnp.sum(norm_tiles[...], axis=0), keepdims=True)
    clip = jnp.minimum(1.0, norm_ref[0] / (jnp.sqrt(total_sq) + NORM_EPS))
    rate = rate_ref[0]

    chips = (chip, chip_x, chip_y, chip_d)
    up_at = [wts.at[core, 0, rows_of(index)] for index in chips]
    dn_at = [wts.at[core, 1, :, cols_of(index, dn_cols)] for index in chips]
    up_x, up_y, up_relay = remote(up_at[0], up_at[0], 37, to_x), remote(up_at[0], up_at[0], 38, to_y), remote(up_at[1], up_at[1], 39, to_y)
    dn_x, dn_y, dn_relay = remote(dn_at[0], dn_at[0], 40, to_x), remote(dn_at[0], dn_at[0], 41, to_y), remote(dn_at[2], dn_at[2], 42, to_x)
    up_peer = [remote(up_at[index], up_at[index], 43 + index, to_peer) for index in range(4)]
    dn_peer = [remote(dn_at[index], dn_at[index], 47 + index, to_peer) for index in range(4)]

    def gather_up():
        up_x.start()
        up_y.start()
        up_peer[0].start()

    def gather_dn():
        dn_y.start()
        dn_x.start()
        dn_peer[0].start()

    def gather_relay():
        up_x.wait_recv()
        up_relay.start()
        up_peer[1].start()
        dn_y.wait_recv()
        dn_relay.start()
        dn_peer[2].start()

    def gather_near():
        up_y.wait_recv()
        up_peer[2].start()
        dn_x.wait_recv()
        dn_peer[1].start()

    def gather_far():
        up_relay.wait_recv()
        up_peer[3].start()
        dn_relay.wait_recv()
        dn_peer[3].start()

    def gather_peer():
        for copy in up_peer + dn_peer:
            copy.wait_recv()

    state = adamw_update(part[0, 0:up_rows], part[0, up_rows:2 * up_rows], part[0, 2 * up_rows:3 * up_rows], clip * last_up[...], rate)
    wts[core, 0, rows_of(chip)] = state[0].astype(jnp.bfloat16)
    for index in range(3):
        part[0, index * up_rows:(index + 1) * up_rows] = state[index]
    pl.when(core == 0)(gather_up)
    state = adamw_update(part[1, :, 0:dn_cols], part[1, :, dn_cols:2 * dn_cols], part[1, :, 2 * dn_cols:3 * dn_cols], clip * last_dn[...], rate)
    wts[core, 1, :, cols_of(chip, dn_cols)] = state[0].astype(jnp.bfloat16)
    for index in range(3):
        part[1, :, index * dn_cols:(index + 1) * dn_cols] = state[index]
    pl.when(core == 0)(gather_dn)
    stores = [pltpu.make_async_copy(src, dst, store_sem.at[index]) for index, (src, dst) in enumerate([
        (part.at[0, 0:up_rows], new_up), (part.at[0, up_rows:2 * up_rows], out1_up), (part.at[0, 2 * up_rows:3 * up_rows], out2_up),
        (part.at[1, :, 0:dn_cols], new_dn), (part.at[1, :, dn_cols:2 * dn_cols], out1_dn),
        (part.at[1, :, 2 * dn_cols:3 * dn_cols], out2_dn)])]
    for copy in stores:
        copy.start()

    @pl.when(core == 0)
    def _():
        gather_relay()
        gather_near()
        gather_far()

    @pl.when(core == 1)
    def _():
        gather_peer()
        gather_up()
        gather_dn()

    swap_acts.wait_send()
    for order in range(2):
        for copy in up_first[order] + [up_next[order]]:
            copy.wait_send()
        for kind in range(2):
            for tile in range(n_sub):
                part_copy(kind, order * n_sub + tile).wait_send()
    for copy in dn_first + [dn_next] + norm_copies + swap_late + [swap_piece(kind, tile) for kind in range(2) for tile in range(n_sub)]:
        copy.wait_send()

    def weights_out(block):
        return [pltpu.make_async_copy(turned, w_up_out.at[block], store_sem.at[6 + block]),
                pltpu.make_async_copy(wts.at[block, 1], w_dn_out.at[block], store_sem.at[8 + block])]

    n_first = own_first.shape[0]
    per_row = ff_width // ROW_TILE

    def mid_slot(tile):
        row = tile // per_row
        return row // 2, lax.rem(row, 2), slice(None), cols_of(lax.rem(tile, per_row), ROW_TILE)

    turned[...] = wts[0, 0].T
    start_all(weights_out(0))

    def first_block(tile, carry):
        for number, action in ((4, gather_relay), (5, gather_near), (7, gather_far)):
            pl.when(jnp.logical_and(core == 1, tile == number))(action)
        x_load(tile).wait()
        mid = tile_forward(x_slot(tile)[...], turned, wts.at[0, 1], hidden_ref, FF_TILE)
        sums[mid_slot(tile)] = mid.astype(jnp.float32)
        pl.when(tile + n_slot < n_first)(lambda: x_load(tile + n_slot).start())
        return carry

    lax.fori_loop(0, n_first, first_block, 0)
    pl.when(core == 0)(gather_peer)
    weights_out(0)[0].wait()
    turned[...] = wts[1, 0].T
    start_all(weights_out(1))

    def y_out(tile):
        slot = lax.rem(tile, 2)
        y_slot = grad.at[:, cols_of(slot, ROW_TILE)]
        keep = pltpu.make_async_copy(y_slot, own_first.at[tile], tile_sem.at[1, slot])
        give = pltpu.make_async_remote_copy(src_ref=y_slot, dst_ref=peer_first.at[tile], send_sem=tile_sem.at[2, slot],
                                            recv_sem=recv_sem.at[51 + tile], device_id=to_peer, device_id_type=MESH_ID)
        return keep, give

    def y_wait(tile):
        keep, give = y_out(tile)
        keep.wait()
        give.wait_send()

    def second_block(tile, carry):
        result = tile_forward(sums[mid_slot(tile)].astype(jnp.bfloat16), turned, wts.at[1, 1], hidden_ref, FF_TILE)
        pl.when(tile >= 2)(lambda: y_wait(tile - 2))
        grad[:, cols_of(lax.rem(tile, 2), ROW_TILE)] = result
        start_all(y_out(tile))
        return carry

    lax.fori_loop(0, n_first, second_block, 0)
    y_wait(n_first - 2)
    y_wait(n_first - 1)
    for tile in range(n_first):
        y_out(tile)[1].wait_recv()

    for copy in [up_x, up_y, up_relay, dn_x, dn_y, dn_relay] + up_peer + dn_peer:
        copy.wait_send()
    for copy in stores + weights_out(0)[1:] + weights_out(1):
        copy.wait()


def update_weights(n_data, arrays, learn_rate, max_norm):
    width, ff_width = arrays[6].shape
    n_rows = arrays[11].shape[1]
    half_rows = n_rows // 2
    up_rows, dn_cols = arrays[0].shape[0], arrays[1].shape[1]
    f32, bf16 = jnp.float32, jnp.bfloat16
    up_state, dn_state = jax.ShapeDtypeStruct((up_rows, ff_width), f32), jax.ShapeDtypeStruct((width, dn_cols), f32)
    first = jax.ShapeDtypeStruct((N_FIRST, width, ROW_TILE), bf16)
    any_spec = pl.BlockSpec(memory_space=pl.ANY)
    smem_spec = pl.BlockSpec(memory_space=pltpu.SMEM)
    n_sem = 51 + N_FIRST

    def body(*refs):
        update_kernel(n_data, *refs)

    flops = 20 * half_rows * width * ff_width + 8 * N_FIRST * ROW_TILE * width * ff_width
    return pl.pallas_call(
        body,
        in_specs=[any_spec] * 13 + [smem_spec] * 2,
        out_specs=[any_spec] * 10,
        out_shape=[up_state, dn_state, up_state, up_state, dn_state, dn_state,
                   jax.ShapeDtypeStruct((2, ff_width, width), bf16), jax.ShapeDtypeStruct((2, width, ff_width), bf16), first, first],
        scratch_shapes=[
            pltpu.VMEM((2, 2, width, ff_width), bf16), pltpu.VMEM((2, width, half_rows), bf16),
            pltpu.VMEM((half_rows, width), bf16), pltpu.VMEM((width, half_rows), bf16), pltpu.VMEM((half_rows, width), bf16),
            pltpu.VMEM((half_rows, ff_width), bf16), pltpu.VMEM((2, 2, width, ff_width), f32), pltpu.VMEM((2, width, ff_width), f32),
            pltpu.VMEM((2, up_rows, ff_width), f32), pltpu.VMEM((2, width, dn_cols), f32),
            pltpu.VMEM((up_rows, ff_width), f32), pltpu.VMEM((width, dn_cols), f32), pltpu.VMEM((2 * n_data, 8, 128), f32),
            pltpu.VMEM((ff_width, width), bf16), pltpu.VMEM((ff_width, ROW_TILE), bf16),
            pltpu.SemaphoreType.DMA((n_sem,)), pltpu.SemaphoreType.DMA((n_sem,)), pltpu.SemaphoreType.DMA((12,)),
            pltpu.SemaphoreType.DMA((10,)), pltpu.SemaphoreType.DMA((3, 4))],
        compiler_params=pltpu.CompilerParams(collective_id=0, has_side_effects=True, vmem_limit_bytes=VMEM_LIMIT),
        cost_estimate=pl.CostEstimate(flops=flops, bytes_accessed=60000000, transcendentals=0),
        name="update",
    )(*arrays, learn_rate.reshape(1), max_norm.reshape(1))


def solution(mesh):
    n_data = mesh.shape['data']

    def step_body(master_up, master_down, moment1_up, moment2_up, moment1_down, moment2_down,
                  compute_up, compute_down, accum_up, accum_down, stage_acts, loss_grad, next_micro,
                  learn_rate, max_norm):
        arrays = (master_up[0], master_down[0].T, moment1_up[0], moment2_up[0], moment1_down[0].T, moment2_down[0].T,
                  compute_up[0], compute_down[0].T, accum_up[0, 0], accum_down[0, 0].T, stage_acts[0].T, loss_grad.T,
                  jnp.swapaxes(next_micro, 1, 2))
        *states, w_up_t, w_dn_t, own_first, peer_first = update_weights(n_data, arrays, learn_rate, max_norm)
        last_acts, states = forward_rest(arrays[12], w_up_t, w_dn_t, own_first, peer_first, states)
        new_up, new_dn, out1_up, out2_up, out1_dn, out2_dn = states
        return (new_up[None], new_dn.T[None], out1_up[None], out2_up[None], out1_dn.T[None], out2_dn.T[None], last_acts)

    shard_spec = P('stage', 'data', None)
    whole_spec = P('stage', None, None)
    accum_spec = P('data', 'stage', None, None)
    micro_spec = P(None, 'data', None)
    in_specs = (shard_spec,) * 6 + (whole_spec, whole_spec, accum_spec, accum_spec,
                                    P('stage', 'data', None), P('data', None), micro_spec, P(), P())
    out_specs = (shard_spec,) * 6 + (micro_spec,)
    return jax.shard_map(step_body, mesh=mesh, in_specs=in_specs, out_specs=out_specs, check_vma=False)
```

```python
import functools

import jax
import jax.numpy as jnp
from jax import lax
from jax.experimental import pallas as pl
from jax.experimental.pallas import tpu as pltpu
from jax.sharding import PartitionSpec as P

BETA_ONE = 0.9
BETA_TWO = 0.95
ADAM_EPS = 1e-8
WEIGHT_DECAY = 0.1
NORM_EPS = 1e-6
STEP_NUM = 10
BIAS_ONE = 1.0 - BETA_ONE ** STEP_NUM
BIAS_TWO = 1.0 - BETA_TWO ** STEP_NUM


def adamw_update(master, moment_one, moment_two, grad_step, learn_rate):
    mom_one = BETA_ONE * moment_one + (1.0 - BETA_ONE) * grad_step
    mom_two = BETA_TWO * moment_two + (1.0 - BETA_TWO) * grad_step * grad_step
    step_dir = (mom_one / BIAS_ONE) / (jnp.sqrt(mom_two / BIAS_TWO) + ADAM_EPS)
    new_master = master - learn_rate * (step_dir + WEIGHT_DECAY * master)
    return new_master, mom_one, mom_two


MESH_ID = pl.DeviceIdType.MESH
GRAD_HALF = 768
GRAD_TILE = 256
GELU_LIN = 0.7978845608028654
GELU_CUB = GELU_LIN * 0.044715
ROW_TILE = 512
FF_TILE = 256
CHUNKS = ((12, 256), (5, 256), (3, 512))
N_FIRST = 12
VMEM_LIMIT = 67000000


def gelu_half(pre_act):
    inner = pre_act * (GELU_LIN + GELU_CUB * (pre_act * pre_act))
    half = 0.5 * pre_act
    return half + half * jnp.tanh(inner)


def tile_forward(cols_in, w_up_t, w_down_t, hidden_ref, ff_tile):
    for start in range(0, hidden_ref.shape[0], ff_tile):
        rows = pl.ds(start, ff_tile)
        pre_act = jnp.dot(w_up_t[rows, :], cols_in, preferred_element_type=jnp.float32)
        hidden_ref[rows, :] = gelu_half(pre_act).astype(jnp.bfloat16)
    branch = jnp.dot(w_down_t[...], hidden_ref[...], preferred_element_type=jnp.float32)
    return (cols_in.astype(jnp.float32) + branch).astype(jnp.bfloat16)


def tile_place(n_own, per_micro, owner, tile):
    return owner * n_own + tile // per_micro, slice(None), pl.ds(pl.multiple_of(lax.rem(tile, per_micro) * ROW_TILE, ROW_TILE), ROW_TILE)


def start_all(copies):
    for copy in copies:
        copy.start()


def wait_all(copies):
    for copy in copies:
        copy.wait()


def forward_kernel(has_prev, ff_tile, copies, n_state, base, n_own, per_micro, *refs):
    refs = list(refs)
    x_ref, w_up_in, w_dn_in = refs[:3]
    refs = refs[3:]
    n_copy = len(copies)
    copy_refs, refs = refs[:n_copy], refs[n_copy:]
    state_in, refs = refs[:n_state], refs[n_state:]
    if has_prev:
        refs.pop(0)
    out_ref, y_ref, refs = refs[0], refs[1], refs[2:]
    state_out, refs = refs[:n_state], refs[n_state:]
    w_up_t, w_dn_t, hidden_ref, y_buf, y_sem, wt_sem, in_sem, out_sem, state_sem, *refs = refs
    copy_bufs, state_buf = refs[:n_copy], refs[n_copy:]
    mine = lax.axis_index('stage')
    step, n_steps = pl.program_id(0), pl.num_programs(0)
    slot = lax.rem(step, 2)

    def y_copy(which):
        return pltpu.make_async_copy(y_buf.at[which], out_ref.at[tile_place(n_own, per_micro, mine, base + step)], y_sem.at[which])

    def enter(index, turn):
        _, _, _, share = copies[index]
        slot = lax.rem(turn, 2)
        return pltpu.make_async_copy(copy_refs[index].at[pl.ds(turn * share, share)], copy_bufs[index].at[slot], in_sem.at[index, slot])

    def leave(index, turn):
        from_peer, first, _, share = copies[index]
        slot = lax.rem(turn, 2)
        owner = 1 - mine if from_peer else mine
        return [pltpu.make_async_copy(copy_bufs[index].at[slot, tile], out_ref.at[tile_place(n_own, per_micro, owner, first + turn * share + tile)],
                                      out_sem.at[index, slot, tile]) for tile in range(share)]

    def weight_copies(block):
        return [pltpu.make_async_copy(src.at[block], dst.at[block], wt_sem.at[block, kind])
                for kind, (src, dst) in enumerate(((w_up_in, w_up_t), (w_dn_in, w_dn_t)))]

    def state_copies(leaving):
        pairs = zip(state_buf, state_out) if leaving else zip(state_in, state_buf)
        return [pltpu.make_async_copy(src, dst, state_sem.at[index]) for index, (src, dst) in enumerate(pairs)]

    def for_copies(turn, action):
        for index in range(n_copy):
            pl.when(jnp.logical_and(turn >= 0, turn * copies[index][3] < copies[index][2]))(functools.partial(action, index, turn))

    def leave_start(index, turn):
        enter(index, turn).wait()
        start_all(leave(index, turn))

    pl.when(step == 0)(lambda: start_all(weight_copies(0) + weight_copies(1) + state_copies(False)))
    for_copies(step - 1, leave_start)
    for_copies(step - 2, lambda index, turn: wait_all(leave(index, turn)))
    for_copies(step, lambda index, turn: enter(index, turn).start())
    pl.when(step >= 2)(lambda: y_copy(slot).wait())
    if n_state:
        @pl.when(step == 1)
        def _():
            wait_all(state_copies(False))
            start_all(state_copies(True))

    pl.when(step == 0)(lambda: wait_all(weight_copies(0) + weight_copies(1)))
    cols = x_ref[0]
    for block in range(2):
        cols = tile_forward(cols, w_up_t.at[block], w_dn_t.at[block], hidden_ref.at[block], ff_tile)
    y_buf[slot] = cols
    y_ref[0] = cols
    y_copy(slot).start()

    @pl.when(step == n_steps - 1)
    def _():
        for_copies(step - 1, lambda index, turn: wait_all(leave(index, turn)))
        y_copy(slot).wait()
        y_copy(1 - slot).wait()
        wait_all(state_copies(True))


def forward_chunk(base, n_chunk, ff_tile, micro_t, w_up_t, w_down_t, prev_out, copied, states):
    n_micro, width, n_rows = micro_t.shape
    n_own, per_micro = n_micro // 2, n_rows // ROW_TILE
    ff_width = w_up_t.shape[1]
    any_spec = pl.BlockSpec(memory_space=pl.ANY)
    scalar = jnp.full((1,), lax.axis_index('stage') * n_own, jnp.int32)
    in_specs = [pl.BlockSpec((1, width, ROW_TILE), lambda i, first: (first[0] + (base + i) // per_micro, 0, lax.rem(base + i, per_micro)))]
    operands = [micro_t, w_up_t, w_down_t] + [array for array, _, _ in copied] + list(states)
    in_specs += [any_spec] * (len(operands) - 1)
    aliases = {}
    if prev_out is not None:
        in_specs.append(any_spec)
        operands.append(prev_out)
        aliases = {len(operands): 0}
    copies = []
    for array, from_peer, first in copied:
        count = array.shape[0]
        share = min(size for size in range(1, count + 1) if count % size == 0 and count // size < n_chunk)
        copies.append((from_peer, first, count, share))
    max_share = max([1] + [share for *_, share in copies])
    dma = pltpu.SemaphoreType.DMA

    def body(first, *refs):
        forward_kernel(prev_out is not None, ff_tile, copies, len(states), base, n_own, per_micro, *refs)

    return pl.pallas_call(
        body,
        grid_spec=pltpu.PrefetchScalarGridSpec(
            num_scalar_prefetch=1, grid=(n_chunk,), in_specs=in_specs,
            out_specs=[any_spec, pl.BlockSpec((1, width, ROW_TILE), lambda i, first: (i, 0, 0))] + [any_spec] * len(states),
            scratch_shapes=[pltpu.VMEM(w_up_t.shape, jnp.bfloat16), pltpu.VMEM(w_down_t.shape, jnp.bfloat16),
                            pltpu.VMEM((2, ff_width, ROW_TILE), jnp.bfloat16), pltpu.VMEM((2, width, ROW_TILE), jnp.bfloat16),
                            dma((2,)), dma((2, 2)), dma((2, 2)), dma((2, 2, max_share)), dma((6,))]
            + [pltpu.VMEM((2, share, width, ROW_TILE), jnp.bfloat16) for *_, share in copies]
            + [pltpu.VMEM(array.shape, array.dtype) for array in states]),
        out_shape=[jax.ShapeDtypeStruct(micro_t.shape, jnp.bfloat16),
                   jax.ShapeDtypeStruct((n_chunk, width, ROW_TILE), jnp.bfloat16)]
        + [jax.ShapeDtypeStruct(array.shape, array.dtype) for array in states],
        input_output_aliases=aliases,
        compiler_params=pltpu.CompilerParams(dimension_semantics=("arbitrary",), vmem_limit_bytes=VMEM_LIMIT),
        cost_estimate=pl.CostEstimate(flops=8 * n_chunk * ROW_TILE * width * ff_width, bytes_accessed=n_chunk * ROW_TILE * width,
                                      transcendentals=0),
        name=f"fwd_{base}",
    )(scalar, *operands)


def place_tiles(out, tiles, first, n_own):
    count, per_micro = tiles.shape[0], out.shape[2] // ROW_TILE
    any_spec = pl.BlockSpec(memory_space=pl.ANY)

    def body(tiles_ref, old_ref, out_ref, buf, in_sem, out_sem):
        owner = 1 - lax.axis_index('stage')
        enter = [pltpu.make_async_copy(tiles_ref.at[tile], buf.at[tile], in_sem.at[tile]) for tile in range(count)]
        leave = [pltpu.make_async_copy(buf.at[tile], out_ref.at[tile_place(n_own, per_micro, owner, first + tile)], out_sem.at[tile])
                 for tile in range(count)]
        start_all(enter)
        for tile in range(count):
            enter[tile].wait()
            leave[tile].start()
        wait_all(leave)

    return pl.pallas_call(
        body, in_specs=[any_spec] * 2, out_specs=any_spec, out_shape=jax.ShapeDtypeStruct(out.shape, out.dtype),
        scratch_shapes=[pltpu.VMEM(tiles.shape, tiles.dtype), pltpu.SemaphoreType.DMA((count,)), pltpu.SemaphoreType.DMA((count,))],
        input_output_aliases={1: 0}, compiler_params=pltpu.CompilerParams(vmem_limit_bytes=VMEM_LIMIT), name=f"place_{first}")(tiles, out)


def forward_rest(micro_t, w_up_t, w_down_t, own_first, peer_first, states):
    n_own = micro_t.shape[0] // 2
    out, base = None, own_first.shape[0]
    received, results = [], []
    for number, (n_chunk, ff_tile) in enumerate(CHUNKS):
        copied, passed = [], []
        if number == 0:
            copied, passed = [(own_first, False, 0), (peer_first, True, 0)], states
        elif number >= 2:
            copied = [received.pop(0)]
        out, part, *handed = forward_chunk(base, n_chunk, ff_tile, micro_t, w_up_t, w_down_t, out, copied, passed)
        results += handed
        received.append((lax.ppermute(part, 'stage', [(0, 1), (1, 0)]), True, base))
        base += n_chunk
    for tiles, _, first in received:
        out = place_tiles(out, tiles, first, n_own)
    return jnp.swapaxes(out, 1, 2), results


def gelu_pair(pre_act):
    square = pre_act * pre_act
    tanh_in = jnp.tanh(pre_act * (GELU_LIN + GELU_CUB * square))
    half = 0.5 * pre_act
    value = half + half * tanh_in
    slope = 0.5 + 0.5 * tanh_in + half * (1.0 - tanh_in * tanh_in) * (GELU_LIN + 3.0 * GELU_CUB * square)
    return value, slope


def update_kernel(n_data, mst_up, mst_dn, mo1_up, mo2_up, mo1_dn, mo2_dn, cmp_up, cmp_dn, acc_up, acc_dn, acts_in, grad_in,
                  micro_in, rate_ref, norm_ref,
                  new_up, new_dn, out1_up, out2_up, out1_dn, out2_dn, w_up_out, w_dn_out, own_first, peer_first,
                  wts, acts, acts_row, grad, grad_row, d_pre, sums, part, fwd_up, fwd_dn, last_up, last_dn,
                  norm_tiles, turned, hidden_ref, send_sem, recv_sem, load_sem, store_sem, tile_sem):
    chip = lax.axis_index('data')
    core = lax.axis_index('stage')
    peer = 1 - core
    pos_x, pos_y = lax.rem(chip, 2), chip // 2
    chip_x = pos_y * 2 + (1 - pos_x)
    chip_y = (1 - pos_y) * 2 + pos_x
    chip_d = 3 - chip
    me = chip * 2 + core
    n_dev = 2 * n_data
    half_rows = grad.shape[1]
    width, ff_width = wts.shape[2:]
    up_rows, dn_cols = last_up.shape[0], last_dn.shape[1]
    n_own = micro_in.shape[0] // 2
    n_sub = GRAD_HALF // GRAD_TILE
    halves = (1 - pos_y, pos_y)

    def cols_of(index, size):
        return pl.ds(pl.multiple_of(index * size, size), size)

    def rows_of(index):
        return pl.ds(pl.multiple_of(index * up_rows, 8), up_rows)

    def remote(src, dst, index, device):
        return pltpu.make_async_remote_copy(src_ref=src, dst_ref=dst, send_sem=send_sem.at[index], recv_sem=recv_sem.at[index],
                                            device_id=device, device_id_type=MESH_ID)

    to_peer, to_x, to_y = (chip, peer), (chip_x, core), (chip_y, core)

    up_state = [part.at[0, index * up_rows:(index + 1) * up_rows] for index in range(3)]
    dn_state = [part.at[1, :, index * dn_cols:(index + 1) * dn_cols] for index in range(3)]
    loads = [pltpu.make_async_copy(src, dst, load_sem.at[index]) for index, (src, dst) in enumerate([
        (grad_in.at[:, cols_of(core, half_rows)], grad), (acts_in.at[:, cols_of(core, half_rows)], acts.at[core]),
        (cmp_up, wts.at[core, 0]), (cmp_dn, wts.at[core, 1]),
        (acc_up, sums.at[core, 0]), (acc_dn, sums.at[core, 1]),
        *zip((mst_up, mo1_up, mo2_up), up_state), *zip((mst_dn, mo1_dn, mo2_dn), dn_state)])]
    for copy in loads[:6]:
        copy.start()

    barrier = pltpu.get_barrier_semaphore()
    for offset in range(1, n_dev):
        other = lax.rem(me + offset, n_dev)
        pl.semaphore_signal(barrier, inc=1, device_id=(other // 2, lax.rem(other, 2)), device_id_type=MESH_ID)
    pl.semaphore_wait(barrier, n_dev - 1)

    swap_acts = remote(acts_in.at[:, cols_of(peer, half_rows)], acts.at[core], 0, to_peer)
    def swap_piece(kind, tile):
        cols = cols_of(halves[0] * n_sub + tile, GRAD_TILE)
        return remote((cmp_up, cmp_dn)[kind].at[:, cols], wts.at[core, kind, :, cols], 1 + kind * n_sub + tile, to_peer)

    swap_late = [remote((cmp_up, cmp_dn)[kind].at[:, cols_of(halves[1], GRAD_HALF)], wts.at[core, kind, :, cols_of(halves[1], GRAD_HALF)],
                        1 + 2 * n_sub + kind, to_peer) for kind in range(2)]
    swap_acts.start()
    for tile in range(n_sub):
        for kind in range(2):
            swap_piece(kind, tile).start()
    for copy in swap_late:
        copy.start()

    def part_copy(kind, step):
        late = step // n_sub
        cols = cols_of((1 - pos_y + late * (2 * pos_y - 1)) * n_sub + lax.rem(step, n_sub), GRAD_TILE)
        return remote(sums.at[peer, kind, :, cols], part.at[kind, :, cols], 9 + kind * 2 * n_sub + step, to_peer)

    up_first = [[remote(sums.at[core, 0, rows_of(row * 2 + 1 - pos_x), cols_of(half, GRAD_HALF)],
                        fwd_up.at[slot, :, cols_of(half, GRAD_HALF)], 21 + order * 2 + slot, to_x)
                 for slot, row in enumerate(halves)] for order, half in enumerate(halves)]
    dn_first = [remote(sums.at[core, 1, :, cols_of((1 - pos_y) * 2 + col, dn_cols)], fwd_dn.at[slot], 25 + slot, to_y)
                for slot, col in enumerate((1 - pos_x, pos_x))]
    up_next = [remote(sums.at[core, 0, rows_of(chip_y), cols_of(half, GRAD_HALF)], last_up.at[:, cols_of(half, GRAD_HALF)],
                      27 + order, to_y) for order, half in enumerate(halves)]
    dn_next = remote(sums.at[core, 1, :, cols_of(chip_x, dn_cols)], last_dn, 29, to_x)

    def add_up(index, order):
        cols = cols_of(halves[order], GRAD_HALF)
        sums[core, 0, rows_of(index), cols] += part[0, rows_of(index), cols]

    def add_dn(index):
        cols = cols_of(index, dn_cols)
        sums[core, 1, :, cols] += part[1, :, cols]

    def scatter_half(order):
        for kind in range(2):
            for tile in range(n_sub):
                part_copy(kind, order * n_sub + tile).wait_recv()
        for slot in range(2):
            add_up((halves[slot]) * 2 + 1 - pos_x, order)
            up_first[order][slot].start()
            if order == 0:
                add_dn((1 - pos_y) * 2 + (1 - pos_x if slot == 0 else pos_x))
                dn_first[slot].start()
        add_up(chip_y, order)
        if order == 1:
            add_dn(chip_x)
            add_dn(chip)
        add_up(chip, order)

    loads[0].wait()
    for block in (1, 0):
        own = core == block

        @pl.when(own)
        def _():
            for copy in loads[1:4]:
                copy.wait()

        @pl.when(jnp.logical_not(own))
        def _():
            swap_acts.wait_recv()

        acts_row[...] = acts[block].T
        grad_row[...] = grad[...].T
        def tile_step(step, carry, block=block, own=own):
            late = step // n_sub
            cols = cols_of((1 - pos_y + late * (2 * pos_y - 1)) * n_sub + lax.rem(step, n_sub), GRAD_TILE)

            @pl.when(jnp.logical_and(jnp.logical_not(own), step < n_sub))
            def _():
                swap_piece(0, step).wait_recv()
                swap_piece(1, step).wait_recv()

            @pl.when(jnp.logical_and(jnp.logical_not(own), step == n_sub))
            def _():
                for copy in swap_late:
                    copy.wait_recv()

            half, at_step = (0, 2 * n_sub - 1) if block == 1 else (1, n_sub)
            pl.when(jnp.logical_and(core == 1, step == at_step))(functools.partial(scatter_half, half))

            pre_act = jnp.dot(acts_row[...], wts[block, 0, :, cols], preferred_element_type=jnp.float32)
            d_hidden = jnp.dot(grad_row[...], wts[block, 1, :, cols], preferred_element_type=jnp.float32)
            hidden, slope = gelu_pair(pre_act)
            dw_down = jnp.dot(grad[...], hidden.astype(jnp.bfloat16), preferred_element_type=jnp.float32)
            d_tile = (d_hidden * slope).astype(jnp.bfloat16)
            if block == 1:
                d_pre[:, cols] = d_tile
            dw_up = jnp.dot(acts[block], d_tile, preferred_element_type=jnp.float32)

            @pl.when(jnp.logical_and(own, step == 0))
            def _():
                for copy in loads[4:6]:
                    copy.wait()

            @pl.when(own)
            def _():
                sums[block, 0, :, cols] += dw_up
                sums[block, 1, :, cols] += dw_down

            @pl.when(jnp.logical_not(own))
            def _():
                sums[block, 0, :, cols] = dw_up
                sums[block, 1, :, cols] = dw_down
                part_copy(0, step).start()
                part_copy(1, step).start()
            return carry

        lax.fori_loop(0, 2 * n_sub, tile_step, 0)
        if block == 1:
            d_in = lax.dot_general(wts[1, 0], d_pre[...], (((1,), (1,)), ((), ())), preferred_element_type=jnp.float32)
            grad[...] = (grad[...].astype(jnp.float32) + d_in).astype(jnp.bfloat16)

    @pl.when(core == 0)
    def _():
        scatter_half(0)
        scatter_half(1)

    for copy in loads[6:]:
        copy.start()

    n_slot = 2 * half_rows // ROW_TILE
    per_micro = micro_in.shape[2] // ROW_TILE

    def x_slot(tile):
        slot = lax.rem(tile, n_slot)
        return acts.at[slot // 2, :, cols_of(lax.rem(slot, 2), ROW_TILE)]

    def x_load(tile):
        return pltpu.make_async_copy(micro_in.at[tile_place(n_own, per_micro, core, tile)], x_slot(tile), tile_sem.at[0, lax.rem(tile, n_slot)])

    start_all([x_load(tile) for tile in range(n_slot)])

    up_first[0][0].wait_recv()
    cols = cols_of(halves[0], GRAD_HALF)
    sums[core, 0, rows_of(chip_y), cols] += fwd_up[0, :, cols]
    up_next[0].start()
    dn_first[0].wait_recv()
    sums[core, 1, :, cols_of(chip_x, dn_cols)] += fwd_dn[0]
    dn_next.start()
    up_first[1][0].wait_recv()
    cols = cols_of(halves[1], GRAD_HALF)
    sums[core, 0, rows_of(chip_y), cols] += fwd_up[0, :, cols]
    up_next[1].start()
    for order in range(2):
        up_first[order][1].wait_recv()
        up_next[order].wait_recv()
    dn_first[1].wait_recv()
    scale = 1.0 / n_data
    mean_up = (sums[core, 0, rows_of(chip)] + fwd_up[1] + last_up[...]) * scale
    last_up[...] = mean_up
    square = jnp.sum((mean_up * mean_up).reshape(up_rows // 8, 8, ff_width), axis=0)
    dn_next.wait_recv()
    mean_dn = (sums[core, 1, :, cols_of(chip, dn_cols)] + fwd_dn[1] + last_dn[...]) * scale
    last_dn[...] = mean_dn
    square_dn = jnp.sum((mean_dn * mean_dn).reshape(width // 8, 8, dn_cols), axis=0)
    tile_sum = sum(square[:, first:first + 128] for first in range(0, ff_width, 128))
    tile_sum = tile_sum + sum(square_dn[:, first:first + 128] for first in range(0, dn_cols, 128))
    norm_tiles[me] = tile_sum
    norm_copies = []
    for offset in range(1, n_dev):
        other = lax.rem(me + offset, n_dev)
        norm_copies.append(remote(norm_tiles.at[me], norm_tiles.at[me], 29 + offset, (other // 2, lax.rem(other, 2))))
    for copy in norm_copies:
        copy.start()
    for copy in loads[6:]:
        copy.wait()
    for copy in norm_copies:
        copy.wait_recv()
    total_sq = jnp.sum(jnp.sum(norm_tiles[...], axis=0), keepdims=True)
    clip = jnp.minimum(1.0, norm_ref[0] / (jnp.sqrt(total_sq) + NORM_EPS))
    rate = rate_ref[0]

    chips = (chip, chip_x, chip_y, chip_d)
    up_at = [wts.at[core, 0, rows_of(index)] for index in chips]
    dn_at = [wts.at[core, 1, :, cols_of(index, dn_cols)] for index in chips]
    up_x, up_y, up_relay = remote(up_at[0], up_at[0], 37, to_x), remote(up_at[0], up_at[0], 38, to_y), remote(up_at[1], up_at[1], 39, to_y)
    dn_x, dn_y, dn_relay = remote(dn_at[0], dn_at[0], 40, to_x), remote(dn_at[0], dn_at[0], 41, to_y), remote(dn_at[2], dn_at[2], 42, to_x)
    up_peer = [remote(up_at[index], up_at[index], 43 + index, to_peer) for index in range(4)]
    dn_peer = [remote(dn_at[index], dn_at[index], 47 + index, to_peer) for index in range(4)]

    def gather_up():
        up_x.start()
        up_y.start()
        up_peer[0].start()

    def gather_dn():
        dn_y.start()
        dn_x.start()
        dn_peer[0].start()

    def gather_relay():
        up_x.wait_recv()
        up_relay.start()
        up_peer[1].start()
        dn_y.wait_recv()
        dn_relay.start()
        dn_peer[2].start()

    def gather_near():
        up_y.wait_recv()
        up_peer[2].start()
        dn_x.wait_recv()
        dn_peer[1].start()

    def gather_far():
        up_relay.wait_recv()
        up_peer[3].start()
        dn_relay.wait_recv()
        dn_peer[3].start()

    def gather_peer():
        for copy in up_peer + dn_peer:
            copy.wait_recv()

    state = adamw_update(*[ref[...] for ref in up_state], clip * last_up[...], rate)
    wts[core, 0, rows_of(chip)] = state[0].astype(jnp.bfloat16)
    for ref, value in zip(up_state, state):
        ref[...] = value
    pl.when(core == 0)(gather_up)
    state = adamw_update(*[ref[...] for ref in dn_state], clip * last_dn[...], rate)
    wts[core, 1, :, cols_of(chip, dn_cols)] = state[0].astype(jnp.bfloat16)
    for ref, value in zip(dn_state, state):
        ref[...] = value
    pl.when(core == 0)(gather_dn)
    stores = [pltpu.make_async_copy(src, dst, store_sem.at[index]) for index, (src, dst) in enumerate([
        *zip(up_state, (new_up, out1_up, out2_up)), *zip(dn_state, (new_dn, out1_dn, out2_dn))])]
    for copy in stores:
        copy.start()

    @pl.when(core == 0)
    def _():
        gather_relay()
        gather_near()
        gather_far()

    @pl.when(core == 1)
    def _():
        gather_peer()
        gather_up()
        gather_dn()

    swap_acts.wait_send()
    for order in range(2):
        for copy in up_first[order] + [up_next[order]]:
            copy.wait_send()
        for kind in range(2):
            for tile in range(n_sub):
                part_copy(kind, order * n_sub + tile).wait_send()
    for copy in dn_first + [dn_next] + norm_copies + swap_late + [swap_piece(kind, tile) for kind in range(2) for tile in range(n_sub)]:
        copy.wait_send()

    def weights_out(block):
        return [pltpu.make_async_copy(turned, w_up_out.at[block], store_sem.at[6 + block]),
                pltpu.make_async_copy(wts.at[block, 1], w_dn_out.at[block], store_sem.at[8 + block])]

    n_first = own_first.shape[0]
    per_row = ff_width // ROW_TILE

    def mid_slot(tile):
        row = tile // per_row
        return row // 2, lax.rem(row, 2), slice(None), cols_of(lax.rem(tile, per_row), ROW_TILE)

    turned[...] = wts[0, 0].T
    start_all(weights_out(0))

    def first_block(pair, carry):
        for number, action in ((2, gather_relay), (3, gather_near), (4, gather_far)):
            pl.when(jnp.logical_and(core == 1, pair == number))(action)
        tiles = (2 * pair, 2 * pair + 1)
        wait_all([x_load(tile) for tile in tiles])
        for half, tile in enumerate(tiles):
            mid = tile_forward(x_slot(tile)[...], turned, wts.at[0, 1], hidden_ref.at[half], FF_TILE)
            sums[mid_slot(tile)] = mid.astype(jnp.float32)
        pl.when(tiles[1] + n_slot < n_first)(lambda: start_all([x_load(tile + n_slot) for tile in tiles]))
        return carry

    lax.fori_loop(0, n_first // 2, first_block, 0)
    pl.when(core == 0)(gather_peer)
    weights_out(0)[0].wait()
    turned[...] = wts[1, 0].T
    start_all(weights_out(1))

    def y_out(tile):
        slot = lax.rem(tile, n_slot)
        keep = pltpu.make_async_copy(x_slot(tile), own_first.at[tile], tile_sem.at[1, slot])
        give = pltpu.make_async_remote_copy(src_ref=x_slot(tile), dst_ref=peer_first.at[tile], send_sem=tile_sem.at[2, slot],
                                            recv_sem=recv_sem.at[51 + tile], device_id=to_peer, device_id_type=MESH_ID)
        return keep, give

    def y_wait(tile):
        keep, give = y_out(tile)
        keep.wait()
        give.wait_send()

    def second_block(pair, carry):
        tiles = (2 * pair, 2 * pair + 1)
        for tile in tiles:
            pl.when(pair >= 2)(functools.partial(y_wait, tile - n_slot))
        for half, tile in enumerate(tiles):
            place = x_slot(tile)
            place[...] = tile_forward(sums[mid_slot(tile)].astype(jnp.bfloat16), turned, wts.at[1, 1], hidden_ref.at[half], FF_TILE)
        for tile in tiles:
            start_all(y_out(tile))
        return carry

    lax.fori_loop(0, n_first // 2, second_block, 0)
    for tile in range(n_first - n_slot, n_first):
        y_wait(tile)
    for tile in range(n_first):
        y_out(tile)[1].wait_recv()

    for copy in [up_x, up_y, up_relay, dn_x, dn_y, dn_relay] + up_peer + dn_peer:
        copy.wait_send()
    for copy in stores + weights_out(0)[1:] + weights_out(1):
        copy.wait()


def update_weights(n_data, arrays, learn_rate, max_norm):
    width, ff_width = arrays[6].shape
    n_rows = arrays[11].shape[1]
    half_rows = n_rows // 2
    up_rows, dn_cols = arrays[0].shape[0], arrays[1].shape[1]
    f32, bf16 = jnp.float32, jnp.bfloat16
    up_state, dn_state = jax.ShapeDtypeStruct((up_rows, ff_width), f32), jax.ShapeDtypeStruct((width, dn_cols), f32)
    first = jax.ShapeDtypeStruct((N_FIRST, width, ROW_TILE), bf16)
    any_spec = pl.BlockSpec(memory_space=pl.ANY)
    smem_spec = pl.BlockSpec(memory_space=pltpu.SMEM)
    n_sem = 51 + N_FIRST

    def body(*refs):
        update_kernel(n_data, *refs)

    flops = 20 * half_rows * width * ff_width + 8 * N_FIRST * ROW_TILE * width * ff_width
    return pl.pallas_call(
        body,
        in_specs=[any_spec] * 13 + [smem_spec] * 2,
        out_specs=[any_spec] * 10,
        out_shape=[up_state, dn_state, up_state, up_state, dn_state, dn_state,
                   jax.ShapeDtypeStruct((2, ff_width, width), bf16), jax.ShapeDtypeStruct((2, width, ff_width), bf16), first, first],
        scratch_shapes=[
            pltpu.VMEM((2, 2, width, ff_width), bf16), pltpu.VMEM((2, width, half_rows), bf16),
            pltpu.VMEM((half_rows, width), bf16), pltpu.VMEM((width, half_rows), bf16), pltpu.VMEM((half_rows, width), bf16),
            pltpu.VMEM((half_rows, ff_width), bf16), pltpu.VMEM((2, 2, width, ff_width), f32), pltpu.VMEM((2, width, ff_width), f32),
            pltpu.VMEM((2, up_rows, ff_width), f32), pltpu.VMEM((2, width, dn_cols), f32),
            pltpu.VMEM((up_rows, ff_width), f32), pltpu.VMEM((width, dn_cols), f32), pltpu.VMEM((2 * n_data, 8, 128), f32),
            pltpu.VMEM((ff_width, width), bf16), pltpu.VMEM((2, ff_width, ROW_TILE), bf16),
            pltpu.SemaphoreType.DMA((n_sem,)), pltpu.SemaphoreType.DMA((n_sem,)), pltpu.SemaphoreType.DMA((12,)),
            pltpu.SemaphoreType.DMA((10,)), pltpu.SemaphoreType.DMA((3, 4))],
        compiler_params=pltpu.CompilerParams(collective_id=0, has_side_effects=True, vmem_limit_bytes=VMEM_LIMIT),
        cost_estimate=pl.CostEstimate(flops=flops, bytes_accessed=60000000, transcendentals=0),
        name="update",
    )(*arrays, learn_rate.reshape(1), max_norm.reshape(1))


def solution(mesh):
    n_data = mesh.shape['data']

    def step_body(master_up, master_down, moment1_up, moment2_up, moment1_down, moment2_down,
                  compute_up, compute_down, accum_up, accum_down, stage_acts, loss_grad, next_micro,
                  learn_rate, max_norm):
        arrays = (master_up[0], master_down[0].T, moment1_up[0], moment2_up[0], moment1_down[0].T, moment2_down[0].T,
                  compute_up[0], compute_down[0].T, accum_up[0, 0], accum_down[0, 0].T, stage_acts[0].T, loss_grad.T,
                  jnp.swapaxes(next_micro, 1, 2))
        *states, w_up_t, w_dn_t, own_first, peer_first = update_weights(n_data, arrays, learn_rate, max_norm)
        last_acts, states = forward_rest(arrays[12], w_up_t, w_dn_t, own_first, peer_first, states)
        new_up, new_dn, out1_up, out2_up, out1_dn, out2_dn = states
        return (new_up[None], new_dn.T[None], out1_up[None], out2_up[None], out1_dn.T[None], out2_dn.T[None], last_acts)

    shard_spec = P('stage', 'data', None)
    whole_spec = P('stage', None, None)
    accum_spec = P('data', 'stage', None, None)
    micro_spec = P(None, 'data', None)
    in_specs = (shard_spec,) * 6 + (whole_spec, whole_spec, accum_spec, accum_spec,
                                    P('stage', 'data', None), P('data', None), micro_spec, P(), P())
    out_specs = (shard_spec,) * 6 + (micro_spec,)
    return jax.shard_map(step_body, mesh=mesh, in_specs=in_specs, out_specs=out_specs, check_vma=False)
```

```python
import functools

import jax
import jax.numpy as jnp
from jax import lax
from jax.experimental import pallas as pl
from jax.experimental.pallas import tpu as pltpu
from jax.sharding import PartitionSpec as P

BETA_ONE = 0.9
BETA_TWO = 0.95
ADAM_EPS = 1e-8
WEIGHT_DECAY = 0.1
NORM_EPS = 1e-6
STEP_NUM = 10
BIAS_ONE = 1.0 - BETA_ONE ** STEP_NUM
BIAS_TWO = 1.0 - BETA_TWO ** STEP_NUM


def adamw_update(master, moment_one, moment_two, grad_step, learn_rate):
    mom_one = BETA_ONE * moment_one + (1.0 - BETA_ONE) * grad_step
    mom_two = BETA_TWO * moment_two + (1.0 - BETA_TWO) * grad_step * grad_step
    step_dir = (mom_one / BIAS_ONE) / (jnp.sqrt(mom_two / BIAS_TWO) + ADAM_EPS)
    new_master = master - learn_rate * (step_dir + WEIGHT_DECAY * master)
    return new_master, mom_one, mom_two


MESH_ID = pl.DeviceIdType.MESH
GRAD_HALF = 768
GRAD_TILE = 256
GELU_LIN = 0.7978845608028654
GELU_CUB = GELU_LIN * 0.044715
ROW_TILE = 512
FF_TILE = 256
CHUNKS = ((6, 256), (2, 256))
N_MID = 12
N_FIRST = 24
VMEM_LIMIT = 67000000


def gelu_half(pre_act):
    inner = pre_act * (GELU_LIN + GELU_CUB * (pre_act * pre_act))
    half = 0.5 * pre_act
    return half + half * jnp.tanh(inner)


def tile_forward(cols_in, w_up_t, w_down_t, hidden_ref, ff_tile):
    for start in range(0, hidden_ref.shape[0], ff_tile):
        rows = pl.ds(start, ff_tile)
        pre_act = jnp.dot(w_up_t[rows, :], cols_in, preferred_element_type=jnp.float32)
        hidden_ref[rows, :] = gelu_half(pre_act).astype(jnp.bfloat16)
    branch = jnp.dot(w_down_t[...], hidden_ref[...], preferred_element_type=jnp.float32)
    return (cols_in.astype(jnp.float32) + branch).astype(jnp.bfloat16)


def tile_place(n_own, per_micro, owner, tile):
    return owner * n_own + tile // per_micro, slice(None), pl.ds(pl.multiple_of(lax.rem(tile, per_micro) * ROW_TILE, ROW_TILE), ROW_TILE)


def start_all(copies):
    for copy in copies:
        copy.start()


def wait_all(copies):
    for copy in copies:
        copy.wait()


def forward_kernel(has_prev, ff_tile, copies, n_state, base, n_own, per_micro, *refs):
    refs = list(refs)
    x_ref, w_up_in, w_dn_in = refs[:3]
    refs = refs[3:]
    n_copy = len(copies)
    copy_refs, refs = refs[:n_copy], refs[n_copy:]
    state_in, refs = refs[:n_state], refs[n_state:]
    if has_prev:
        refs.pop(0)
    out_ref, y_ref, refs = refs[0], refs[1], refs[2:]
    state_out, refs = refs[:n_state], refs[n_state:]
    w_up_t, w_dn_t, hidden_ref, y_buf, y_sem, wt_sem, in_sem, out_sem, state_sem, *refs = refs
    copy_bufs, state_buf = refs[:n_copy], refs[n_copy:]
    mine = lax.axis_index('stage')
    step, n_steps = pl.program_id(0), pl.num_programs(0)
    slot = lax.rem(step, 2)

    def y_copy(which):
        return pltpu.make_async_copy(y_buf.at[which], out_ref.at[tile_place(n_own, per_micro, mine, base + step)], y_sem.at[which])

    def enter(index, turn):
        _, _, _, share = copies[index]
        slot = lax.rem(turn, 2)
        return pltpu.make_async_copy(copy_refs[index].at[pl.ds(turn * share, share)], copy_bufs[index].at[slot], in_sem.at[index, slot])

    def leave(index, turn):
        from_peer, first, _, share = copies[index]
        slot = lax.rem(turn, 2)
        owner = 1 - mine if from_peer else mine
        return [pltpu.make_async_copy(copy_bufs[index].at[slot, tile], out_ref.at[tile_place(n_own, per_micro, owner, first + turn * share + tile)],
                                      out_sem.at[index, slot, tile]) for tile in range(share)]

    def weight_copies(block):
        return [pltpu.make_async_copy(src.at[block], dst.at[block], wt_sem.at[block, kind])
                for kind, (src, dst) in enumerate(((w_up_in, w_up_t), (w_dn_in, w_dn_t)))]

    def state_copies(leaving):
        pairs = zip(state_buf, state_out) if leaving else zip(state_in, state_buf)
        return [pltpu.make_async_copy(src, dst, state_sem.at[index]) for index, (src, dst) in enumerate(pairs)]

    def for_copies(turn, action):
        for index in range(n_copy):
            pl.when(jnp.logical_and(turn >= 0, turn * copies[index][3] < copies[index][2]))(functools.partial(action, index, turn))

    def leave_start(index, turn):
        enter(index, turn).wait()
        start_all(leave(index, turn))

    pl.when(step == 0)(lambda: start_all(weight_copies(0) + weight_copies(1) + state_copies(False)))
    for_copies(step - 1, leave_start)
    for_copies(step - 2, lambda index, turn: wait_all(leave(index, turn)))
    for_copies(step, lambda index, turn: enter(index, turn).start())
    pl.when(step >= 2)(lambda: y_copy(slot).wait())
    if n_state:
        @pl.when(step == 1)
        def _():
            wait_all(state_copies(False))
            start_all(state_copies(True))

    pl.when(step == 0)(lambda: wait_all(weight_copies(0) + weight_copies(1)))
    cols = x_ref[0]
    for block in range(2):
        cols = tile_forward(cols, w_up_t.at[block], w_dn_t.at[block], hidden_ref.at[block], ff_tile)
    y_buf[slot] = cols
    y_ref[0] = cols
    y_copy(slot).start()

    @pl.when(step == n_steps - 1)
    def _():
        for_copies(step - 1, lambda index, turn: wait_all(leave(index, turn)))
        y_copy(slot).wait()
        y_copy(1 - slot).wait()
        wait_all(state_copies(True))


def forward_chunk(base, n_chunk, ff_tile, micro_t, w_up_t, w_down_t, prev_out, copied, states):
    n_micro, width, n_rows = micro_t.shape
    n_own, per_micro = n_micro // 2, n_rows // ROW_TILE
    ff_width = w_up_t.shape[1]
    any_spec = pl.BlockSpec(memory_space=pl.ANY)
    scalar = jnp.full((1,), lax.axis_index('stage') * n_own, jnp.int32)
    in_specs = [pl.BlockSpec((1, width, ROW_TILE), lambda i, first: (first[0] + (base + i) // per_micro, 0, lax.rem(base + i, per_micro)))]
    operands = [micro_t, w_up_t, w_down_t] + [array for array, _, _ in copied] + list(states)
    in_specs += [any_spec] * (len(operands) - 1)
    aliases = {}
    if prev_out is not None:
        in_specs.append(any_spec)
        operands.append(prev_out)
        aliases = {len(operands): 0}
    copies = []
    for array, from_peer, first in copied:
        count = array.shape[0]
        share = min(size for size in range(1, count + 1) if count % size == 0 and count // size < n_chunk)
        copies.append((from_peer, first, count, share))
    max_share = max([1] + [share for *_, share in copies])
    dma = pltpu.SemaphoreType.DMA

    def body(first, *refs):
        forward_kernel(prev_out is not None, ff_tile, copies, len(states), base, n_own, per_micro, *refs)

    return pl.pallas_call(
        body,
        grid_spec=pltpu.PrefetchScalarGridSpec(
            num_scalar_prefetch=1, grid=(n_chunk,), in_specs=in_specs,
            out_specs=[any_spec, pl.BlockSpec((1, width, ROW_TILE), lambda i, first: (i, 0, 0))] + [any_spec] * len(states),
            scratch_shapes=[pltpu.VMEM(w_up_t.shape, jnp.bfloat16), pltpu.VMEM(w_down_t.shape, jnp.bfloat16),
                            pltpu.VMEM((2, ff_width, ROW_TILE), jnp.bfloat16), pltpu.VMEM((2, width, ROW_TILE), jnp.bfloat16),
                            dma((2,)), dma((2, 2)), dma((2, 2)), dma((2, 2, max_share)), dma((6,))]
            + [pltpu.VMEM((2, share, width, ROW_TILE), jnp.bfloat16) for *_, share in copies]
            + [pltpu.VMEM(array.shape, array.dtype) for array in states]),
        out_shape=[jax.ShapeDtypeStruct(micro_t.shape, jnp.bfloat16),
                   jax.ShapeDtypeStruct((n_chunk, width, ROW_TILE), jnp.bfloat16)]
        + [jax.ShapeDtypeStruct(array.shape, array.dtype) for array in states],
        input_output_aliases=aliases,
        compiler_params=pltpu.CompilerParams(dimension_semantics=("arbitrary",), vmem_limit_bytes=VMEM_LIMIT),
        cost_estimate=pl.CostEstimate(flops=8 * n_chunk * ROW_TILE * width * ff_width, bytes_accessed=n_chunk * ROW_TILE * width,
                                      transcendentals=0),
        name=f"fwd_{base}",
    )(scalar, *operands)


def place_tiles(out, tiles, first, n_own):
    count, per_micro = tiles.shape[0], out.shape[2] // ROW_TILE
    any_spec = pl.BlockSpec(memory_space=pl.ANY)

    def body(tiles_ref, old_ref, out_ref, buf, in_sem, out_sem):
        owner = 1 - lax.axis_index('stage')
        enter = [pltpu.make_async_copy(tiles_ref.at[tile], buf.at[tile], in_sem.at[tile]) for tile in range(count)]
        leave = [pltpu.make_async_copy(buf.at[tile], out_ref.at[tile_place(n_own, per_micro, owner, first + tile)], out_sem.at[tile])
                 for tile in range(count)]
        start_all(enter)
        for tile in range(count):
            enter[tile].wait()
            leave[tile].start()
        wait_all(leave)

    return pl.pallas_call(
        body, in_specs=[any_spec] * 2, out_specs=any_spec, out_shape=jax.ShapeDtypeStruct(out.shape, out.dtype),
        scratch_shapes=[pltpu.VMEM(tiles.shape, tiles.dtype), pltpu.SemaphoreType.DMA((count,)), pltpu.SemaphoreType.DMA((count,))],
        input_output_aliases={1: 0}, compiler_params=pltpu.CompilerParams(vmem_limit_bytes=VMEM_LIMIT), name=f"place_{first}")(tiles, out)


def forward_rest(micro_t, w_up_t, w_down_t, own_first, peer_first, states):
    n_own = micro_t.shape[0] // 2
    out, base = None, own_first.shape[0]
    received, results = [], []
    for number, (n_chunk, ff_tile) in enumerate(CHUNKS):
        copied, passed = [], []
        if number == 0:
            copied, passed = [(own_first, False, 0), (peer_first, True, 0)], states
        elif number >= 2:
            copied = [received.pop(0)]
        out, part, *handed = forward_chunk(base, n_chunk, ff_tile, micro_t, w_up_t, w_down_t, out, copied, passed)
        results += handed
        received.append((lax.ppermute(part, 'stage', [(0, 1), (1, 0)]), True, base))
        base += n_chunk
    for tiles, _, first in received:
        out = place_tiles(out, tiles, first, n_own)
    return jnp.swapaxes(out, 1, 2), results


def gelu_pair(pre_act):
    square = pre_act * pre_act
    tanh_in = jnp.tanh(pre_act * (GELU_LIN + GELU_CUB * square))
    half = 0.5 * pre_act
    value = half + half * tanh_in
    slope = 0.5 + 0.5 * tanh_in + half * (1.0 - tanh_in * tanh_in) * (GELU_LIN + 3.0 * GELU_CUB * square)
    return value, slope


def update_kernel(n_data, mst_up, mst_dn, mo1_up, mo2_up, mo1_dn, mo2_dn, cmp_up, cmp_dn, acc_up, acc_dn, acts_in, grad_in,
                  micro_in, rate_ref, norm_ref,
                  new_up, new_dn, out1_up, out2_up, out1_dn, out2_dn, w_up_out, w_dn_out, own_first, peer_first,
                  wts, acts, acts_row, grad, grad_row, d_pre, sums, part, fwd_up, fwd_dn, last_up, last_dn,
                  norm_tiles, turned, hidden_ref, send_sem, recv_sem, load_sem, store_sem, tile_sem):
    chip = lax.axis_index('data')
    core = lax.axis_index('stage')
    peer = 1 - core
    pos_x, pos_y = lax.rem(chip, 2), chip // 2
    chip_x = pos_y * 2 + (1 - pos_x)
    chip_y = (1 - pos_y) * 2 + pos_x
    chip_d = 3 - chip
    me = chip * 2 + core
    n_dev = 2 * n_data
    half_rows = grad.shape[1]
    width, ff_width = wts.shape[2:]
    up_rows, dn_cols = last_up.shape[0], last_dn.shape[1]
    n_own = micro_in.shape[0] // 2
    n_sub = GRAD_HALF // GRAD_TILE
    halves = (1 - pos_y, pos_y)

    def cols_of(index, size):
        return pl.ds(pl.multiple_of(index * size, size), size)

    def rows_of(index):
        return pl.ds(pl.multiple_of(index * up_rows, 8), up_rows)

    def remote(src, dst, index, device):
        return pltpu.make_async_remote_copy(src_ref=src, dst_ref=dst, send_sem=send_sem.at[index], recv_sem=recv_sem.at[index],
                                            device_id=device, device_id_type=MESH_ID)

    to_peer, to_x, to_y = (chip, peer), (chip_x, core), (chip_y, core)

    up_state = [part.at[0, index * up_rows:(index + 1) * up_rows] for index in range(3)]
    dn_state = [part.at[1, :, index * dn_cols:(index + 1) * dn_cols] for index in range(3)]
    loads = [pltpu.make_async_copy(src, dst, load_sem.at[index]) for index, (src, dst) in enumerate([
        (grad_in.at[:, cols_of(core, half_rows)], grad), (acts_in.at[:, cols_of(core, half_rows)], acts.at[core]),
        (cmp_up, wts.at[core, 0]), (cmp_dn, wts.at[core, 1]),
        (acc_up, sums.at[core, 0]), (acc_dn, sums.at[core, 1]),
        *zip((mst_up, mo1_up, mo2_up), up_state), *zip((mst_dn, mo1_dn, mo2_dn), dn_state)])]
    for copy in loads[:6]:
        copy.start()

    barrier = pltpu.get_barrier_semaphore()
    for offset in range(1, n_dev):
        other = lax.rem(me + offset, n_dev)
        pl.semaphore_signal(barrier, inc=1, device_id=(other // 2, lax.rem(other, 2)), device_id_type=MESH_ID)
    pl.semaphore_wait(barrier, n_dev - 1)

    swap_acts = remote(acts_in.at[:, cols_of(peer, half_rows)], acts.at[core], 0, to_peer)
    def swap_piece(kind, tile):
        cols = cols_of(halves[0] * n_sub + tile, GRAD_TILE)
        return remote((cmp_up, cmp_dn)[kind].at[:, cols], wts.at[core, kind, :, cols], 1 + kind * n_sub + tile, to_peer)

    swap_late = [remote((cmp_up, cmp_dn)[kind].at[:, cols_of(halves[1], GRAD_HALF)], wts.at[core, kind, :, cols_of(halves[1], GRAD_HALF)],
                        1 + 2 * n_sub + kind, to_peer) for kind in range(2)]
    swap_acts.start()
    for tile in range(n_sub):
        for kind in range(2):
            swap_piece(kind, tile).start()
    for copy in swap_late:
        copy.start()

    def part_copy(kind, step):
        late = step // n_sub
        cols = cols_of((1 - pos_y + late * (2 * pos_y - 1)) * n_sub + lax.rem(step, n_sub), GRAD_TILE)
        return remote(sums.at[peer, kind, :, cols], part.at[kind, :, cols], 9 + kind * 2 * n_sub + step, to_peer)

    up_first = [[remote(sums.at[core, 0, rows_of(row * 2 + 1 - pos_x), cols_of(half, GRAD_HALF)],
                        fwd_up.at[slot, :, cols_of(half, GRAD_HALF)], 21 + order * 2 + slot, to_x)
                 for slot, row in enumerate(halves)] for order, half in enumerate(halves)]
    dn_first = [remote(sums.at[core, 1, :, cols_of((1 - pos_y) * 2 + col, dn_cols)], fwd_dn.at[slot], 25 + slot, to_y)
                for slot, col in enumerate((1 - pos_x, pos_x))]
    up_next = [remote(sums.at[core, 0, rows_of(chip_y), cols_of(half, GRAD_HALF)], last_up.at[:, cols_of(half, GRAD_HALF)],
                      27 + order, to_y) for order, half in enumerate(halves)]
    dn_next = remote(sums.at[core, 1, :, cols_of(chip_x, dn_cols)], last_dn, 29, to_x)

    def add_up(index, order):
        cols = cols_of(halves[order], GRAD_HALF)
        sums[core, 0, rows_of(index), cols] += part[0, rows_of(index), cols]

    def add_dn(index):
        cols = cols_of(index, dn_cols)
        sums[core, 1, :, cols] += part[1, :, cols]

    def scatter_half(order):
        for kind in range(2):
            for tile in range(n_sub):
                part_copy(kind, order * n_sub + tile).wait_recv()
        for slot in range(2):
            add_up((halves[slot]) * 2 + 1 - pos_x, order)
            up_first[order][slot].start()
            if order == 0:
                add_dn((1 - pos_y) * 2 + (1 - pos_x if slot == 0 else pos_x))
                dn_first[slot].start()
        add_up(chip_y, order)
        if order == 1:
            add_dn(chip_x)
            add_dn(chip)
        add_up(chip, order)

    loads[0].wait()
    for block in (1, 0):
        own = core == block

        @pl.when(own)
        def _():
            for copy in loads[1:4]:
                copy.wait()

        @pl.when(jnp.logical_not(own))
        def _():
            swap_acts.wait_recv()

        acts_row[...] = acts[block].T
        grad_row[...] = grad[...].T
        def tile_step(step, carry, block=block, own=own):
            late = step // n_sub
            cols = cols_of((1 - pos_y + late * (2 * pos_y - 1)) * n_sub + lax.rem(step, n_sub), GRAD_TILE)

            @pl.when(jnp.logical_and(jnp.logical_not(own), step < n_sub))
            def _():
                swap_piece(0, step).wait_recv()
                swap_piece(1, step).wait_recv()

            @pl.when(jnp.logical_and(jnp.logical_not(own), step == n_sub))
            def _():
                for copy in swap_late:
                    copy.wait_recv()

            half, at_step = (0, 2 * n_sub - 1) if block == 1 else (1, n_sub)
            pl.when(jnp.logical_and(core == 1, step == at_step))(functools.partial(scatter_half, half))

            pre_act = jnp.dot(acts_row[...], wts[block, 0, :, cols], preferred_element_type=jnp.float32)
            d_hidden = jnp.dot(grad_row[...], wts[block, 1, :, cols], preferred_element_type=jnp.float32)
            hidden, slope = gelu_pair(pre_act)
            dw_down = jnp.dot(grad[...], hidden.astype(jnp.bfloat16), preferred_element_type=jnp.float32)
            d_tile = (d_hidden * slope).astype(jnp.bfloat16)
            if block == 1:
                d_pre[:, cols] = d_tile
            dw_up = jnp.dot(acts[block], d_tile, preferred_element_type=jnp.float32)

            @pl.when(jnp.logical_and(own, step == 0))
            def _():
                for copy in loads[4:6]:
                    copy.wait()

            @pl.when(own)
            def _():
                sums[block, 0, :, cols] += dw_up
                sums[block, 1, :, cols] += dw_down

            @pl.when(jnp.logical_not(own))
            def _():
                sums[block, 0, :, cols] = dw_up
                sums[block, 1, :, cols] = dw_down
                part_copy(0, step).start()
                part_copy(1, step).start()
            return carry

        lax.fori_loop(0, 2 * n_sub, tile_step, 0)
        if block == 1:
            d_in = lax.dot_general(wts[1, 0], d_pre[...], (((1,), (1,)), ((), ())), preferred_element_type=jnp.float32)
            grad[...] = (grad[...].astype(jnp.float32) + d_in).astype(jnp.bfloat16)

    @pl.when(core == 0)
    def _():
        scatter_half(0)
        scatter_half(1)

    for copy in loads[6:]:
        copy.start()

    n_slot = 2 * half_rows // ROW_TILE
    per_micro = micro_in.shape[2] // ROW_TILE

    def x_slot(tile):
        slot = lax.rem(tile, n_slot)
        return acts.at[slot // 2, :, cols_of(lax.rem(slot, 2), ROW_TILE)]

    def x_load(tile):
        return pltpu.make_async_copy(micro_in.at[tile_place(n_own, per_micro, core, tile)], x_slot(tile), tile_sem.at[0, lax.rem(tile, n_slot)])

    start_all([x_load(tile) for tile in range(n_slot)])

    up_first[0][0].wait_recv()
    cols = cols_of(halves[0], GRAD_HALF)
    sums[core, 0, rows_of(chip_y), cols] += fwd_up[0, :, cols]
    up_next[0].start()
    dn_first[0].wait_recv()
    sums[core, 1, :, cols_of(chip_x, dn_cols)] += fwd_dn[0]
    dn_next.start()
    up_first[1][0].wait_recv()
    cols = cols_of(halves[1], GRAD_HALF)
    sums[core, 0, rows_of(chip_y), cols] += fwd_up[0, :, cols]
    up_next[1].start()
    for order in range(2):
        up_first[order][1].wait_recv()
        up_next[order].wait_recv()
    dn_first[1].wait_recv()
    scale = 1.0 / n_data
    mean_up = (sums[core, 0, rows_of(chip)] + fwd_up[1] + last_up[...]) * scale
    last_up[...] = mean_up
    square = jnp.sum((mean_up * mean_up).reshape(up_rows // 8, 8, ff_width), axis=0)
    dn_next.wait_recv()
    mean_dn = (sums[core, 1, :, cols_of(chip, dn_cols)] + fwd_dn[1] + last_dn[...]) * scale
    last_dn[...] = mean_dn
    square_dn = jnp.sum((mean_dn * mean_dn).reshape(width // 8, 8, dn_cols), axis=0)
    tile_sum = sum(square[:, first:first + 128] for first in range(0, ff_width, 128))
    tile_sum = tile_sum + sum(square_dn[:, first:first + 128] for first in range(0, dn_cols, 128))
    norm_tiles[me] = tile_sum
    norm_copies = []
    for offset in range(1, n_dev):
        other = lax.rem(me + offset, n_dev)
        norm_copies.append(remote(norm_tiles.at[me], norm_tiles.at[me], 29 + offset, (other // 2, lax.rem(other, 2))))
    for copy in norm_copies:
        copy.start()
    for copy in loads[6:]:
        copy.wait()
    for copy in norm_copies:
        copy.wait_recv()
    total_sq = jnp.sum(jnp.sum(norm_tiles[...], axis=0), keepdims=True)
    clip = jnp.minimum(1.0, norm_ref[0] / (jnp.sqrt(total_sq) + NORM_EPS))
    rate = rate_ref[0]

    chips = (chip, chip_x, chip_y, chip_d)
    up_at = [wts.at[core, 0, rows_of(index)] for index in chips]
    dn_at = [wts.at[core, 1, :, cols_of(index, dn_cols)] for index in chips]
    up_x, up_y, up_relay = remote(up_at[0], up_at[0], 37, to_x), remote(up_at[0], up_at[0], 38, to_y), remote(up_at[1], up_at[1], 39, to_y)
    dn_x, dn_y, dn_relay = remote(dn_at[0], dn_at[0], 40, to_x), remote(dn_at[0], dn_at[0], 41, to_y), remote(dn_at[2], dn_at[2], 42, to_x)
    up_peer = [remote(up_at[index], up_at[index], 43 + index, to_peer) for index in range(4)]
    dn_peer = [remote(dn_at[index], dn_at[index], 47 + index, to_peer) for index in range(4)]

    def gather_up():
        up_x.start()
        up_y.start()
        up_peer[0].start()

    def gather_dn():
        dn_y.start()
        dn_x.start()
        dn_peer[0].start()

    def gather_relay():
        up_x.wait_recv()
        up_relay.start()
        up_peer[1].start()
        dn_y.wait_recv()
        dn_relay.start()
        dn_peer[2].start()

    def gather_near():
        up_y.wait_recv()
        up_peer[2].start()
        dn_x.wait_recv()
        dn_peer[1].start()

    def gather_far():
        up_relay.wait_recv()
        up_peer[3].start()
        dn_relay.wait_recv()
        dn_peer[3].start()

    def gather_peer():
        for copy in up_peer + dn_peer:
            copy.wait_recv()

    state = adamw_update(*[ref[...] for ref in up_state], clip * last_up[...], rate)
    wts[core, 0, rows_of(chip)] = state[0].astype(jnp.bfloat16)
    for ref, value in zip(up_state, state):
        ref[...] = value
    pl.when(core == 0)(gather_up)
    state = adamw_update(*[ref[...] for ref in dn_state], clip * last_dn[...], rate)
    wts[core, 1, :, cols_of(chip, dn_cols)] = state[0].astype(jnp.bfloat16)
    for ref, value in zip(dn_state, state):
        ref[...] = value
    pl.when(core == 0)(gather_dn)
    stores = [pltpu.make_async_copy(src, dst, store_sem.at[index]) for index, (src, dst) in enumerate([
        *zip(up_state, (new_up, out1_up, out2_up)), *zip(dn_state, (new_dn, out1_dn, out2_dn))])]
    for copy in stores:
        copy.start()

    @pl.when(core == 0)
    def _():
        gather_relay()
        gather_near()
        gather_far()

    @pl.when(core == 1)
    def _():
        gather_peer()
        gather_up()
        gather_dn()

    swap_acts.wait_send()
    for order in range(2):
        for copy in up_first[order] + [up_next[order]]:
            copy.wait_send()
        for kind in range(2):
            for tile in range(n_sub):
                part_copy(kind, order * n_sub + tile).wait_send()
    for copy in dn_first + [dn_next] + norm_copies + swap_late + [swap_piece(kind, tile) for kind in range(2) for tile in range(n_sub)]:
        copy.wait_send()

    def weights_out(block):
        return [pltpu.make_async_copy(turned.at[block], w_up_out.at[block], store_sem.at[6 + block]),
                pltpu.make_async_copy(wts.at[block, 1], w_dn_out.at[block], store_sem.at[8 + block])]

    n_first = own_first.shape[0]
    per_row = ff_width // ROW_TILE

    def mid_slot(tile):
        row = tile // per_row
        return row // 2, lax.rem(row, 2), slice(None), cols_of(lax.rem(tile, per_row), ROW_TILE)

    turned[0] = wts[0, 0].T
    start_all(weights_out(0))

    def first_block(pair, carry):
        for number, action in ((2, gather_relay), (3, gather_near), (4, gather_far)):
            pl.when(jnp.logical_and(core == 1, pair == number))(action)
        tiles = (2 * pair, 2 * pair + 1)
        wait_all([x_load(tile) for tile in tiles])
        for half, tile in enumerate(tiles):
            mid = tile_forward(x_slot(tile)[...], turned.at[0], wts.at[0, 1], hidden_ref.at[half], FF_TILE)
            sums[mid_slot(tile)] = mid.astype(jnp.float32)
        pl.when(tiles[1] + n_slot < N_MID)(lambda: start_all([x_load(tile + n_slot) for tile in tiles]))
        return carry

    lax.fori_loop(0, N_MID // 2, first_block, 0)
    pl.when(core == 0)(gather_peer)
    turned[1] = wts[1, 0].T
    start_all(weights_out(1))

    def y_out(tile):
        slot = lax.rem(tile, n_slot)
        keep = pltpu.make_async_copy(x_slot(tile), own_first.at[tile], tile_sem.at[1, slot])
        give = pltpu.make_async_remote_copy(src_ref=x_slot(tile), dst_ref=peer_first.at[tile], send_sem=tile_sem.at[2, slot],
                                            recv_sem=recv_sem.at[51 + tile], device_id=to_peer, device_id_type=MESH_ID)
        return keep, give

    def y_wait(tile):
        keep, give = y_out(tile)
        keep.wait()
        give.wait_send()

    def second_block(pair, carry):
        tiles = (2 * pair, 2 * pair + 1)
        for tile in tiles:
            pl.when(pair >= 2)(functools.partial(y_wait, tile - n_slot))
        for half, tile in enumerate(tiles):
            place = x_slot(tile)
            place[...] = tile_forward(sums[mid_slot(tile)].astype(jnp.bfloat16), turned.at[1], wts.at[1, 1], hidden_ref.at[half], FF_TILE)
        for tile in tiles:
            start_all(y_out(tile))
        return carry

    n_late = ff_width // ROW_TILE

    def late_slot(tile):
        return d_pre.at[0:width, cols_of(lax.rem(tile, n_late), ROW_TILE)]

    def late_load(tile):
        return pltpu.make_async_copy(micro_in.at[tile_place(n_own, per_micro, core, tile)], late_slot(tile), tile_sem.at[3, lax.rem(tile, n_late)])

    def whole_tile(tile, carry):
        y_wait(tile - n_slot)
        late_load(tile).wait()
        cols = late_slot(tile)[...]
        for block in range(2):
            cols = tile_forward(cols, turned.at[block], wts.at[block, 1], hidden_ref.at[block], FF_TILE)
        place = x_slot(tile)
        place[...] = cols
        start_all(y_out(tile))
        pl.when(tile + n_late < n_first)(lambda: late_load(tile + n_late).start())
        return carry

    start_all([late_load(N_MID + tile) for tile in range(n_late)])
    lax.fori_loop(0, N_MID // 2, second_block, 0)
    lax.fori_loop(N_MID, n_first, whole_tile, 0)
    for tile in range(n_first - n_slot, n_first):
        y_wait(tile)
    for tile in range(n_first):
        y_out(tile)[1].wait_recv()

    for copy in [up_x, up_y, up_relay, dn_x, dn_y, dn_relay] + up_peer + dn_peer:
        copy.wait_send()
    for copy in stores + weights_out(0) + weights_out(1):
        copy.wait()


def update_weights(n_data, arrays, learn_rate, max_norm):
    width, ff_width = arrays[6].shape
    n_rows = arrays[11].shape[1]
    half_rows = n_rows // 2
    up_rows, dn_cols = arrays[0].shape[0], arrays[1].shape[1]
    f32, bf16 = jnp.float32, jnp.bfloat16
    up_state, dn_state = jax.ShapeDtypeStruct((up_rows, ff_width), f32), jax.ShapeDtypeStruct((width, dn_cols), f32)
    first = jax.ShapeDtypeStruct((N_FIRST, width, ROW_TILE), bf16)
    any_spec = pl.BlockSpec(memory_space=pl.ANY)
    smem_spec = pl.BlockSpec(memory_space=pltpu.SMEM)
    n_sem = 51 + N_FIRST

    def body(*refs):
        update_kernel(n_data, *refs)

    flops = 20 * half_rows * width * ff_width + 8 * N_FIRST * ROW_TILE * width * ff_width
    return pl.pallas_call(
        body,
        in_specs=[any_spec] * 13 + [smem_spec] * 2,
        out_specs=[any_spec] * 10,
        out_shape=[up_state, dn_state, up_state, up_state, dn_state, dn_state,
                   jax.ShapeDtypeStruct((2, ff_width, width), bf16), jax.ShapeDtypeStruct((2, width, ff_width), bf16), first, first],
        scratch_shapes=[
            pltpu.VMEM((2, 2, width, ff_width), bf16), pltpu.VMEM((2, width, half_rows), bf16),
            pltpu.VMEM((half_rows, width), bf16), pltpu.VMEM((width, half_rows), bf16), pltpu.VMEM((half_rows, width), bf16),
            pltpu.VMEM((half_rows, ff_width), bf16), pltpu.VMEM((2, 2, width, ff_width), f32), pltpu.VMEM((2, width, ff_width), f32),
            pltpu.VMEM((2, up_rows, ff_width), f32), pltpu.VMEM((2, width, dn_cols), f32),
            pltpu.VMEM((up_rows, ff_width), f32), pltpu.VMEM((width, dn_cols), f32), pltpu.VMEM((2 * n_data, 8, 128), f32),
            pltpu.VMEM((2, ff_width, width), bf16), pltpu.VMEM((2, ff_width, ROW_TILE), bf16),
            pltpu.SemaphoreType.DMA((n_sem,)), pltpu.SemaphoreType.DMA((n_sem,)), pltpu.SemaphoreType.DMA((12,)),
            pltpu.SemaphoreType.DMA((10,)), pltpu.SemaphoreType.DMA((4, 4))],
        compiler_params=pltpu.CompilerParams(collective_id=0, has_side_effects=True, vmem_limit_bytes=VMEM_LIMIT),
        cost_estimate=pl.CostEstimate(flops=flops, bytes_accessed=60000000, transcendentals=0),
        name="update",
    )(*arrays, learn_rate.reshape(1), max_norm.reshape(1))


def solution(mesh):
    n_data = mesh.shape['data']

    def step_body(master_up, master_down, moment1_up, moment2_up, moment1_down, moment2_down,
                  compute_up, compute_down, accum_up, accum_down, stage_acts, loss_grad, next_micro,
                  learn_rate, max_norm):
        arrays = (master_up[0], master_down[0].T, moment1_up[0], moment2_up[0], moment1_down[0].T, moment2_down[0].T,
                  compute_up[0], compute_down[0].T, accum_up[0, 0], accum_down[0, 0].T, stage_acts[0].T, loss_grad.T,
                  jnp.swapaxes(next_micro, 1, 2))
        *states, w_up_t, w_dn_t, own_first, peer_first = update_weights(n_data, arrays, learn_rate, max_norm)
        last_acts, states = forward_rest(arrays[12], w_up_t, w_dn_t, own_first, peer_first, states)
        new_up, new_dn, out1_up, out2_up, out1_dn, out2_dn = states
        return (new_up[None], new_dn.T[None], out1_up[None], out2_up[None], out1_dn.T[None], out2_dn.T[None], last_acts)

    shard_spec = P('stage', 'data', None)
    whole_spec = P('stage', None, None)
    accum_spec = P('data', 'stage', None, None)
    micro_spec = P(None, 'data', None)
    in_specs = (shard_spec,) * 6 + (whole_spec, whole_spec, accum_spec, accum_spec,
                                    P('stage', 'data', None), P('data', None), micro_spec, P(), P())
    out_specs = (shard_spec,) * 6 + (micro_spec,)
    return jax.shard_map(step_body, mesh=mesh, in_specs=in_specs, out_specs=out_specs, check_vma=False)
```

```python
import functools

import jax
import jax.numpy as jnp
from jax import lax
from jax.experimental import pallas as pl
from jax.experimental.pallas import tpu as pltpu
from jax.sharding import PartitionSpec as P

BETA_ONE = 0.9
BETA_TWO = 0.95
ADAM_EPS = 1e-8
WEIGHT_DECAY = 0.1
NORM_EPS = 1e-6
STEP_NUM = 10
BIAS_ONE = 1.0 - BETA_ONE ** STEP_NUM
BIAS_TWO = 1.0 - BETA_TWO ** STEP_NUM


def adamw_update(master, moment_one, moment_two, grad_step, learn_rate):
    mom_one = BETA_ONE * moment_one + (1.0 - BETA_ONE) * grad_step
    mom_two = BETA_TWO * moment_two + (1.0 - BETA_TWO) * grad_step * grad_step
    step_dir = (mom_one / BIAS_ONE) / (jnp.sqrt(mom_two / BIAS_TWO) + ADAM_EPS)
    new_master = master - learn_rate * (step_dir + WEIGHT_DECAY * master)
    return new_master, mom_one, mom_two


MESH_ID = pl.DeviceIdType.MESH
GRAD_HALF = 768
GRAD_TILE = 256
GELU_LIN = 0.7978845608028654
GELU_CUB = GELU_LIN * 0.044715
ROW_TILE = 512
FF_TILE = 256
CHUNKS = ((10, 256), (2, 256))
N_MID = 12
N_FIRST = 20
VMEM_LIMIT = 67000000


def gelu_half(pre_act):
    inner = pre_act * (GELU_LIN + GELU_CUB * (pre_act * pre_act))
    half = 0.5 * pre_act
    return half + half * jnp.tanh(inner)


def tile_forward(cols_in, w_up_t, w_down_t, hidden_ref, ff_tile):
    for start in range(0, hidden_ref.shape[0], ff_tile):
        rows = pl.ds(start, ff_tile)
        pre_act = jnp.dot(w_up_t[rows, :], cols_in, preferred_element_type=jnp.float32)
        hidden_ref[rows, :] = gelu_half(pre_act).astype(jnp.bfloat16)
    branch = jnp.dot(w_down_t[...], hidden_ref[...], preferred_element_type=jnp.float32)
    return (cols_in.astype(jnp.float32) + branch).astype(jnp.bfloat16)


def tile_place(n_own, per_micro, owner, tile):
    return owner * n_own + tile // per_micro, slice(None), pl.ds(pl.multiple_of(lax.rem(tile, per_micro) * ROW_TILE, ROW_TILE), ROW_TILE)


def start_all(copies):
    for copy in copies:
        copy.start()


def wait_all(copies):
    for copy in copies:
        copy.wait()


def forward_kernel(has_prev, ff_tile, copies, n_state, base, n_own, per_micro, *refs):
    refs = list(refs)
    x_ref, w_up_in, w_dn_in = refs[:3]
    refs = refs[3:]
    n_copy = len(copies)
    copy_refs, refs = refs[:n_copy], refs[n_copy:]
    state_in, refs = refs[:n_state], refs[n_state:]
    if has_prev:
        refs.pop(0)
    out_ref, y_ref, refs = refs[0], refs[1], refs[2:]
    state_out, refs = refs[:n_state], refs[n_state:]
    w_up_t, w_dn_t, hidden_ref, y_buf, y_sem, wt_sem, in_sem, out_sem, state_sem, *refs = refs
    copy_bufs, state_buf = refs[:n_copy], refs[n_copy:]
    mine = lax.axis_index('stage')
    step, n_steps = pl.program_id(0), pl.num_programs(0)
    slot = lax.rem(step, 2)

    def y_copy(which):
        return pltpu.make_async_copy(y_buf.at[which], out_ref.at[tile_place(n_own, per_micro, mine, base + step)], y_sem.at[which])

    def enter(index, turn):
        _, _, _, share = copies[index]
        slot = lax.rem(turn, 2)
        return pltpu.make_async_copy(copy_refs[index].at[pl.ds(turn * share, share)], copy_bufs[index].at[slot], in_sem.at[index, slot])

    def leave(index, turn):
        from_peer, first, _, share = copies[index]
        slot = lax.rem(turn, 2)
        owner = 1 - mine if from_peer else mine
        return [pltpu.make_async_copy(copy_bufs[index].at[slot, tile], out_ref.at[tile_place(n_own, per_micro, owner, first + turn * share + tile)],
                                      out_sem.at[index, slot, tile]) for tile in range(share)]

    def weight_copies(block):
        return [pltpu.make_async_copy(src.at[block], dst.at[block], wt_sem.at[block, kind])
                for kind, (src, dst) in enumerate(((w_up_in, w_up_t), (w_dn_in, w_dn_t)))]

    def state_copies(leaving):
        pairs = zip(state_buf, state_out) if leaving else zip(state_in, state_buf)
        return [pltpu.make_async_copy(src, dst, state_sem.at[index]) for index, (src, dst) in enumerate(pairs)]

    def for_copies(turn, action):
        for index in range(n_copy):
            pl.when(jnp.logical_and(turn >= 0, turn * copies[index][3] < copies[index][2]))(functools.partial(action, index, turn))

    def leave_start(index, turn):
        enter(index, turn).wait()
        start_all(leave(index, turn))

    pl.when(step == 0)(lambda: start_all(weight_copies(0) + weight_copies(1) + state_copies(False)))
    for_copies(step - 1, leave_start)
    for_copies(step - 2, lambda index, turn: wait_all(leave(index, turn)))
    for_copies(step, lambda index, turn: enter(index, turn).start())
    pl.when(step >= 2)(lambda: y_copy(slot).wait())
    if n_state:
        @pl.when(step == 1)
        def _():
            wait_all(state_copies(False))
            start_all(state_copies(True))

    pl.when(step == 0)(lambda: wait_all(weight_copies(0) + weight_copies(1)))
    cols = x_ref[0]
    for block in range(2):
        cols = tile_forward(cols, w_up_t.at[block], w_dn_t.at[block], hidden_ref.at[block], ff_tile)
    y_buf[slot] = cols
    y_ref[0] = cols
    y_copy(slot).start()

    @pl.when(step == n_steps - 1)
    def _():
        for_copies(step - 1, lambda index, turn: wait_all(leave(index, turn)))
        y_copy(slot).wait()
        y_copy(1 - slot).wait()
        wait_all(state_copies(True))


def forward_chunk(base, n_chunk, ff_tile, micro_t, w_up_t, w_down_t, prev_out, copied, states):
    n_micro, width, n_rows = micro_t.shape
    n_own, per_micro = n_micro // 2, n_rows // ROW_TILE
    ff_width = w_up_t.shape[1]
    any_spec = pl.BlockSpec(memory_space=pl.ANY)
    scalar = jnp.full((1,), lax.axis_index('stage') * n_own, jnp.int32)
    in_specs = [pl.BlockSpec((1, width, ROW_TILE), lambda i, first: (first[0] + (base + i) // per_micro, 0, lax.rem(base + i, per_micro)))]
    operands = [micro_t, w_up_t, w_down_t] + [array for array, _, _ in copied] + list(states)
    in_specs += [any_spec] * (len(operands) - 1)
    aliases = {}
    if prev_out is not None:
        in_specs.append(any_spec)
        operands.append(prev_out)
        aliases = {len(operands): 0}
    copies = []
    for array, from_peer, first in copied:
        count = array.shape[0]
        share = min(size for size in range(1, count + 1) if count % size == 0 and count // size < n_chunk)
        copies.append((from_peer, first, count, share))
    max_share = max([1] + [share for *_, share in copies])
    dma = pltpu.SemaphoreType.DMA

    def body(first, *refs):
        forward_kernel(prev_out is not None, ff_tile, copies, len(states), base, n_own, per_micro, *refs)

    return pl.pallas_call(
        body,
        grid_spec=pltpu.PrefetchScalarGridSpec(
            num_scalar_prefetch=1, grid=(n_chunk,), in_specs=in_specs,
            out_specs=[any_spec, pl.BlockSpec((1, width, ROW_TILE), lambda i, first: (i, 0, 0))] + [any_spec] * len(states),
            scratch_shapes=[pltpu.VMEM(w_up_t.shape, jnp.bfloat16), pltpu.VMEM(w_down_t.shape, jnp.bfloat16),
                            pltpu.VMEM((2, ff_width, ROW_TILE), jnp.bfloat16), pltpu.VMEM((2, width, ROW_TILE), jnp.bfloat16),
                            dma((2,)), dma((2, 2)), dma((2, 2)), dma((2, 2, max_share)), dma((6,))]
            + [pltpu.VMEM((2, share, width, ROW_TILE), jnp.bfloat16) for *_, share in copies]
            + [pltpu.VMEM(array.shape, array.dtype) for array in states]),
        out_shape=[jax.ShapeDtypeStruct(micro_t.shape, jnp.bfloat16),
                   jax.ShapeDtypeStruct((n_chunk, width, ROW_TILE), jnp.bfloat16)]
        + [jax.ShapeDtypeStruct(array.shape, array.dtype) for array in states],
        input_output_aliases=aliases,
        compiler_params=pltpu.CompilerParams(dimension_semantics=("arbitrary",), vmem_limit_bytes=VMEM_LIMIT),
        cost_estimate=pl.CostEstimate(flops=8 * n_chunk * ROW_TILE * width * ff_width, bytes_accessed=n_chunk * ROW_TILE * width,
                                      transcendentals=0),
        name=f"fwd_{base}",
    )(scalar, *operands)


def place_tiles(out, tiles, first, n_own):
    count, per_micro = tiles.shape[0], out.shape[2] // ROW_TILE
    any_spec = pl.BlockSpec(memory_space=pl.ANY)

    def body(tiles_ref, old_ref, out_ref, buf, in_sem, out_sem):
        owner = 1 - lax.axis_index('stage')
        enter = [pltpu.make_async_copy(tiles_ref.at[tile], buf.at[tile], in_sem.at[tile]) for tile in range(count)]
        leave = [pltpu.make_async_copy(buf.at[tile], out_ref.at[tile_place(n_own, per_micro, owner, first + tile)], out_sem.at[tile])
                 for tile in range(count)]
        start_all(enter)
        for tile in range(count):
            enter[tile].wait()
            leave[tile].start()
        wait_all(leave)

    return pl.pallas_call(
        body, in_specs=[any_spec] * 2, out_specs=any_spec, out_shape=jax.ShapeDtypeStruct(out.shape, out.dtype),
        scratch_shapes=[pltpu.VMEM(tiles.shape, tiles.dtype), pltpu.SemaphoreType.DMA((count,)), pltpu.SemaphoreType.DMA((count,))],
        input_output_aliases={1: 0}, compiler_params=pltpu.CompilerParams(vmem_limit_bytes=VMEM_LIMIT), name=f"place_{first}")(tiles, out)


def forward_rest(micro_t, w_up_t, w_down_t, own_first, peer_first, states):
    n_own = micro_t.shape[0] // 2
    out, base = None, own_first.shape[0]
    received, results = [], []
    for number, (n_chunk, ff_tile) in enumerate(CHUNKS):
        copied, passed = [], []
        if number == 0:
            copied, passed = [(own_first, False, 0), (peer_first, True, 0)], states
        elif number >= 2:
            copied = [received.pop(0)]
        out, part, *handed = forward_chunk(base, n_chunk, ff_tile, micro_t, w_up_t, w_down_t, out, copied, passed)
        results += handed
        received.append((lax.ppermute(part, 'stage', [(0, 1), (1, 0)]), True, base))
        base += n_chunk
    for tiles, _, first in received:
        out = place_tiles(out, tiles, first, n_own)
    return jnp.swapaxes(out, 1, 2), results


def gelu_pair(pre_act):
    square = pre_act * pre_act
    tanh_in = jnp.tanh(pre_act * (GELU_LIN + GELU_CUB * square))
    half = 0.5 * pre_act
    value = half + half * tanh_in
    slope = 0.5 + 0.5 * tanh_in + half * (1.0 - tanh_in * tanh_in) * (GELU_LIN + 3.0 * GELU_CUB * square)
    return value, slope


def update_kernel(n_data, mst_up, mst_dn, mo1_up, mo2_up, mo1_dn, mo2_dn, cmp_up, cmp_dn, acc_up, acc_dn, acts_in, grad_in,
                  micro_in, rate_ref, norm_ref,
                  new_up, new_dn, out1_up, out2_up, out1_dn, out2_dn, w_up_out, w_dn_out, own_first, peer_first,
                  wts, acts, acts_row, grad, grad_row, d_pre, sums, part, fwd_up, fwd_dn, last_up, last_dn,
                  norm_tiles, turned, hidden_ref, send_sem, recv_sem, load_sem, store_sem, tile_sem):
    chip = lax.axis_index('data')
    core = lax.axis_index('stage')
    peer = 1 - core
    pos_x, pos_y = lax.rem(chip, 2), chip // 2
    chip_x = pos_y * 2 + (1 - pos_x)
    chip_y = (1 - pos_y) * 2 + pos_x
    chip_d = 3 - chip
    me = chip * 2 + core
    n_dev = 2 * n_data
    half_rows = grad.shape[1]
    width, ff_width = wts.shape[2:]
    up_rows, dn_cols = last_up.shape[0], last_dn.shape[1]
    n_own = micro_in.shape[0] // 2
    n_sub = GRAD_HALF // GRAD_TILE
    halves = (1 - pos_y, pos_y)

    def cols_of(index, size):
        return pl.ds(pl.multiple_of(index * size, size), size)

    def rows_of(index):
        return pl.ds(pl.multiple_of(index * up_rows, 8), up_rows)

    def remote(src, dst, index, device):
        return pltpu.make_async_remote_copy(src_ref=src, dst_ref=dst, send_sem=send_sem.at[index], recv_sem=recv_sem.at[index],
                                            device_id=device, device_id_type=MESH_ID)

    to_peer, to_x, to_y = (chip, peer), (chip_x, core), (chip_y, core)

    up_state = [part.at[0, index * up_rows:(index + 1) * up_rows] for index in range(3)]
    dn_state = [part.at[1, :, index * dn_cols:(index + 1) * dn_cols] for index in range(3)]
    loads = [pltpu.make_async_copy(src, dst, load_sem.at[index]) for index, (src, dst) in enumerate([
        (grad_in.at[:, cols_of(core, half_rows)], grad), (acts_in.at[:, cols_of(core, half_rows)], acts.at[core]),
        (cmp_up, wts.at[core, 0]), (cmp_dn, wts.at[core, 1]),
        (acc_up, sums.at[core, 0]), (acc_dn, sums.at[core, 1]),
        *zip((mst_up, mo1_up, mo2_up), up_state), *zip((mst_dn, mo1_dn, mo2_dn), dn_state)])]
    for copy in loads[:6]:
        copy.start()

    barrier = pltpu.get_barrier_semaphore()
    for offset in range(1, n_dev):
        other = lax.rem(me + offset, n_dev)
        pl.semaphore_signal(barrier, inc=1, device_id=(other // 2, lax.rem(other, 2)), device_id_type=MESH_ID)
    pl.semaphore_wait(barrier, n_dev - 1)

    swap_acts = remote(acts_in.at[:, cols_of(peer, half_rows)], acts.at[core], 0, to_peer)
    def swap_piece(kind, tile):
        cols = cols_of(halves[0] * n_sub + tile, GRAD_TILE)
        return remote((cmp_up, cmp_dn)[kind].at[:, cols], wts.at[core, kind, :, cols], 1 + kind * n_sub + tile, to_peer)

    swap_late = [remote((cmp_up, cmp_dn)[kind].at[:, cols_of(halves[1], GRAD_HALF)], wts.at[core, kind, :, cols_of(halves[1], GRAD_HALF)],
                        1 + 2 * n_sub + kind, to_peer) for kind in range(2)]
    swap_acts.start()
    for tile in range(n_sub):
        for kind in range(2):
            swap_piece(kind, tile).start()
    for copy in swap_late:
        copy.start()

    def part_copy(kind, step):
        late = step // n_sub
        cols = cols_of((1 - pos_y + late * (2 * pos_y - 1)) * n_sub + lax.rem(step, n_sub), GRAD_TILE)
        return remote(sums.at[peer, kind, :, cols], part.at[kind, :, cols], 9 + kind * 2 * n_sub + step, to_peer)

    up_first = [[remote(sums.at[core, 0, rows_of(row * 2 + 1 - pos_x), cols_of(half, GRAD_HALF)],
                        fwd_up.at[slot, :, cols_of(half, GRAD_HALF)], 21 + order * 2 + slot, to_x)
                 for slot, row in enumerate(halves)] for order, half in enumerate(halves)]
    dn_first = [remote(sums.at[core, 1, :, cols_of((1 - pos_y) * 2 + col, dn_cols)], fwd_dn.at[slot], 25 + slot, to_y)
                for slot, col in enumerate((1 - pos_x, pos_x))]
    up_next = [remote(sums.at[core, 0, rows_of(chip_y), cols_of(half, GRAD_HALF)], last_up.at[:, cols_of(half, GRAD_HALF)],
                      27 + order, to_y) for order, half in enumerate(halves)]
    dn_next = remote(sums.at[core, 1, :, cols_of(chip_x, dn_cols)], last_dn, 29, to_x)

    def add_up(index, order):
        cols = cols_of(halves[order], GRAD_HALF)
        sums[core, 0, rows_of(index), cols] += part[0, rows_of(index), cols]

    def add_dn(index):
        cols = cols_of(index, dn_cols)
        sums[core, 1, :, cols] += part[1, :, cols]

    def scatter_half(order):
        for kind in range(2):
            for tile in range(n_sub):
                part_copy(kind, order * n_sub + tile).wait_recv()
        for slot in range(2):
            add_up((halves[slot]) * 2 + 1 - pos_x, order)
            up_first[order][slot].start()
            if order == 0:
                add_dn((1 - pos_y) * 2 + (1 - pos_x if slot == 0 else pos_x))
                dn_first[slot].start()
        add_up(chip_y, order)
        if order == 1:
            add_dn(chip_x)
            add_dn(chip)
        add_up(chip, order)

    loads[0].wait()
    for block in (1, 0):
        own = core == block

        @pl.when(own)
        def _():
            for copy in loads[1:4]:
                copy.wait()

        @pl.when(jnp.logical_not(own))
        def _():
            swap_acts.wait_recv()

        acts_row[...] = acts[block].T
        grad_row[...] = grad[...].T
        def tile_step(step, carry, block=block, own=own):
            late = step // n_sub
            cols = cols_of((1 - pos_y + late * (2 * pos_y - 1)) * n_sub + lax.rem(step, n_sub), GRAD_TILE)

            @pl.when(jnp.logical_and(jnp.logical_not(own), step < n_sub))
            def _():
                swap_piece(0, step).wait_recv()
                swap_piece(1, step).wait_recv()

            @pl.when(jnp.logical_and(jnp.logical_not(own), step == n_sub))
            def _():
                for copy in swap_late:
                    copy.wait_recv()

            half, at_step = (0, 2 * n_sub - 1) if block == 1 else (1, n_sub)
            pl.when(jnp.logical_and(core == 1, step == at_step))(functools.partial(scatter_half, half))

            pre_act = jnp.dot(acts_row[...], wts[block, 0, :, cols], preferred_element_type=jnp.float32)
            d_hidden = jnp.dot(grad_row[...], wts[block, 1, :, cols], preferred_element_type=jnp.float32)
            hidden, slope = gelu_pair(pre_act)
            dw_down = jnp.dot(grad[...], hidden.astype(jnp.bfloat16), preferred_element_type=jnp.float32)
            d_tile = (d_hidden * slope).astype(jnp.bfloat16)
            if block == 1:
                d_pre[:, cols] = d_tile
            dw_up = jnp.dot(acts[block], d_tile, preferred_element_type=jnp.float32)

            @pl.when(jnp.logical_and(own, step == 0))
            def _():
                for copy in loads[4:6]:
                    copy.wait()

            @pl.when(own)
            def _():
                sums[block, 0, :, cols] += dw_up
                sums[block, 1, :, cols] += dw_down

            @pl.when(jnp.logical_not(own))
            def _():
                sums[block, 0, :, cols] = dw_up
                sums[block, 1, :, cols] = dw_down
                part_copy(0, step).start()
                part_copy(1, step).start()
            return carry

        lax.fori_loop(0, 2 * n_sub, tile_step, 0)
        if block == 1:
            d_in = lax.dot_general(wts[1, 0], d_pre[...], (((1,), (1,)), ((), ())), preferred_element_type=jnp.float32)
            grad[...] = (grad[...].astype(jnp.float32) + d_in).astype(jnp.bfloat16)

    @pl.when(core == 0)
    def _():
        scatter_half(0)
        scatter_half(1)

    for copy in loads[6:]:
        copy.start()

    n_slot = 2 * half_rows // ROW_TILE
    per_micro = micro_in.shape[2] // ROW_TILE

    def x_slot(tile):
        slot = lax.rem(tile, n_slot)
        return acts.at[slot // 2, :, cols_of(lax.rem(slot, 2), ROW_TILE)]

    def x_load(tile):
        return pltpu.make_async_copy(micro_in.at[tile_place(n_own, per_micro, core, tile)], x_slot(tile), tile_sem.at[0, lax.rem(tile, n_slot)])

    start_all([x_load(tile) for tile in range(n_slot)])

    up_first[0][0].wait_recv()
    cols = cols_of(halves[0], GRAD_HALF)
    sums[core, 0, rows_of(chip_y), cols] += fwd_up[0, :, cols]
    up_next[0].start()
    dn_first[0].wait_recv()
    sums[core, 1, :, cols_of(chip_x, dn_cols)] += fwd_dn[0]
    dn_next.start()
    up_first[1][0].wait_recv()
    cols = cols_of(halves[1], GRAD_HALF)
    sums[core, 0, rows_of(chip_y), cols] += fwd_up[0, :, cols]
    up_next[1].start()
    for order in range(2):
        up_first[order][1].wait_recv()
        up_next[order].wait_recv()
    dn_first[1].wait_recv()
    scale = 1.0 / n_data
    mean_up = (sums[core, 0, rows_of(chip)] + fwd_up[1] + last_up[...]) * scale
    last_up[...] = mean_up
    square = jnp.sum((mean_up * mean_up).reshape(up_rows // 8, 8, ff_width), axis=0)
    dn_next.wait_recv()
    mean_dn = (sums[core, 1, :, cols_of(chip, dn_cols)] + fwd_dn[1] + last_dn[...]) * scale
    last_dn[...] = mean_dn
    square_dn = jnp.sum((mean_dn * mean_dn).reshape(width // 8, 8, dn_cols), axis=0)
    tile_sum = sum(square[:, first:first + 128] for first in range(0, ff_width, 128))
    tile_sum = tile_sum + sum(square_dn[:, first:first + 128] for first in range(0, dn_cols, 128))
    norm_tiles[me] = tile_sum
    norm_copies = []
    for offset in range(1, n_dev):
        other = lax.rem(me + offset, n_dev)
        norm_copies.append(remote(norm_tiles.at[me], norm_tiles.at[me], 29 + offset, (other // 2, lax.rem(other, 2))))
    for copy in norm_copies:
        copy.start()
    for copy in loads[6:]:
        copy.wait()
    for copy in norm_copies:
        copy.wait_recv()
    total_sq = jnp.sum(jnp.sum(norm_tiles[...], axis=0), keepdims=True)
    clip = jnp.minimum(1.0, norm_ref[0] / (jnp.sqrt(total_sq) + NORM_EPS))
    rate = rate_ref[0]

    chips = (chip, chip_x, chip_y, chip_d)
    up_at = [wts.at[core, 0, rows_of(index)] for index in chips]
    dn_at = [wts.at[core, 1, :, cols_of(index, dn_cols)] for index in chips]
    up_x, up_y, up_relay = remote(up_at[0], up_at[0], 37, to_x), remote(up_at[0], up_at[0], 38, to_y), remote(up_at[1], up_at[1], 39, to_y)
    dn_x, dn_y, dn_relay = remote(dn_at[0], dn_at[0], 40, to_x), remote(dn_at[0], dn_at[0], 41, to_y), remote(dn_at[2], dn_at[2], 42, to_x)
    up_peer = [remote(up_at[index], up_at[index], 43 + index, to_peer) for index in range(4)]
    dn_peer = [remote(dn_at[index], dn_at[index], 47 + index, to_peer) for index in range(4)]

    def gather_up():
        up_x.start()
        up_y.start()
        up_peer[0].start()

    def gather_dn():
        dn_y.start()
        dn_x.start()
        dn_peer[0].start()

    def gather_relay():
        up_x.wait_recv()
        up_relay.start()
        up_peer[1].start()
        dn_y.wait_recv()
        dn_relay.start()
        dn_peer[2].start()

    def gather_near():
        up_y.wait_recv()
        up_peer[2].start()
        dn_x.wait_recv()
        dn_peer[1].start()

    def gather_far():
        up_relay.wait_recv()
        up_peer[3].start()
        dn_relay.wait_recv()
        dn_peer[3].start()

    def gather_peer():
        for copy in up_peer + dn_peer:
            copy.wait_recv()

    state = adamw_update(*[ref[...] for ref in up_state], clip * last_up[...], rate)
    wts[core, 0, rows_of(chip)] = state[0].astype(jnp.bfloat16)
    for ref, value in zip(up_state, state):
        ref[...] = value
    pl.when(core == 0)(gather_up)
    state = adamw_update(*[ref[...] for ref in dn_state], clip * last_dn[...], rate)
    wts[core, 1, :, cols_of(chip, dn_cols)] = state[0].astype(jnp.bfloat16)
    for ref, value in zip(dn_state, state):
        ref[...] = value
    pl.when(core == 0)(gather_dn)
    stores = [pltpu.make_async_copy(src, dst, store_sem.at[index]) for index, (src, dst) in enumerate([
        *zip(up_state, (new_up, out1_up, out2_up)), *zip(dn_state, (new_dn, out1_dn, out2_dn))])]
    for copy in stores:
        copy.start()

    @pl.when(core == 0)
    def _():
        gather_relay()
        gather_near()
        gather_far()

    @pl.when(core == 1)
    def _():
        gather_peer()
        gather_up()
        gather_dn()

    swap_acts.wait_send()
    for order in range(2):
        for copy in up_first[order] + [up_next[order]]:
            copy.wait_send()
        for kind in range(2):
            for tile in range(n_sub):
                part_copy(kind, order * n_sub + tile).wait_send()
    for copy in dn_first + [dn_next] + norm_copies + swap_late + [swap_piece(kind, tile) for kind in range(2) for tile in range(n_sub)]:
        copy.wait_send()

    def weights_out(block):
        return [pltpu.make_async_copy(turned.at[block], w_up_out.at[block], store_sem.at[6 + block]),
                pltpu.make_async_copy(wts.at[block, 1], w_dn_out.at[block], store_sem.at[8 + block])]

    n_first = own_first.shape[0]
    per_row = ff_width // ROW_TILE

    def mid_slot(tile):
        row = tile // per_row
        return row // 2, lax.rem(row, 2), slice(None), cols_of(lax.rem(tile, per_row), ROW_TILE)

    turned[0] = wts[0, 0].T
    start_all(weights_out(0))

    def first_block(pair, carry):
        for number, action in ((2, gather_relay), (3, gather_near), (4, gather_far)):
            pl.when(jnp.logical_and(core == 1, pair == number))(action)
        tiles = (2 * pair, 2 * pair + 1)
        wait_all([x_load(tile) for tile in tiles])
        for half, tile in enumerate(tiles):
            mid = tile_forward(x_slot(tile)[...], turned.at[0], wts.at[0, 1], hidden_ref.at[half], FF_TILE)
            sums[mid_slot(tile)] = mid.astype(jnp.float32)
        pl.when(tiles[1] + n_slot < N_MID)(lambda: start_all([x_load(tile + n_slot) for tile in tiles]))
        return carry

    lax.fori_loop(0, N_MID // 2, first_block, 0)
    pl.when(core == 0)(gather_peer)
    turned[1] = wts[1, 0].T
    start_all(weights_out(1))

    def y_out(tile):
        slot = lax.rem(tile, n_slot)
        keep = pltpu.make_async_copy(x_slot(tile), own_first.at[tile], tile_sem.at[1, slot])
        give = pltpu.make_async_remote_copy(src_ref=x_slot(tile), dst_ref=peer_first.at[tile], send_sem=tile_sem.at[2, slot],
                                            recv_sem=recv_sem.at[51 + tile], device_id=to_peer, device_id_type=MESH_ID)
        return keep, give

    def y_wait(tile):
        keep, give = y_out(tile)
        keep.wait()
        give.wait_send()

    def second_block(pair, carry):
        tiles = (2 * pair, 2 * pair + 1)
        for tile in tiles:
            pl.when(pair >= 2)(functools.partial(y_wait, tile - n_slot))
        for half, tile in enumerate(tiles):
            place = x_slot(tile)
            place[...] = tile_forward(sums[mid_slot(tile)].astype(jnp.bfloat16), turned.at[1], wts.at[1, 1], hidden_ref.at[half], FF_TILE)
        for tile in tiles:
            start_all(y_out(tile))
        return carry

    n_late = ff_width // ROW_TILE

    def late_slot(tile):
        return d_pre.at[0:width, cols_of(lax.rem(tile, n_late), ROW_TILE)]

    def late_load(tile):
        return pltpu.make_async_copy(micro_in.at[tile_place(n_own, per_micro, core, tile)], late_slot(tile), tile_sem.at[3, lax.rem(tile, n_late)])

    def whole_tile(tile, carry):
        y_wait(tile - n_slot)
        late_load(tile).wait()
        cols = late_slot(tile)[...]
        for block in range(2):
            cols = tile_forward(cols, turned.at[block], wts.at[block, 1], hidden_ref.at[block], FF_TILE)
        place = x_slot(tile)
        place[...] = cols
        start_all(y_out(tile))
        pl.when(tile + n_late < n_first)(lambda: late_load(tile + n_late).start())
        return carry

    start_all([late_load(N_MID + tile) for tile in range(n_late)])
    lax.fori_loop(0, N_MID // 2, second_block, 0)
    lax.fori_loop(N_MID, n_first, whole_tile, 0)
    for tile in range(n_first - n_slot, n_first):
        y_wait(tile)
    for tile in range(n_first):
        y_out(tile)[1].wait_recv()

    for copy in [up_x, up_y, up_relay, dn_x, dn_y, dn_relay] + up_peer + dn_peer:
        copy.wait_send()
    for copy in stores + weights_out(0) + weights_out(1):
        copy.wait()


def update_weights(n_data, arrays, learn_rate, max_norm):
    width, ff_width = arrays[6].shape
    n_rows = arrays[11].shape[1]
    half_rows = n_rows // 2
    up_rows, dn_cols = arrays[0].shape[0], arrays[1].shape[1]
    f32, bf16 = jnp.float32, jnp.bfloat16
    up_state, dn_state = jax.ShapeDtypeStruct((up_rows, ff_width), f32), jax.ShapeDtypeStruct((width, dn_cols), f32)
    first = jax.ShapeDtypeStruct((N_FIRST, width, ROW_TILE), bf16)
    any_spec = pl.BlockSpec(memory_space=pl.ANY)
    smem_spec = pl.BlockSpec(memory_space=pltpu.SMEM)
    n_sem = 51 + N_FIRST

    def body(*refs):
        update_kernel(n_data, *refs)

    flops = 20 * half_rows * width * ff_width + 8 * N_FIRST * ROW_TILE * width * ff_width
    return pl.pallas_call(
        body,
        in_specs=[any_spec] * 13 + [smem_spec] * 2,
        out_specs=[any_spec] * 10,
        out_shape=[up_state, dn_state, up_state, up_state, dn_state, dn_state,
                   jax.ShapeDtypeStruct((2, ff_width, width), bf16), jax.ShapeDtypeStruct((2, width, ff_width), bf16), first, first],
        scratch_shapes=[
            pltpu.VMEM((2, 2, width, ff_width), bf16), pltpu.VMEM((2, width, half_rows), bf16),
            pltpu.VMEM((half_rows, width), bf16), pltpu.VMEM((width, half_rows), bf16), pltpu.VMEM((half_rows, width), bf16),
            pltpu.VMEM((half_rows, ff_width), bf16), pltpu.VMEM((2, 2, width, ff_width), f32), pltpu.VMEM((2, width, ff_width), f32),
            pltpu.VMEM((2, up_rows, ff_width), f32), pltpu.VMEM((2, width, dn_cols), f32),
            pltpu.VMEM((up_rows, ff_width), f32), pltpu.VMEM((width, dn_cols), f32), pltpu.VMEM((2 * n_data, 8, 128), f32),
            pltpu.VMEM((2, ff_width, width), bf16), pltpu.VMEM((2, ff_width, ROW_TILE), bf16),
            pltpu.SemaphoreType.DMA((n_sem,)), pltpu.SemaphoreType.DMA((n_sem,)), pltpu.SemaphoreType.DMA((12,)),
            pltpu.SemaphoreType.DMA((10,)), pltpu.SemaphoreType.DMA((4, 4))],
        compiler_params=pltpu.CompilerParams(collective_id=0, has_side_effects=True, vmem_limit_bytes=VMEM_LIMIT),
        cost_estimate=pl.CostEstimate(flops=flops, bytes_accessed=60000000, transcendentals=0),
        name="update",
    )(*arrays, learn_rate.reshape(1), max_norm.reshape(1))


def solution(mesh):
    n_data = mesh.shape['data']

    def step_body(master_up, master_down, moment1_up, moment2_up, moment1_down, moment2_down,
                  compute_up, compute_down, accum_up, accum_down, stage_acts, loss_grad, next_micro,
                  learn_rate, max_norm):
        arrays = (master_up[0], master_down[0].T, moment1_up[0], moment2_up[0], moment1_down[0].T, moment2_down[0].T,
                  compute_up[0], compute_down[0].T, accum_up[0, 0], accum_down[0, 0].T, stage_acts[0].T, loss_grad.T,
                  jnp.swapaxes(next_micro, 1, 2))
        *states, w_up_t, w_dn_t, own_first, peer_first = update_weights(n_data, arrays, learn_rate, max_norm)
        last_acts, states = forward_rest(arrays[12], w_up_t, w_dn_t, own_first, peer_first, states)
        new_up, new_dn, out1_up, out2_up, out1_dn, out2_dn = states
        return (new_up[None], new_dn.T[None], out1_up[None], out2_up[None], out1_dn.T[None], out2_dn.T[None], last_acts)

    shard_spec = P('stage', 'data', None)
    whole_spec = P('stage', None, None)
    accum_spec = P('data', 'stage', None, None)
    micro_spec = P(None, 'data', None)
    in_specs = (shard_spec,) * 6 + (whole_spec, whole_spec, accum_spec, accum_spec,
                                    P('stage', 'data', None), P('data', None), micro_spec, P(), P())
    out_specs = (shard_spec,) * 6 + (micro_spec,)
    return jax.shard_map(step_body, mesh=mesh, in_specs=in_specs, out_specs=out_specs, check_vma=False)
```
